32 devices in a mesh: dp: 8 (over z, y), replica: 4 (over x, core).
Axes of the slice: x: 2, y: 2, z: 4, core: 2. Of those that a mesh axis runs over, the one named last changes fastest.
Arguments:
- text_tokens: bfloat16 [32768, 384], P(('dp', 'replica')), may hold values from -6 to 6
- segment_ids: int32 [512, 64], P(('dp', 'replica')), may hold values from 0 to 3, never falling along the last dimension, each value on 1 to 32 neighbouring positions
- pair_index: int32 [2048], P(('dp', 'replica')), may hold values from 0 to 2047, each once
- image_tokens: bfloat16 [2048, 50, 384], P(('dp', 'replica')), may hold values from -6 to 6
- img_ln1: float32 [384], replicated, may hold values from 0.5 to 1.5
- img_qkv: bfloat16 [384, 1152], replicated, may hold values from -0.4375 to 0.4375
- img_out: bfloat16 [384, 384], replicated, may hold values from -1.75 to 1.75
- img_ln2: float32 [384], replicated, may hold values from 0.5 to 1.5
- img_up: bfloat16 [384, 1536], replicated, may hold values from -0.3125 to 0.3125
- img_down: bfloat16 [1536, 384], replicated, may hold values from -0.15625 to 0.15625
- img_proj: bfloat16 [384, 384], replicated, may hold values from -0.3125 to 0.3125
- txt_ln1: float32 [384], replicated, may hold values from 0.5 to 1.5
- txt_qkv: bfloat16 [384, 1152], replicated, may hold values from -0.4375 to 0.4375
- txt_out: bfloat16 [384, 384], replicated, may hold values from -1.25 to 1.25
- txt_ln2: float32 [384], replicated, may hold values from 0.5 to 1.5
- txt_up: bfloat16 [384, 1536], replicated, may hold values from -0.3125 to 0.3125
- txt_down: bfloat16 [1536, 384], replicated, may hold values from -0.15625 to 0.15625
- txt_proj: bfloat16 [384, 384], replicated, may hold values from -0.3125 to 0.3125
- log_scale: float32 [1], replicated, may hold values from 3 to 4.1
Outputs:
- loss: float32 [1], replicated
- grad_text_tokens: float32 [32768, 384], P(('dp', 'replica'))
- grad_txt_ln1: float32 [384], replicated
- grad_txt_qkv: float32 [384, 1152], replicated
- grad_txt_out: float32 [384, 384], replicated
- grad_txt_ln2: float32 [384], replicated
- grad_txt_up: float32 [384, 1536], replicated
- grad_txt_down: float32 [1536, 384], replicated
- grad_txt_proj: float32 [384, 384], replicated
- grad_log_scale: float32 [1], replicated
The draws below stay inside these ranges and needn't reach their ends.
Inputs may be any that keep to these rules, and one draw needn't show every extreme that they name: `segment_ids`: in every packed row the ids never fall, every caption 0 to 3 appears, and a caption has 1 to 32 tokens. `pair_index`: a permutation: every image is paired with exactly one caption.
All inputs are finite; a program needn't handle non-finite values.
Results may differ from the reference program's by a relative error of at most 0.014.
The reference program's roundings to bfloat16 on the way count: a program that leaves them out, or rounds other values in their place, can miss the bound.
Values may be sent and summed in bfloat16 or wider, within the bound.
No kernel may reach another device: no remote copies, remote signals or barrier semaphores. Data moves between devices by JAX's collectives and lax.ppermute only.
A program may use at most 192 MiB of HBM per device.

```python
import math
import jax
import jax.numpy as jnp
import numpy as np
from jax import lax

D = 384
HEADS = 6
HEAD = 64
FF = 1536
EMB = 384
TEXT_LEN = 64
IMG_LEN = 50
PACK = 4
CAPS_DEV = 64
ROWS = 512
CAPTIONS = 2048
TXT_TOKENS = 32768


def block_levels(rng, dims, cuts, least, largest):
    gain, own = 1.0, jax.random.fold_in(rng, 6)
    for dim, parts in cuts:
        draws = jnp.exp(jax.random.uniform(jax.random.fold_in(own, dim), (parts,), jnp.float32, least / len(cuts), largest / len(cuts)))
        gain = gain * jnp.repeat(draws, dims[dim] // parts).reshape([-1 if axis == dim else 1 for axis in range(len(dims))])
    return gain


def length_profile(count, total, reach, slope):
    loads = [(1 << 20) // math.isqrt(rank ** slope) + 1 for rank in range(2, count + 1)]
    rest, given = total - reach - (count - 1), [1] * (count - 1)
    while rest > 0:
        candidates = [i for i in range(count - 1) if given[i] < reach]
        pool, remaining = sum([loads[i] for i in candidates]), rest
        for i in candidates:
            more = min(reach - given[i], max(1, remaining * loads[i] // pool), rest)
            given[i] = given[i] + more
            rest = rest - more
    return np.array([reach] + given)


def ragged(rng, number_of, total, bound, slope):
    if number_of == 2:
        one = jax.random.randint(rng, (), max(1, total - bound), min(bound, total - 1) + 1)
        return jnp.stack([one, total - one])
    tallies = jnp.asarray(length_profile(number_of, total, bound, slope), jnp.int32)
    couples = (number_of - 1) // 2
    donor, receiver = tallies[1:1 + 2 * couples:2], tallies[2:2 + 2 * couples:2]
    room = jnp.minimum(donor - 1, bound - receiver)
    moved = jax.random.randint(jax.random.fold_in(rng, 1), (couples,), 0, 1 << 20) % (room + 1)
    tallies = tallies.at[1:1 + 2 * couples:2].set(donor - moved).at[2:2 + 2 * couples:2].set(receiver + moved)
    return tallies[jax.random.permutation(jax.random.fold_in(rng, 2), number_of)]


def centred(key, dims, width, bound, pieces=(), kind=jnp.bfloat16):
    result = width * jax.random.normal(key, dims, jnp.float32)
    if pieces:
        result = result * block_levels(key, dims, pieces, -0.22, 0.18)
    return jnp.clip(result, -bound, bound).astype(kind)


def setup_inputs(seed: int = 0) -> dict:
    keys = jax.random.split(jax.random.key(seed), 20)
    text_tokens = centred(keys[0], (TXT_TOKENS, D), 1.0, 6.0, ((0, 32),))
    segment_ids = jax.vmap(lambda own: jnp.searchsorted(jnp.cumsum(ragged(own, PACK, TEXT_LEN, 32, 1)), jnp.arange(TEXT_LEN), side="right"))(jax.random.split(keys[1], ROWS)).reshape((ROWS, TEXT_LEN)).astype(jnp.int32)
    pair_index = jax.random.permutation(keys[2], CAPTIONS).astype(jnp.int32)
    image_tokens = centred(keys[3], (CAPTIONS, IMG_LEN, D), 1.0, 6.0, ((0, 32),))
    img_ln1 = jnp.clip(1.0 + 0.1 * jax.random.normal(keys[4], (D,), jnp.float32), 0.5, 1.5)
    img_qkv = centred(keys[5], (D, 3 * D), (D // 2) ** -0.5, 0.4375)
    img_out = centred(keys[6], (D, D), (D // 32) ** -0.5, 1.75)
    img_ln2 = jnp.clip(1.0 + 0.1 * jax.random.normal(keys[7], (D,), jnp.float32), 0.5, 1.5)
    img_up = centred(keys[8], (D, FF), D ** -0.5, 0.3125)
    img_down = centred(keys[9], (FF, D), FF ** -0.5, 0.15625)
    img_proj = centred(keys[10], (D, EMB), D ** -0.5, 0.3125)
    txt_ln1 = jnp.clip(1.0 + 0.1 * jax.random.normal(keys[11], (D,), jnp.float32), 0.5, 1.5)
    txt_qkv = centred(keys[12], (D, 3 * D), (D // 2) ** -0.5, 0.4375)
    txt_out = centred(keys[13], (D, D), (D // 16) ** -0.5, 1.25)
    txt_ln2 = jnp.clip(1.0 + 0.1 * jax.random.normal(keys[14], (D,), jnp.float32), 0.5, 1.5)
    txt_up = centred(keys[15], (D, FF), D ** -0.5, 0.3125)
    txt_down = centred(keys[16], (FF, D), FF ** -0.5, 0.15625)
    txt_proj = centred(keys[17], (D, EMB), D ** -0.5, 0.3125)
    log_scale = jnp.clip(jax.random.uniform(keys[18], (1,), jnp.float32, 3.0, 4.1), 3.0, 4.1)
    return dict(text_tokens=text_tokens, segment_ids=segment_ids, pair_index=pair_index, image_tokens=image_tokens, img_ln1=img_ln1, img_qkv=img_qkv, img_out=img_out, img_ln2=img_ln2, img_up=img_up, img_down=img_down, img_proj=img_proj, txt_ln1=txt_ln1, txt_qkv=txt_qkv, txt_out=txt_out, txt_ln2=txt_ln2, txt_up=txt_up, txt_down=txt_down, txt_proj=txt_proj, log_scale=log_scale)


precise = lax.Precision.HIGHEST

@jax.custom_vjp
def low(v):
    return lax.optimization_barrier(v.astype(jnp.bfloat16)).astype(jnp.float32)

@jax.custom_vjp
def low_back(v):
    return v

def low_keep(v):
    return (low(v), None)

def low_pass(kept, grad):
    return (grad,)

def back_keep(v):
    return (v, None)

def back_low(kept, grad):
    return (low(grad),)
low.defvjp(low_keep, low_pass)
low_back.defvjp(back_keep, back_low)

def matmul(left_mat, right_mat):
    return jnp.dot(left_mat, right_mat, precision=precise)

def layer_norm(values, gain_vec):
    centre = values - lax.optimization_barrier(jnp.mean(values, -1, keepdims=True))
    spread = lax.optimization_barrier(jnp.mean(centre * centre, -1, keepdims=True))
    return centre * lax.rsqrt(spread + 1e-06) * gain_vec

def gelu_tanh(values):
    return jax.nn.gelu(values, approximate=True)

def softmax_rows(scores):
    top_val = lax.optimization_barrier(jnp.max(scores, -1, keepdims=True))
    expo_val = jnp.exp(scores - top_val)
    return expo_val / lax.optimization_barrier(jnp.sum(expo_val, -1, keepdims=True))

def log_total(scores):
    top_val = lax.optimization_barrier(jnp.max(scores, -1, keepdims=True))
    return top_val[..., 0] + jnp.log(lax.optimization_barrier(jnp.sum(jnp.exp(scores - top_val), -1)))

def unit_rows(values):
    return values * lax.rsqrt(lax.optimization_barrier(jnp.sum(values * values, -1, keepdims=True)) + 1e-06)

def block_core(tokens_in, weights, groups, group_len, keep_mask):
    gain_one, w_qkv, w_out, gain_two, w_up, w_down = weights
    normed = low(layer_norm(tokens_in, gain_one))
    packed = low_back(low(matmul(normed, w_qkv))).reshape(groups, group_len, 3, HEADS, HEAD)
    scores = low_back(jnp.einsum('gqhd,gkhd->ghqk', packed[:, :, 0], packed[:, :, 1], precision=precise) * HEAD ** (-0.5))
    if keep_mask is not None:
        scores = jnp.where(keep_mask[:, None], scores, -1000000000.0)
    weights_p = low(softmax_rows(scores))
    attended = jnp.einsum('ghqk,gkhd->gqhd', weights_p, packed[:, :, 2], precision=precise).reshape(groups * group_len, D)
    attended = low_back(low(attended))
    residual = tokens_in + low_back(matmul(attended, w_out))
    normed_two = low(layer_norm(residual, gain_two))
    hidden_act = low(gelu_tanh(low_back(matmul(normed_two, w_up))))
    return residual + low_back(matmul(hidden_act, w_down))

def text_pool(tokens_in, seg_rows, weights):
    row_count = seg_rows.shape[0]
    keep_mask = seg_rows[:, :, None] == seg_rows[:, None, :]
    out_tok = block_core(tokens_in, weights, row_count, TEXT_LEN, keep_mask)
    member = (seg_rows[:, :, None] == jnp.arange(PACK, dtype=jnp.int32)[None, None, :]).astype(jnp.float32)
    counts = lax.optimization_barrier(jnp.sum(member, 1))
    pooled = jnp.einsum('rlp,rld->rpd', member, out_tok.reshape(row_count, TEXT_LEN, D), precision=precise) / counts[:, :, None]
    return pooled.reshape(row_count * PACK, D)

def image_embed(tokens_in, weights, w_proj):
    image_count = tokens_in.shape[0]
    flat_tokens = tokens_in.reshape(image_count * IMG_LEN, D)
    out_tok = block_core(flat_tokens, weights, image_count, IMG_LEN, None)
    first_token = out_tok.reshape(image_count, IMG_LEN, D)[:, 0]
    return low(unit_rows(low_back(matmul(low(first_token), w_proj))))

def reference(text_tokens, segment_ids, pair_index, image_tokens, img_ln1, img_qkv, img_out, img_ln2, img_up, img_down, img_proj, txt_ln1, txt_qkv, txt_out, txt_ln2, txt_up, txt_down, txt_proj, log_scale):
    img_weights = (img_ln1.astype(jnp.float32), img_qkv.astype(jnp.float32), img_out.astype(jnp.float32), img_ln2.astype(jnp.float32), img_up.astype(jnp.float32), img_down.astype(jnp.float32))
    img_head = img_proj.astype(jnp.float32)
    image_blocks = image_tokens.astype(jnp.float32).reshape(CAPTIONS // CAPS_DEV, CAPS_DEV, IMG_LEN, D)
    image_emb = lax.map(lambda block_in: image_embed(block_in, img_weights, img_head), image_blocks).reshape(CAPTIONS, EMB)

    def forward(tokens32, gain_one, w_qkv, w_out, gain_two, w_up, w_down, w_proj, scale_log):
        weights = (gain_one, w_qkv, w_out, gain_two, w_up, w_down)
        tok_blocks = tokens32.reshape(ROWS // 32, 32 * TEXT_LEN, D)
        seg_blocks = segment_ids.reshape(ROWS // 32, 32, TEXT_LEN)
        pooled = lax.map(jax.checkpoint(lambda pair_in: text_pool(pair_in[0], pair_in[1], weights)), (tok_blocks, seg_blocks)).reshape(CAPTIONS, D)
        text_emb = low(unit_rows(low_back(matmul(low(pooled), w_proj))))
        inv_temp = jnp.exp(scale_log[0])

        def row_terms(pair_in):
            emb_rows, targets = pair_in
            logits = inv_temp * low_back(jnp.dot(emb_rows, image_emb.T, precision=precise))
            positive = jnp.take_along_axis(logits, targets[:, None], 1)[:, 0]
            return jnp.sum(log_total(logits)) - 2.0 * jnp.sum(positive)

        def col_terms(emb_rows):
            logits = inv_temp * low_back(jnp.dot(emb_rows, text_emb.T, precision=precise))
            return jnp.sum(log_total(logits))
        rows_part = lax.map(jax.checkpoint(row_terms), (text_emb.reshape(CAPTIONS // CAPS_DEV, CAPS_DEV, EMB), pair_index.reshape(CAPTIONS // CAPS_DEV, CAPS_DEV)))
        cols_part = lax.map(jax.checkpoint(col_terms), image_emb.reshape(CAPTIONS // CAPS_DEV, CAPS_DEV, EMB))
        return (jnp.sum(rows_part) + jnp.sum(cols_part)) / (2.0 * CAPTIONS)
    loss_value, pullback = jax.vjp(forward, text_tokens.astype(jnp.float32), txt_ln1.astype(jnp.float32), txt_qkv.astype(jnp.float32), txt_out.astype(jnp.float32), txt_ln2.astype(jnp.float32), txt_up.astype(jnp.float32), txt_down.astype(jnp.float32), txt_proj.astype(jnp.float32), log_scale.astype(jnp.float32))
    gradients = pullback(jnp.ones_like(loss_value))
    return (loss_value.reshape(1), gradients[0], gradients[1], gradients[2], gradients[3], gradients[4], gradients[5], gradients[6], gradients[7], gradients[8])
```

```python
import functools
import math

import jax
import jax.numpy as jnp
from jax import lax
from jax.experimental import pallas as pl
from jax.experimental.pallas import tpu as pltpu
from jax.sharding import PartitionSpec as P

D = 384
HEADS = 6
HEAD = 64
FF = 1536
IMG_LEN = 50
PACK = 4
CAPS = 64
TOK_BLOCK = 256
CAP_BLOCK = 16
BLOCKS = 4
PAIR = 128
IMG_BLOCK = 16
EPS = 1e-06

BF = jnp.bfloat16
F32 = jnp.float32
GELU_K = math.sqrt(2.0 / math.pi)
GELU_C = 0.044715


def mm(a, b):
    return lax.dot_general(a, b, (((1,), (0,)), ((), ())), preferred_element_type=F32)


def mm_nt(a, b):
    return lax.dot_general(a, b, (((1,), (1,)), ((), ())), preferred_element_type=F32)


def mm_tn(a, b):
    return lax.dot_general(a, b, (((0,), (0,)), ((), ())), preferred_element_type=F32)


def row_mean(v):
    return jnp.sum(v, -1, keepdims=True) * (1.0 / D)


def normalize(v):
    centre = v - row_mean(v)
    return centre * lax.rsqrt(row_mean(centre * centre) + EPS)


def split3(v):
    high = v.astype(BF)
    rest = v - high.astype(F32)
    mid = rest.astype(BF)
    low = (rest - mid.astype(F32)).astype(BF)
    return high, mid, low


def wide_mm(v, w):
    high, mid, low = split3(v)
    n = v.shape[0]
    out = mm(jnp.concatenate([high, mid, low], 0), w)
    return out[:n] + out[n : 2 * n] + out[2 * n :]


def gelu_parts(z):
    z2 = z * z
    t = jnp.tanh(z * (z2 * (GELU_K * GELU_C) + GELU_K))
    hp = t * 0.5 + 0.5
    u = z * hp
    slope = hp + (u * (1.0 - hp)) * (z2 * (6.0 * GELU_K * GELU_C) + 2.0 * GELU_K)
    return u, slope


def lanes_head(shape):
    return lax.broadcasted_iota(jnp.int32, shape, len(shape) - 1) // HEAD


def image_kernel(x_ref, g1, wqkv, wout, g2, wup, wdown, wproj, emb_ref, hs, x0, att):
    step = pl.program_id(0)

    @pl.when(step == 0)
    def _():
        hs[...] = jnp.zeros_like(hs)

    gain = g1[...]
    for i in range(IMG_BLOCK):
        x = x_ref[i].astype(F32)
        hs[64 * i : 64 * i + IMG_LEN, :] = (normalize(x) * gain).astype(BF)
        x0[pl.ds(step * IMG_BLOCK + i, 1), :] = x[0:1]
    first = x0[pl.ds(pl.multiple_of(step * IMG_BLOCK, IMG_BLOCK), IMG_BLOCK), :]
    h0 = (normalize(first) * gain).astype(BF)
    q = mm(h0, wqkv[:, :D]).astype(BF).astype(F32) * (HEAD**-0.5)
    kv = mm(hs[...], wqkv[:, D:]).astype(BF)
    head8 = lanes_head((8, D))
    rows = lax.broadcasted_iota(jnp.int32, (48, 512), 0)
    cols = lax.broadcasted_iota(jnp.int32, (48, 512), 1)
    own = (cols // 64 == rows % 8) & (cols % 64 < IMG_LEN)
    for g in range(IMG_BLOCK // 8):
        q8 = q[8 * g : 8 * g + 8]
        q48 = jnp.concatenate([jnp.where(head8 == h, q8, 0.0) for h in range(HEADS)], 0)
        s = mm_nt(q48.astype(BF), kv[512 * g : 512 * g + 512, :D])
        s = jnp.where(own, s, -1e30)
        e = jnp.exp(s - jnp.max(s, -1, keepdims=True))
        p = (e / jnp.sum(e, -1, keepdims=True)).astype(BF)
        r = mm(p, kv[512 * g : 512 * g + 512, D:])
        o8 = jnp.where(head8 == 0, r[0:8], 0.0)
        for h in range(1, HEADS):
            o8 = jnp.where(head8 == h, r[8 * h : 8 * h + 8], o8)
        att[pl.ds(pl.multiple_of(step * IMG_BLOCK + 8 * g, 8), 8), :] = o8

    @pl.when(step == pl.num_programs(0) - 1)
    def _():
        x1 = x0[...] + mm(att[...].astype(BF), wout[...])
        h2 = (normalize(x1) * g2[...]).astype(BF)
        u, _ = gelu_parts(mm(h2, wup[...]))
        y = x1 + mm(u.astype(BF), wdown[...])
        e = mm(y.astype(BF), wproj[...])
        emb_ref[...] = (e * lax.rsqrt(jnp.sum(e * e, -1, keepdims=True) + EPS)).astype(BF)


def const_spec(shape):
    zeros = (0,) * len(shape)
    return pl.BlockSpec(shape, lambda *_: zeros, pipeline_mode=pl.Buffered(1))


def image_tower(x, g1, wqkv, wout, g2, wup, wdown, wproj):
    count = x.shape[0]
    return pl.pallas_call(
        image_kernel,
        grid=(count // IMG_BLOCK,),
        in_specs=[
            pl.BlockSpec((IMG_BLOCK, IMG_LEN, D), lambda i: (i, 0, 0)),
            const_spec((1, D)),
            const_spec((D, 3 * D)),
            const_spec((D, D)),
            const_spec((1, D)),
            const_spec((D, FF)),
            const_spec((FF, D)),
            const_spec((D, D)),
        ],
        out_specs=pl.BlockSpec((count, D), lambda i: (0, 0)),
        out_shape=jax.ShapeDtypeStruct((count, D), BF),
        scratch_shapes=[
            pltpu.VMEM((IMG_BLOCK * 64, D), BF),
            pltpu.VMEM((count, D), F32),
            pltpu.VMEM((count, D), F32),
        ],
        name="image_tower",
    )(x, g1, wqkv, wout, g2, wup, wdown, wproj)


def pair_mask(lab_ref, pair):
    lab = lab_ref[0, :, PAIR * pair : PAIR * pair + PAIR].astype(F32)
    wide = jnp.broadcast_to(lab, (PAIR, PAIR))
    return wide == wide.T


def text_kernel(
    tok_ref, lab_ref, g1, wqkv, wout, g2, wup, wdown, wproj,
    h2_ref, o_ref, qkv_ref, p_ref, c2_ref, gp_ref, pu_ref, pb_ref, e_ref, emb_ref, cnt_ref,
    pt, po, osc,
):
    step = pl.program_id(0)
    tok = tok_ref[...]
    x = tok.astype(F32)
    h1 = (normalize(x) * g1[...]).astype(BF)
    qkv = mm(h1, wqkv[...]).astype(BF)
    qkv_ref[...] = qkv
    low = lax.broadcasted_iota(jnp.int32, (PAIR, PAIR), 1) < HEAD
    for pair in range(2):
        rows = slice(PAIR * pair, PAIR * pair + PAIR)
        mask = pair_mask(lab_ref, pair)
        mask = jnp.concatenate([mask, mask], 0)
        for j in range(HEADS // 2):
            cols = slice(PAIR * j, PAIR * j + PAIR)
            q2 = qkv[rows, PAIR * j : PAIR * j + PAIR] * jnp.asarray(HEAD**-0.5, BF)
            k2 = qkv[rows, D + PAIR * j : D + PAIR * j + PAIR]
            v2 = qkv[rows, 2 * D + PAIR * j : 2 * D + PAIR * j + PAIR]
            zero = jnp.zeros_like(q2)
            q22 = jnp.concatenate([jnp.where(low, q2, zero), jnp.where(low, zero, q2)], 0)
            s = jnp.where(mask, mm_nt(q22, k2), -1e30)
            ex = jnp.exp(s - jnp.max(s, -1, keepdims=True))
            p = (ex * (1.0 / jnp.sum(ex, -1, keepdims=True))).astype(BF)
            p_ref[pair, j] = p
            v22 = jnp.concatenate([jnp.where(low, v2, zero), jnp.where(low, zero, v2)], 0)
            o = mm(jnp.concatenate([p[:PAIR], p[PAIR:]], 1), v22)
            osc[rows, cols] = o.astype(BF)
    o = osc[...]
    o_ref[...] = o
    x1 = x + mm(o, wout[...])
    c2 = x1 - row_mean(x1)
    c2_ref[...] = c2
    h2 = (c2 * lax.rsqrt(row_mean(c2 * c2) + EPS) * g2[...]).astype(BF)
    h2_ref[...] = h2
    u, slope = gelu_parts(mm(h2, wup[...]))
    gp_ref[...] = slope.astype(BF)
    hit = lax.broadcasted_iota(jnp.int32, (CAP_BLOCK, TOK_BLOCK), 0) == lab_ref[0]
    member = jnp.where(hit, 1.0, 0.0)
    caps = pl.ds(pl.multiple_of(step * CAP_BLOCK, CAP_BLOCK), CAP_BLOCK)
    member_b = member.astype(BF)
    pt[caps, :] = mm(member_b, tok)
    po[caps, :] = mm(member_b, o)
    pu_ref[caps, :] = mm(member_b, u.astype(BF))
    cnt_ref[caps, :] = jnp.broadcast_to(jnp.sum(member, -1, keepdims=True), (CAP_BLOCK, 128))

    @pl.when(step == pl.num_programs(0) - 1)
    def _():
        total = pt[...] + wide_mm(po[...], wout[...]) + wide_mm(pu_ref[...], wdown[...])
        pooled = (total * (1.0 / cnt_ref[:, 0:1])).astype(BF)
        pb_ref[...] = pooled
        e = mm(pooled, wproj[...])
        e_ref[...] = e
        emb_ref[...] = (e * lax.rsqrt(jnp.sum(e * e, -1, keepdims=True) + EPS)).astype(BF)


def text_forward(tok, lab, g1, wqkv, wout, g2, wup, wdown, wproj):
    n = tok.shape[0]
    blocks = n // TOK_BLOCK

    def rows(width):
        return pl.BlockSpec((TOK_BLOCK, width), lambda i: (i, 0))

    def whole(width):
        return pl.BlockSpec((CAPS, width), lambda i: (0, 0))

    shape = jax.ShapeDtypeStruct
    return pl.pallas_call(
        text_kernel,
        grid=(blocks,),
        in_specs=[
            rows(D),
            pl.BlockSpec((1, 1, TOK_BLOCK), lambda i: (i, 0, 0)),
            const_spec((1, D)),
            const_spec((D, 3 * D)),
            const_spec((D, D)),
            const_spec((1, D)),
            const_spec((D, FF)),
            const_spec((FF, D)),
            const_spec((D, D)),
        ],
        out_specs=[
            rows(D), rows(D), rows(3 * D),
            pl.BlockSpec((2, 3, 2 * PAIR, PAIR), lambda i: (i, 0, 0, 0)),
            rows(D), rows(FF),
            whole(FF), whole(D), whole(D), whole(D), whole(128),
        ],
        out_shape=[
            shape((n, D), BF), shape((n, D), BF), shape((n, 3 * D), BF),
            shape((2 * blocks, 3, 2 * PAIR, PAIR), BF),
            shape((n, D), F32), shape((n, FF), BF),
            shape((CAPS, FF), F32), shape((CAPS, D), BF), shape((CAPS, D), F32),
            shape((CAPS, D), BF), shape((CAPS, 128), F32),
        ],
        scratch_shapes=[
            pltpu.VMEM((CAPS, D), F32),
            pltpu.VMEM((CAPS, D), F32),
            pltpu.VMEM((TOK_BLOCK, D), BF),
        ],
        name="text_forward",
    )(tok, lab, g1, wqkv, wout, g2, wup, wdown, wproj)


def cosine_kernel(scale_ref, emb, images, g_ref, sum_ref):
    scale = jnp.exp(jnp.full((1, 1), scale_ref[0], F32))
    g = mm_nt(emb[...], images[...])
    g_ref[...] = g
    sum_ref[...] = jnp.sum(jnp.exp(g * scale), 0, keepdims=True)


def rows_kernel(denom, scale_ref, g_ref, images, pair, dt_ref, part_ref):
    scale = jnp.exp(jnp.full((1, 1), scale_ref[0], F32))
    g = g_ref[...]
    logits = g * scale
    e = jnp.exp(logits)
    total = jnp.sum(e, -1, keepdims=True)
    hit = lax.broadcasted_iota(jnp.int32, g.shape, 1) == pair[...]
    target = jnp.where(hit, 1.0, 0.0)
    lse = jnp.log(total)
    pos = jnp.sum(jnp.where(hit, logits, 0.0), -1, keepdims=True)
    dl = (e * (1.0 / total) - 2.0 * target) * (1.0 / denom)
    dt_ref[...] = mm((dl * scale).astype(BF), images[...])
    temp = jnp.sum(jnp.sum(dl * g, -1, keepdims=True), 0, keepdims=True)
    loss = jnp.sum(lse - 2.0 * pos, 0, keepdims=True)
    lane = lax.broadcasted_iota(jnp.int32, (1, 128), 1)
    part_ref[...] = jnp.where(lane == 0, loss, jnp.where(lane == 1, temp, 0.0))


def place(mine, rb, acc, send_ref, keep_ref):
    for rel in range(32):
        src = acc[pl.ds(pl.multiple_of((mine ^ rel) * rb, 16), rb), :].astype(BF)
        if rel < 16:
            keep_ref[rel * rb : (rel + 1) * rb, :] = src
        else:
            send_ref[(rel - 16) * rb : (rel - 15) * rb, :] = src


def head_kernel(
    denom, devices, scale_ref, mine_ref, g_ref, images, sums, dt_row, part, e_ref, pb, cnt, pu, wproj, wdown,
    send_ref, keep_ref, du_ref, dy_ref, part_out, acc,
):
    scale = jnp.exp(jnp.full((1, 1), scale_ref[0], F32))
    g = g_ref[...]
    total = sums[...]
    dl = jnp.exp(g * scale) * (1.0 / total) * (1.0 / denom)
    temp = jnp.sum(jnp.sum(dl * g, -1, keepdims=True), 0, keepdims=True)
    lse = jnp.sum(jnp.log(total), -1, keepdims=True)
    lane = lax.broadcasted_iota(jnp.int32, (1, 128), 1)
    both = part[...] + jnp.where(lane == 0, lse * (1.0 / devices), jnp.where(lane == 1, temp, 0.0))
    part_out[...] = both * jnp.where(lane == 0, 1.0 / denom, scale)
    dt = dt_row[...] + mm((dl * scale).astype(BF), images[...])
    e = e_ref[...]
    r = lax.rsqrt(jnp.sum(e * e, -1, keepdims=True) + EPS)
    de = (dt - e * (r * r * jnp.sum(dt * e, -1, keepdims=True))) * r
    de = de.astype(BF)
    dpooled = mm_nt(de, wproj[...])
    dy = dpooled * (1.0 / cnt[:, 0:1])
    dyb = dy.astype(BF)
    du = mm_nt(dyb, wdown[...])
    for i, piece in enumerate(split3(du)):
        for b in range(BLOCKS):
            du_ref[b, CAP_BLOCK * i : CAP_BLOCK * (i + 1), :] = piece[CAP_BLOCK * b : CAP_BLOCK * (b + 1)]
    for i, piece in enumerate(split3(dy)):
        for b in range(BLOCKS):
            dy_ref[b, CAP_BLOCK * i : CAP_BLOCK * (i + 1), :] = piece[CAP_BLOCK * b : CAP_BLOCK * (b + 1)]
    acc[0:FF, :] = mm_tn(jnp.concatenate(split3(pu[...]), 0), jnp.concatenate([dyb, dyb, dyb], 0))
    acc[FF : FF + D, :] = mm_tn(pb[...], de)
    acc[FF + D :, :] = jnp.zeros((2048 - FF - D, D), F32)
    place(mine_ref[0], 64, acc, send_ref, keep_ref)


def mlp_back_kernel(
    mine_ref, lab_ref, h2_ref, gp_ref, c2_ref, du_ref, dy_ref, g2, wup,
    dx_ref, gain_ref, send_ref, keep_ref, acc,
):
    step = pl.program_id(0)

    @pl.when(step == 0)
    def _():
        acc[...] = jnp.zeros_like(acc)
        gain_ref[...] = jnp.zeros_like(gain_ref)

    hit = lax.broadcasted_iota(jnp.int32, (3 * CAP_BLOCK, TOK_BLOCK), 0) % CAP_BLOCK == lab_ref[0]
    spread = jnp.where(hit, 1.0, 0.0).astype(BF)
    du = mm_tn(spread, du_ref[0])
    dz = (du * gp_ref[...].astype(F32)).astype(BF)
    dy = mm_tn(spread, dy_ref[0])
    dh = mm_nt(dz, wup[...])
    c2 = c2_ref[...]
    r = lax.rsqrt(row_mean(c2 * c2) + EPS)
    unit = c2 * r
    gain_ref[...] += jnp.sum(dh * unit, 0, keepdims=True)
    dn = dh * g2[...]
    dx_ref[...] = dy + r * (dn - row_mean(dn) - unit * row_mean(dn * unit))
    h2 = h2_ref[...]
    for k in range(4):
        acc[D * k : D * (k + 1), :] += mm_tn(h2, dz[:, D * k : D * (k + 1)])

    @pl.when(step == pl.num_programs(0) - 1)
    def _():
        place(mine_ref[0], 48, acc, send_ref, keep_ref)


def att_back_kernel(
    mine_ref, tok_ref, qkv_ref, p_ref, o_ref, dx_ref, g1, wqkv, wout,
    gtok_ref, gain_ref, send_ref, keep_ref, acc, dsc,
):
    step = pl.program_id(0)

    @pl.when(step == 0)
    def _():
        acc[...] = jnp.zeros_like(acc)
        gain_ref[...] = jnp.zeros_like(gain_ref)

    dx = dx_ref[...]
    dxb = dx.astype(BF)
    acc[0:D, :] += mm_tn(o_ref[...], dxb)
    do = mm_nt(dxb, wout[...]).astype(BF)
    low = lax.broadcasted_iota(jnp.int32, (PAIR, PAIR), 1) < HEAD
    zero = jnp.zeros((PAIR, PAIR), BF)
    half = HEAD**-0.5

    def twice(v):
        return jnp.concatenate([jnp.where(low, v, zero), jnp.where(low, zero, v)], 0)

    for pair in range(2):
        rows = slice(PAIR * pair, PAIR * pair + PAIR)
        for j in range(HEADS // 2):
            cols = slice(PAIR * j, PAIR * j + PAIR)
            q2 = qkv_ref[rows, PAIR * j : PAIR * j + PAIR]
            k2 = qkv_ref[rows, D + PAIR * j : D + PAIR * j + PAIR]
            v2 = qkv_ref[rows, 2 * D + PAIR * j : 2 * D + PAIR * j + PAIR]
            do2 = twice(do[rows, cols])
            pb = p_ref[pair, j]
            p = pb.astype(F32)
            dp = mm_nt(do2, v2)
            ds = (p * (dp - jnp.sum(dp * p, -1, keepdims=True))).astype(BF)
            dq = mm(jnp.concatenate([ds[:PAIR], ds[PAIR:]], 1), twice(k2)) * half
            dk = mm_tn(ds, twice(q2)) * half
            dv = mm_tn(pb, do2)
            dsc[rows, PAIR * j : PAIR * j + PAIR] = dq.astype(BF)
            dsc[rows, D + PAIR * j : D + PAIR * j + PAIR] = dk.astype(BF)
            dsc[rows, 2 * D + PAIR * j : 2 * D + PAIR * j + PAIR] = dv.astype(BF)
    x = tok_ref[...].astype(F32)
    centre = x - row_mean(x)
    r = lax.rsqrt(row_mean(centre * centre) + EPS)
    unit = centre * r
    gain = g1[...]
    h1 = (unit * gain).astype(BF)
    dqkv = dsc[...]
    for k in range(3):
        acc[D * (k + 1) : D * (k + 2), :] += mm_tn(h1, dqkv[:, D * k : D * (k + 1)])
    dh = mm_nt(dqkv, wqkv[...])
    gain_ref[...] += jnp.sum(dh * unit, 0, keepdims=True)
    dn = dh * gain
    gtok_ref[...] = dx + r * (dn - row_mean(dn) - unit * row_mean(dn * unit))

    @pl.when(step == pl.num_programs(0) - 1)
    def _():
        place(mine_ref[0], 48, acc, send_ref, keep_ref)


def spread_head_kernel(mine_ref, own, other, proj_ref, down_ref, full):
    mine = mine_ref[0]
    for rel in range(32):
        src = own if rel < 16 else other
        at = (rel % 16) * 64
        full[pl.ds(pl.multiple_of((mine ^ rel) * 64, 64), 64), :] = src[at : at + 64, :].astype(F32)
    down_ref[...] = full[0:FF, :]
    proj_ref[...] = full[FF : FF + D, :]


def spread_up_kernel(mine_ref, own, other, up_ref, full):
    mine = mine_ref[0]
    for rel in range(32):
        src = own if rel < 16 else other
        at = (rel % 16) * 48
        full[pl.ds(pl.multiple_of((mine ^ rel) * 48, 16), 48), :] = src[at : at + 48, :].astype(F32)
    for k in range(4):
        up_ref[:, D * k : D * (k + 1)] = full[D * k : D * (k + 1), :]


def spread_att_kernel(mine_ref, own, other, out_ref, qkv_ref, full):
    mine = mine_ref[0]
    for rel in range(32):
        src = own if rel < 16 else other
        at = (rel % 16) * 48
        full[pl.ds(pl.multiple_of((mine ^ rel) * 48, 16), 48), :] = src[at : at + 48, :].astype(F32)
    out_ref[...] = full[0:D, :]
    for k in range(3):
        qkv_ref[:, D * k : D * (k + 1)] = full[D * (k + 1) : D * (k + 2), :]


SMEM = pl.BlockSpec(memory_space=pltpu.SMEM)
VMEM = pl.BlockSpec(memory_space=pltpu.VMEM)


def simple(kernel, outs, scratch=(), smem=0, name=None):
    def call(*args):
        return pl.pallas_call(
            kernel,
            in_specs=[SMEM] * smem + [VMEM] * (len(args) - smem),
            out_specs=[VMEM] * len(outs),
            out_shape=[jax.ShapeDtypeStruct(s, t) for s, t in outs],
            scratch_shapes=list(scratch),
            name=name,
        )(*args)

    return call


def mlp_back(mine, lab, h2, gp, c2, du, dy, g2, wup):
    n = h2.shape[0]

    def rows(width):
        return pl.BlockSpec((TOK_BLOCK, width), lambda i: (i, 0))

    def blk(a, b):
        return pl.BlockSpec((1, a, b), lambda i: (i, 0, 0))

    shape = jax.ShapeDtypeStruct
    return pl.pallas_call(
        mlp_back_kernel,
        grid=(n // TOK_BLOCK,),
        in_specs=[
            SMEM, blk(1, TOK_BLOCK), rows(D), rows(FF), rows(D), blk(3 * CAP_BLOCK, FF), blk(3 * CAP_BLOCK, D),
            const_spec((1, D)), const_spec((D, FF)),
        ],
        out_specs=[rows(D), pl.BlockSpec((1, D), lambda i: (0, 0))]
        + [pl.BlockSpec((768, D), lambda i: (0, 0))] * 2,
        out_shape=[shape((n, D), F32), shape((1, D), F32), shape((768, D), BF), shape((768, D), BF)],
        scratch_shapes=[pltpu.VMEM((1536, D), F32)],
        name="mlp_back",
    )(mine, lab, h2, gp, c2, du, dy, g2, wup)


def att_back(mine, tok, qkv, p, o, dx, g1, wqkv, wout):
    n = tok.shape[0]

    def rows(width):
        return pl.BlockSpec((TOK_BLOCK, width), lambda i: (i, 0))

    shape = jax.ShapeDtypeStruct
    return pl.pallas_call(
        att_back_kernel,
        grid=(n // TOK_BLOCK,),
        in_specs=[
            SMEM, rows(D), rows(3 * D), pl.BlockSpec((2, 3, 2 * PAIR, PAIR), lambda i: (i, 0, 0, 0)), rows(D), rows(D),
            const_spec((1, D)), const_spec((D, 3 * D)), const_spec((D, D)),
        ],
        out_specs=[rows(D), pl.BlockSpec((1, D), lambda i: (0, 0))]
        + [pl.BlockSpec((768, D), lambda i: (0, 0))] * 2,
        out_shape=[shape((n, D), F32), shape((1, D), F32), shape((768, D), BF), shape((768, D), BF)],
        scratch_shapes=[pltpu.VMEM((1536, D), F32), pltpu.VMEM((TOK_BLOCK, 3 * D), BF)],
        name="att_back",
    )(mine, tok, qkv, p, o, dx, g1, wqkv, wout)


AXES = ("dp", "replica")


class Hops:
    def __init__(self):
        index = lax.axis_index(AXES)
        self.mine = ((index & 1) * 16 + ((index >> 1) & 3) * 4 + (index >> 3)).astype(jnp.int32).reshape(1)

    def swap(self, v, mask):
        return lax.ppermute(v, AXES, [(i, i ^ mask) for i in range(32)])

    def gather_images(self, emb):
        zs = jnp.concatenate([emb] + [self.swap(emb, 8 * m) for m in (1, 2, 3)], 0)
        ps = jnp.concatenate([zs] + [self.swap(zs, 2 * m) for m in (1, 2, 3)], 0)
        return jnp.concatenate([ps, self.swap(ps, 1)], 0)

    def image_ids(self, pair):
        owner, row = pair // CAPS, pair % CAPS
        block = ((owner & 1) * 16 + ((owner >> 1) & 3) * 4 + (owner >> 3)) ^ self.mine
        return block * CAPS + row

    def sum_columns(self, sums):
        return sums

    def total(self, v):
        for mask in (1, 2, 4, 8, 16):
            v = v + self.swap(v, mask)
        return v

    def reduce(self, send, keep, rb):
        part = keep.astype(F32) + self.swap(send, 1).astype(F32)
        part = part.astype(BF).reshape(4, 4 * rb, D)
        got = [self.swap(part[m], 2 * m) for m in (1, 2, 3)]
        part = part[0].astype(F32) + (got[0].astype(F32) + got[1].astype(F32) + got[2].astype(F32))
        part = part.astype(BF).reshape(4, rb, D)
        got = [self.swap(part[m], 8 * m) for m in (1, 2, 3)]
        part = part[0].astype(F32) + (got[0].astype(F32) + got[1].astype(F32) + got[2].astype(F32))
        return part.astype(BF)

    def collect(self, part):
        zs = jnp.concatenate([part] + [self.swap(part, 8 * m) for m in (1, 2, 3)], 0)
        ps = jnp.concatenate([zs] + [self.swap(zs, 2 * m) for m in (1, 2, 3)], 0)
        return ps, self.swap(ps, 1)

    def all_sum(self, send, keep, rb):
        return self.collect(self.reduce(send, keep, rb))


class Plain:
    def __init__(self):
        self.mine = jnp.zeros((1,), jnp.int32)

    def gather_images(self, emb):
        return lax.all_gather(emb, AXES, axis=0, tiled=True)

    def image_ids(self, pair):
        return pair

    def total(self, v):
        return lax.psum(v, AXES)

    def all_sum(self, send, keep, rb):
        both = lax.psum((keep.astype(F32), send.astype(F32)), AXES)
        return both[0].astype(BF), both[1].astype(BF)


def shards(
    devices, tuned,
    text_tokens, segment_ids, pair_index, image_tokens,
    img_ln1, img_qkv, img_out, img_ln2, img_up, img_down, img_proj,
    txt_ln1, txt_qkv, txt_out, txt_ln2, txt_up, txt_down, txt_proj, log_scale,
):
    net = Hops() if tuned else Plain()
    mine = net.mine
    total = CAPS * devices
    denom = 2.0 * total
    emb = image_tower(
        image_tokens, img_ln1.reshape(1, D), img_qkv, img_out, img_ln2.reshape(1, D), img_up, img_down, img_proj
    )
    images = net.gather_images(emb)
    row_of = jnp.arange(segment_ids.shape[0], dtype=jnp.int32) % (TOK_BLOCK // segment_ids.shape[1])
    lab = (segment_ids + PACK * row_of[:, None]).reshape(BLOCKS, 1, TOK_BLOCK)
    g1, g2 = txt_ln1.reshape(1, D), txt_ln2.reshape(1, D)
    h2, o, qkv, p, c2, gp, pu, pb, e, temb, cnt = text_forward(
        text_tokens, lab, g1, txt_qkv, txt_out, g2, txt_up, txt_down, txt_proj
    )
    g, sums = simple(cosine_kernel, [((CAPS, total), F32), ((1, total), F32)], smem=1, name="cosine")(
        log_scale, temb, images
    )
    dt_row, part = simple(
        functools.partial(rows_kernel, denom), [((CAPS, D), F32), ((1, 128), F32)], smem=1, name="rows"
    )(log_scale, g, images, net.image_ids(pair_index).reshape(CAPS, 1))
    sums = net.total(sums) if not tuned else column_total(net, sums)
    send, keep, du, dy, part = simple(
        functools.partial(head_kernel, denom, devices),
        [((1024, D), BF), ((1024, D), BF), ((BLOCKS, 48, FF), BF), ((BLOCKS, 48, D), BF), ((1, 128), F32)],
        [pltpu.VMEM((2048, D), F32)],
        smem=2,
        name="head_back",
    )(log_scale, mine, g, images, sums, dt_row, part, e, pb, cnt, pu, txt_proj, txt_down)
    grad_proj, grad_down = simple(
        spread_head_kernel, [((D, D), F32), ((FF, D), F32)], [pltpu.VMEM((2048, D), F32)], smem=1, name="spread_head"
    )(mine, *net.all_sum(send, keep, 64))
    dx, gain2, send, keep = mlp_back(mine, lab, h2, gp, c2, du, dy, g2, txt_up)
    (grad_up,) = simple(
        spread_up_kernel, [((D, FF), F32)], [pltpu.VMEM((1536, D), F32)], smem=1, name="spread_up"
    )(mine, *net.all_sum(send, keep, 48))
    grad_tokens, gain1, send, keep = att_back(mine, text_tokens, qkv, p, o, dx, g1, txt_qkv, txt_out)
    grad_out, grad_qkv = simple(
        spread_att_kernel, [((D, D), F32), ((D, 3 * D), F32)], [pltpu.VMEM((1536, D), F32)], smem=1, name="spread_att"
    )(mine, *net.all_sum(send, keep, 48))
    small = net.total(jnp.concatenate([gain1, gain2, part], 1))
    return (
        small[0, 768:769], grad_tokens, small[0, 0:384], grad_qkv, grad_out, small[0, 384:768],
        grad_up, grad_down, grad_proj, small[0, 769:770],
    )


def column_total(net, sums):
    v = sums.reshape(32, CAPS)
    for mask, bit in ((1, 16), (2, 4), (4, 8), (8, 1), (16, 2)):
        other = net.swap(v, mask)
        other = other.reshape(32 // (2 * bit), 2, bit, CAPS)[:, ::-1].reshape(32, CAPS)
        v = v + other
    return v.reshape(1, 32 * CAPS)


def solution(mesh):
    both = ("dp", "replica")
    devices = mesh.shape["dp"] * mesh.shape["replica"]
    tuned = (mesh.shape["dp"], mesh.shape["replica"]) == (8, 4)
    rows = P(both, None)
    return jax.shard_map(
        functools.partial(shards, devices, tuned),
        mesh=mesh,
        in_specs=(rows, rows, P(both), P(both, None, None)) + (P(),) * 15,
        out_specs=(P(), rows) + (P(),) * 8,
        check_vma=False,
    )
```

```python
import functools
import math

import jax
import jax.numpy as jnp
from jax import lax
from jax.experimental import pallas as pl
from jax.experimental.pallas import tpu as pltpu
from jax.sharding import PartitionSpec as P

D = 384
HEADS = 6
HEAD = 64
FF = 1536
IMG_LEN = 50
PACK = 4
CAPS = 64
TOK_BLOCK = 256
CAP_BLOCK = 16
BLOCKS = 4
PAIR = 128
IMG_BLOCK = 16
IMG_ROWS = IMG_BLOCK * IMG_LEN
EPS = 1e-06

BF = jnp.bfloat16
F32 = jnp.float32
GELU_K = math.sqrt(2.0 / math.pi)
GELU_C = 0.044715


def mm(a, b):
    return lax.dot_general(a, b, (((1,), (0,)), ((), ())), preferred_element_type=F32)


def mm_nt(a, b):
    return lax.dot_general(a, b, (((1,), (1,)), ((), ())), preferred_element_type=F32)


def mm_tn(a, b):
    return lax.dot_general(a, b, (((0,), (0,)), ((), ())), preferred_element_type=F32)


def row_mean(v):
    return jnp.sum(v, -1, keepdims=True) * (1.0 / D)


def normalize(v):
    centre = v - row_mean(v)
    return centre * lax.rsqrt(row_mean(centre * centre) + EPS)


def split3(v):
    high = v.astype(BF)
    rest = v - high.astype(F32)
    mid = rest.astype(BF)
    low = (rest - mid.astype(F32)).astype(BF)
    return high, mid, low


def wide_mm(v, w):
    high, mid, low = split3(v)
    n = v.shape[0]
    out = mm(jnp.concatenate([high, mid, low], 0), w)
    return out[:n] + out[n : 2 * n] + out[2 * n :]


def gelu_parts(z):
    z2 = z * z
    t = jnp.tanh(z * (z2 * (GELU_K * GELU_C) + GELU_K))
    hp = t * 0.5 + 0.5
    u = z * hp
    slope = hp + (u * (1.0 - hp)) * (z2 * (6.0 * GELU_K * GELU_C) + 2.0 * GELU_K)
    return u, slope


def lanes_head(shape):
    return lax.broadcasted_iota(jnp.int32, shape, len(shape) - 1) // HEAD


def image_kernel(x_ref, g1, wqkv, wout, g2, wup, wdown, wproj, emb_ref, kv, x0, att):
    step = pl.program_id(0)
    gain = g1[...].reshape(1, D)
    for c in range(2):
        x = x_ref[IMG_LEN // 2 * c : IMG_LEN // 2 * (c + 1)].astype(F32).reshape(IMG_ROWS // 2, D)
        h = (normalize(x) * gain).astype(BF)
        kv[IMG_ROWS // 2 * c : IMG_ROWS // 2 * (c + 1), :] = mm(h, wqkv[:, D:]).astype(BF)
        if c == 0:
            x0[pl.ds(pl.multiple_of(step * IMG_BLOCK, IMG_BLOCK), IMG_BLOCK), :] = x[:IMG_BLOCK]
            h0 = h[:IMG_BLOCK]
    q = mm(h0, wqkv[:, :D]).astype(BF).astype(F32) * (HEAD**-0.5)
    head = lanes_head((IMG_BLOCK, D))
    queries = HEADS * IMG_BLOCK
    rows = lax.broadcasted_iota(jnp.int32, (queries, IMG_ROWS), 0)
    cols = lax.broadcasted_iota(jnp.int32, (queries, IMG_ROWS), 1)
    own = cols % IMG_BLOCK == rows % IMG_BLOCK
    q6 = jnp.concatenate([jnp.where(head == h, q, 0.0) for h in range(HEADS)], 0)
    s = mm_nt(q6.astype(BF), kv[:, :D])
    s = jnp.where(own, s, -1e30)
    e = jnp.exp(s - jnp.max(s, -1, keepdims=True))
    p = (e * (1.0 / jnp.sum(e, -1, keepdims=True))).astype(BF)
    r = mm(p, kv[:, D:])
    o = jnp.where(head == 0, r[0:IMG_BLOCK], 0.0)
    for h in range(1, HEADS):
        o = jnp.where(head == h, r[IMG_BLOCK * h : IMG_BLOCK * (h + 1)], o)
    att[pl.ds(pl.multiple_of(step * IMG_BLOCK, IMG_BLOCK), IMG_BLOCK), :] = o

    @pl.when(step == pl.num_programs(0) - 1)
    def _():
        x1 = x0[...] + mm(att[...].astype(BF), wout[...])
        h2 = (normalize(x1) * g2[...].reshape(1, D)).astype(BF)
        u, _ = gelu_parts(mm(h2, wup[...]))
        y = x1 + mm(u.astype(BF), wdown[...])
        e = mm(y.astype(BF), wproj[...])
        emb_ref[...] = (e * lax.rsqrt(jnp.sum(e * e, -1, keepdims=True) + EPS)).astype(BF)


def cost(us):
    return pl.CostEstimate(flops=int(us * 1e9), bytes_accessed=int(us * 3e6), transcendentals=0)


def const_spec(shape):
    zeros = (0,) * len(shape)
    return pl.BlockSpec(shape, lambda *_: zeros, pipeline_mode=pl.Buffered(1))


def image_tower(x, g1, wqkv, wout, g2, wup, wdown, wproj):
    count = x.shape[1]
    return pl.pallas_call(
        image_kernel,
        grid=(count // IMG_BLOCK,),
        in_specs=[
            pl.BlockSpec((IMG_LEN, IMG_BLOCK, D), lambda i: (0, i, 0)),
            const_spec((D,)),
            const_spec((D, 3 * D)),
            const_spec((D, D)),
            const_spec((D,)),
            const_spec((D, FF)),
            const_spec((FF, D)),
            const_spec((D, D)),
        ],
        out_specs=pl.BlockSpec((count, D), lambda i: (0, 0)),
        out_shape=jax.ShapeDtypeStruct((count, D), BF),
        scratch_shapes=[
            pltpu.VMEM((IMG_ROWS, 2 * D), BF),
            pltpu.VMEM((count, D), F32),
            pltpu.VMEM((count, D), F32),
        ],
        cost_estimate=cost(12),
        name="image_tower",
    )(x, g1, wqkv, wout, g2, wup, wdown, wproj)


def pair_mask(lab_ref, pair):
    lab = lab_ref[0, :, PAIR * pair : PAIR * pair + PAIR].astype(F32)
    wide = jnp.broadcast_to(lab, (PAIR, PAIR))
    return wide == wide.T


def text_att_kernel(tok_ref, lab_ref, g1, wqkv, o_ref, qkv_ref, p_ref, h1_ref):
    x = tok_ref[...].astype(F32)
    h1 = (normalize(x) * g1[...].reshape(1, D)).astype(BF)
    h1_ref[...] = h1
    qkv = mm(h1, wqkv[...]).astype(BF)
    qkv_ref[...] = qkv
    low = lax.broadcasted_iota(jnp.int32, (PAIR, PAIR), 1) < HEAD
    for pair in range(2):
        rows = slice(PAIR * pair, PAIR * pair + PAIR)
        mask = pair_mask(lab_ref, pair)
        mask = jnp.concatenate([mask, mask], 0)
        for j in range(HEADS // 2):
            cols = slice(PAIR * j, PAIR * j + PAIR)
            q2 = qkv[rows, PAIR * j : PAIR * j + PAIR] * jnp.asarray(HEAD**-0.5, BF)
            k2 = qkv[rows, D + PAIR * j : D + PAIR * j + PAIR]
            v2 = qkv[rows, 2 * D + PAIR * j : 2 * D + PAIR * j + PAIR]
            zero = jnp.zeros_like(q2)
            q22 = jnp.concatenate([jnp.where(low, q2, zero), jnp.where(low, zero, q2)], 0)
            s = jnp.where(mask, mm_nt(q22, k2), -1e30)
            ex = jnp.exp(s - jnp.max(s, -1, keepdims=True))
            p = (ex * (1.0 / jnp.sum(ex, -1, keepdims=True))).astype(BF)
            p_ref[pair, j] = p
            v22 = jnp.concatenate([jnp.where(low, v2, zero), jnp.where(low, zero, v2)], 0)
            o = mm(jnp.concatenate([p[:PAIR], p[PAIR:]], 1), v22)
            o_ref[rows, cols] = o.astype(BF)


def text_mlp_kernel(
    tok_ref, o_ref, lab_ref, wout, g2, wup, wdown, wproj,
    h2_ref, c2_ref, gp_ref, pu_ref, pb_ref, e_ref, emb_ref, cnt_ref, pt, po,
):
    step = pl.program_id(0)
    tok = tok_ref[...]
    o = o_ref[...]
    x1 = tok.astype(F32) + mm(o, wout[...])
    c2 = x1 - row_mean(x1)
    c2_ref[...] = c2
    h2 = (c2 * lax.rsqrt(row_mean(c2 * c2) + EPS) * g2[...].reshape(1, D)).astype(BF)
    h2_ref[...] = h2
    hit = lax.broadcasted_iota(jnp.int32, (CAP_BLOCK, TOK_BLOCK), 0) == lab_ref[0]
    member = jnp.where(hit, 1.0, 0.0)
    caps = pl.ds(pl.multiple_of(step * CAP_BLOCK, CAP_BLOCK), CAP_BLOCK)
    member_b = member.astype(BF)
    pt[caps, :] = mm(member_b, tok)
    po[caps, :] = mm(member_b, o)
    cnt_ref[caps, :] = jnp.broadcast_to(jnp.sum(member, -1, keepdims=True), (CAP_BLOCK, 128))
    for k in range(FF // 512):
        cols = slice(512 * k, 512 * (k + 1))
        u, slope = gelu_parts(mm(h2, wup[:, cols]))
        gp_ref[:, cols] = slope.astype(BF)
        pu_ref[caps, cols] = mm(member_b, u.astype(BF))

    @pl.when(step == pl.num_programs(0) - 1)
    def _():
        total = pt[...] + wide_mm(po[...], wout[...]) + wide_mm(pu_ref[...], wdown[...])
        pooled = (total * (1.0 / cnt_ref[:, 0:1])).astype(BF)
        pb_ref[...] = pooled
        e = mm(pooled, wproj[...])
        e_ref[...] = e
        emb_ref[...] = (e * lax.rsqrt(jnp.sum(e * e, -1, keepdims=True) + EPS)).astype(BF)


def token_rows(width):
    return pl.BlockSpec((TOK_BLOCK, width), lambda i: (i, 0))


def block_of(a, b):
    return pl.BlockSpec((1, a, b), lambda i: (i, 0, 0))


def whole(a, b):
    return pl.BlockSpec((a, b), lambda i: (0, 0))


def text_att(tok, lab, g1, wqkv):
    n = tok.shape[0]
    blocks = n // TOK_BLOCK
    shape = jax.ShapeDtypeStruct
    return pl.pallas_call(
        text_att_kernel,
        grid=(blocks,),
        in_specs=[token_rows(D), block_of(1, TOK_BLOCK), const_spec((D,)), const_spec((D, 3 * D))],
        out_specs=[
            token_rows(D),
            token_rows(3 * D),
            pl.BlockSpec((2, 3, 2 * PAIR, PAIR), lambda i: (i, 0, 0, 0)),
            token_rows(D),
        ],
        out_shape=[
            shape((n, D), BF), shape((n, 3 * D), BF), shape((2 * blocks, 3, 2 * PAIR, PAIR), BF), shape((n, D), BF),
        ],
        cost_estimate=cost(9),
        name="text_att",
    )(tok, lab, g1, wqkv)


def text_mlp(tok, o, lab, wout, g2, wup, wdown, wproj):
    n = tok.shape[0]
    shape = jax.ShapeDtypeStruct
    return pl.pallas_call(
        text_mlp_kernel,
        grid=(n // TOK_BLOCK,),
        in_specs=[
            token_rows(D), token_rows(D), block_of(1, TOK_BLOCK),
            const_spec((D, D)), const_spec((D,)), const_spec((D, FF)), const_spec((FF, D)), const_spec((D, D)),
        ],
        out_specs=[
            token_rows(D), token_rows(D), token_rows(FF),
            whole(CAPS, FF), whole(CAPS, D), whole(CAPS, D), whole(CAPS, D), whole(CAPS, 128),
        ],
        out_shape=[
            shape((n, D), BF), shape((n, D), F32), shape((n, FF), BF),
            shape((CAPS, FF), F32), shape((CAPS, D), BF), shape((CAPS, D), F32),
            shape((CAPS, D), BF), shape((CAPS, 128), F32),
        ],
        scratch_shapes=[pltpu.VMEM((CAPS, D), F32), pltpu.VMEM((CAPS, D), F32)],
        cost_estimate=cost(11),
        name="text_mlp",
    )(tok, o, lab, wout, g2, wup, wdown, wproj)


def reorder(mine, row):
    return jnp.where(mine & 1 == 1, pltpu.roll(row, 64, 1), row)


def cosine_kernel(denom, scale_ref, mine_ref, emb, images, pair, g_ref, sum_ref):
    mine = mine_ref[0]
    scale = jnp.exp(jnp.full((1, 1), scale_ref[0], F32))
    g = mm_nt(emb[...], images[...])
    g_ref[...] = g
    e = jnp.exp(g * scale)
    eg = e * g
    total = jnp.sum(e, -1, keepdims=True)
    hit = lax.broadcasted_iota(jnp.int32, g.shape, 1) == pair[...]
    own = jnp.sum(jnp.where(hit, g, 0.0), -1, keepdims=True)
    loss = jnp.sum(jnp.log(total) - 2.0 * scale * own, 0, keepdims=True)
    temp = jnp.sum(jnp.sum(eg, -1, keepdims=True) / total - 2.0 * own, 0, keepdims=True)
    n = g.shape[1] // 128
    for k, v in enumerate((jnp.sum(e, 0, keepdims=True), jnp.sum(eg, 0, keepdims=True))):
        for r in range(n):
            sum_ref[pl.ds(k * n + ((mine >> 1) ^ r), 1), :] = reorder(mine, v[:, 128 * r : 128 * (r + 1)])
    lane = lax.broadcasted_iota(jnp.int32, (8, 128), 1)
    sum_ref[2 * n :, :] = jnp.where(lane == 0, loss, jnp.where(lane == 1, temp, 0.0))


def rows_kernel(denom, scale_ref, g_ref, images, pair, dt_ref):
    scale = jnp.exp(jnp.full((1, 1), scale_ref[0], F32))
    g = g_ref[...]
    e = jnp.exp(g * scale)
    hit = lax.broadcasted_iota(jnp.int32, g.shape, 1) == pair[...]
    p = e * (1.0 / jnp.sum(e, -1, keepdims=True))
    dl = jnp.where(hit, p - 2.0, p) * (scale * (1.0 / denom))
    dt_ref[...] = mm(dl.astype(BF), images[...])


def halves(place, rows, send_ref, keep_ref, pieces):
    for rel in range(8):
        ref = keep_ref if rel < 4 else send_ref
        at = (rel % 4) * rows
        for v in pieces(place ^ rel):
            ref[at : at + v.shape[0], :] = v.astype(BF)
            at += v.shape[0]


def block(acc, at, rows, col=0):
    return acc[pl.ds(pl.multiple_of(at * rows, 16), rows), D * col : D * (col + 1)]


def head_kernel(
    denom, scale_ref, mine_ref, g_ref, images, sums, dt_row, e_ref, pb, cnt, pu, wproj, wdown,
    sd_ref, kd_ref, sp_ref, kp_ref, du_ref, dy_ref, loss_out, temp_out, down, proj,
):
    mine = mine_ref[0]
    scale = jnp.exp(jnp.full((1, 1), scale_ref[0], F32))
    n = g_ref.shape[1] // 128

    def columns(k):
        return jnp.concatenate([reorder(mine, sums[pl.ds(k * n + ((mine >> 1) ^ r), 1), :]) for r in range(n)], 1)

    temp = jnp.sum(jnp.sum(sums[n : 2 * n, :] / sums[0:n, :], 0, keepdims=True), -1, keepdims=True)
    loss = jnp.sum(jnp.sum(jnp.log(sums[0:n, :]), 0, keepdims=True), -1, keepdims=True)
    loss_out[...] = (sums[2 * n : 2 * n + 1, 0:1] + loss) * (1.0 / denom)
    temp_out[...] = (sums[2 * n : 2 * n + 1, 1:2] + temp) * (scale * (1.0 / denom))
    inverse = 1.0 / columns(0)
    dl = jnp.exp(g_ref[...] * scale) * (inverse * (scale * (1.0 / denom)))
    dt = dt_row[...] + mm(dl.astype(BF), images[...])
    e = e_ref[...]
    r = lax.rsqrt(jnp.sum(e * e, -1, keepdims=True) + EPS)
    de = (dt - e * (r * r * jnp.sum(dt * e, -1, keepdims=True))) * r
    de = de.astype(BF)
    dpooled = mm_nt(de, wproj[...])
    dy = dpooled * (1.0 / cnt[:, 0:1])
    dyb = dy.astype(BF)
    du = mm_nt(dyb, wdown[...])
    for i, piece in enumerate(split3(du)):
        for b in range(BLOCKS):
            du_ref[b, CAP_BLOCK * i : CAP_BLOCK * (i + 1), :] = piece[CAP_BLOCK * b : CAP_BLOCK * (b + 1)]
    for i, piece in enumerate(split3(dy)):
        for b in range(BLOCKS):
            dy_ref[b, CAP_BLOCK * i : CAP_BLOCK * (i + 1), :] = piece[CAP_BLOCK * b : CAP_BLOCK * (b + 1)]
    down[...] = mm_tn(jnp.concatenate(split3(pu[...]), 0), jnp.concatenate([dyb, dyb, dyb], 0))
    proj[...] = mm_tn(pb[...], de)
    halves(mine >> 2, 192, sd_ref, kd_ref, lambda at: [block(down, at, 192)])
    halves(mine >> 2, 48, sp_ref, kp_ref, lambda at: [block(proj, at, 48)])


def mlp_back_kernel(
    mine_ref, lab_ref, h2_ref, gp_ref, c2_ref, du_ref, dy_ref, g2, wup,
    dx_ref, dxb_ref, send_ref, keep_ref, acc,
):
    step = pl.program_id(0)

    @pl.when(step == 0)
    def _():
        acc[...] = jnp.zeros_like(acc)

    hit = lax.broadcasted_iota(jnp.int32, (3 * CAP_BLOCK, TOK_BLOCK), 0) % CAP_BLOCK == lab_ref[0]
    spread = jnp.where(hit, 1.0, 0.0).astype(BF)
    du = mm_tn(spread, du_ref[0])
    dz = (du * gp_ref[...].astype(F32)).astype(BF)
    dy = mm_tn(spread, dy_ref[0])
    dh = mm_nt(dz, wup[...])
    c2 = c2_ref[...]
    r = lax.rsqrt(row_mean(c2 * c2) + EPS)
    unit = c2 * r
    dn = dh * g2[...].reshape(1, D)
    dx = dy + r * (dn - row_mean(dn) - unit * row_mean(dn * unit))
    dx_ref[...] = dx
    dxb_ref[...] = dx.astype(BF)
    h2 = h2_ref[...]
    acc[...] += mm_tn(h2, dz)

    @pl.when(step == pl.num_programs(0) - 1)
    def _():
        halves(mine_ref[0] >> 2, 192, send_ref, keep_ref, lambda at: [block(acc, at, 48, k) for k in range(4)])


def att_core_kernel(qkv_ref, p_ref, dxb_ref, wout, dqkv_ref):
    do = mm_nt(dxb_ref[...], wout[...]).astype(BF)
    low = lax.broadcasted_iota(jnp.int32, (PAIR, PAIR), 1) < HEAD
    zero = jnp.zeros((PAIR, PAIR), BF)
    half = HEAD**-0.5

    def twice(v):
        return jnp.concatenate([jnp.where(low, v, zero), jnp.where(low, zero, v)], 0)

    for pair in range(2):
        rows = slice(PAIR * pair, PAIR * pair + PAIR)
        for j in range(HEADS // 2):
            cols = slice(PAIR * j, PAIR * j + PAIR)
            q2 = qkv_ref[rows, PAIR * j : PAIR * j + PAIR]
            k2 = qkv_ref[rows, D + PAIR * j : D + PAIR * j + PAIR]
            v2 = qkv_ref[rows, 2 * D + PAIR * j : 2 * D + PAIR * j + PAIR]
            do2 = twice(do[rows, cols])
            pb = p_ref[pair, j]
            p = pb.astype(F32)
            dp = mm_nt(do2, v2)
            ds = (p * (dp - jnp.sum(dp * p, -1, keepdims=True))).astype(BF)
            dq = mm(jnp.concatenate([ds[:PAIR], ds[PAIR:]], 1), twice(k2)) * half
            dk = mm_tn(ds, twice(q2)) * half
            dv = mm_tn(pb, do2)
            dqkv_ref[rows, PAIR * j : PAIR * j + PAIR] = dq.astype(BF)
            dqkv_ref[rows, D + PAIR * j : D + PAIR * j + PAIR] = dk.astype(BF)
            dqkv_ref[rows, 2 * D + PAIR * j : 2 * D + PAIR * j + PAIR] = dv.astype(BF)


def att_grads_kernel(mine_ref, h1_ref, dqkv_ref, o_ref, dxb_ref, send_ref, keep_ref, acc, out):
    step = pl.program_id(0)

    @pl.when(step == 0)
    def _():
        acc[...] = jnp.zeros_like(acc)
        out[...] = jnp.zeros_like(out)

    out[...] += mm_tn(o_ref[...], dxb_ref[...])
    acc[...] += mm_tn(h1_ref[...], dqkv_ref[...])

    @pl.when(step == pl.num_programs(0) - 1)
    def _():
        def pieces(at):
            return [block(out, at, 48)] + [block(acc, at, 48, k) for k in range(3)]

        halves(mine_ref[0] >> 2, 192, send_ref, keep_ref, pieces)


def tok_back_kernel(tok_ref, dqkv_ref, dx_ref, g1, wqkv, gtok_ref):
    x = tok_ref[...].astype(F32)
    centre = x - row_mean(x)
    r = lax.rsqrt(row_mean(centre * centre) + EPS)
    unit = centre * r
    dn = mm_nt(dqkv_ref[...], wqkv[...]) * g1[...].reshape(1, D)
    gtok_ref[...] = dx_ref[...] + r * (dn - row_mean(dn) - unit * row_mean(dn * unit))


def gain_of(grad, weight, gain):
    high, mid, _ = split3(grad * weight.astype(F32))
    ones = jnp.ones((8, grad.shape[1]), BF)
    total = mm_nt(ones, high) + mm_nt(ones, mid)
    return total[0:1] / gain.reshape(1, D)


def arrived(mine_ref, own, other, rows):
    for rel in range(8):
        src = own if rel < 4 else other
        yield (mine_ref[0] >> 2) ^ rel, src, (rel % 4) * rows


def spread_mlp_kernel(mine_ref, own, other, wup, g2, down_ref, up_ref, gain_ref):
    for at, src, row in arrived(mine_ref, own, other, 384):
        down_ref[pl.ds(pl.multiple_of(at * 192, 64), 192), :] = src[row : row + 192, :].astype(F32)
        rows = pl.ds(pl.multiple_of(at * 48, 16), 48)
        for k in range(4):
            up_ref[rows, D * k : D * (k + 1)] = src[row + 192 + 48 * k : row + 240 + 48 * k, :].astype(F32)
    gain_ref[...] = gain_of(up_ref[...], wup[...], g2[...])


def spread_att_kernel(mine_ref, own, other, wqkv, g1, out_ref, qkv_ref, proj_ref, gain_ref):
    for at, src, row in arrived(mine_ref, own, other, 240):
        rows = pl.ds(pl.multiple_of(at * 48, 16), 48)
        out_ref[rows, :] = src[row : row + 48, :].astype(F32)
        for k in range(3):
            qkv_ref[rows, D * k : D * (k + 1)] = src[row + 48 + 48 * k : row + 96 + 48 * k, :].astype(F32)
        proj_ref[rows, :] = src[row + 192 : row + 240, :].astype(F32)
    gain_ref[...] = gain_of(qkv_ref[...], wqkv[...], g1[...])


SMEM = pl.BlockSpec(memory_space=pltpu.SMEM)
VMEM = pl.BlockSpec(memory_space=pltpu.VMEM)


def simple(kernel, outs, scratch=(), smem=0, us=3, name=None):
    def call(*args):
        return pl.pallas_call(
            kernel,
            in_specs=[SMEM] * smem + [VMEM] * (len(args) - smem),
            out_specs=[VMEM] * len(outs),
            out_shape=[jax.ShapeDtypeStruct(s, t) for s, t in outs],
            scratch_shapes=list(scratch),
            cost_estimate=cost(us),
            name=name,
        )(*args)

    return call


def mlp_back(mine, lab, h2, gp, c2, du, dy, g2, wup):
    n = h2.shape[0]

    def rows(width):
        return pl.BlockSpec((TOK_BLOCK, width), lambda i: (i, 0))

    def blk(a, b):
        return pl.BlockSpec((1, a, b), lambda i: (i, 0, 0))

    shape = jax.ShapeDtypeStruct
    return pl.pallas_call(
        mlp_back_kernel,
        grid=(n // TOK_BLOCK,),
        in_specs=[
            SMEM, blk(1, TOK_BLOCK), rows(D), rows(FF), rows(D), blk(3 * CAP_BLOCK, FF), blk(3 * CAP_BLOCK, D),
            const_spec((D,)), const_spec((D, FF)),
        ],
        out_specs=[rows(D), rows(D)] + [pl.BlockSpec((768, D), lambda i: (0, 0))] * 2,
        out_shape=[shape((n, D), F32), shape((n, D), BF), shape((768, D), BF), shape((768, D), BF)],
        scratch_shapes=[pltpu.VMEM((D, FF), F32)],
        cost_estimate=cost(9),
        name="mlp_back",
    )(mine, lab, h2, gp, c2, du, dy, g2, wup)


def att_core(qkv, p, dxb, wout):
    n = dxb.shape[0]
    return pl.pallas_call(
        att_core_kernel,
        grid=(n // TOK_BLOCK,),
        in_specs=[
            token_rows(3 * D),
            pl.BlockSpec((2, 3, 2 * PAIR, PAIR), lambda i: (i, 0, 0, 0)),
            token_rows(D),
            const_spec((D, D)),
        ],
        out_specs=token_rows(3 * D),
        out_shape=jax.ShapeDtypeStruct((n, 3 * D), BF),
        cost_estimate=cost(10),
        name="att_core",
    )(qkv, p, dxb, wout)


def att_grads(mine, h1, dqkv, o, dxb):
    n = h1.shape[0]
    return pl.pallas_call(
        att_grads_kernel,
        grid=(n // TOK_BLOCK,),
        in_specs=[SMEM, token_rows(D), token_rows(3 * D), token_rows(D), token_rows(D)],
        out_specs=[whole(768, D)] * 2,
        out_shape=[jax.ShapeDtypeStruct((768, D), BF)] * 2,
        scratch_shapes=[pltpu.VMEM((D, 3 * D), F32), pltpu.VMEM((D, D), F32)],
        cost_estimate=cost(4),
        name="att_grads",
    )(mine, h1, dqkv, o, dxb)


def tok_back(tok, dqkv, dx, g1, wqkv):
    n = tok.shape[0]
    return pl.pallas_call(
        tok_back_kernel,
        grid=(n // TOK_BLOCK,),
        in_specs=[token_rows(D), token_rows(3 * D), token_rows(D), const_spec((D,)), const_spec((D, 3 * D))],
        out_specs=token_rows(D),
        out_shape=jax.ShapeDtypeStruct((n, D), F32),
        cost_estimate=cost(4),
        name="tok_back",
    )(tok, dqkv, dx, g1, wqkv)


AXES = ("dp", "replica")


def swap(v, mask):
    return lax.ppermute(v, AXES, [(i, i ^ mask) for i in range(32)])


def plane(parts):
    return [swap(parts[m], 2 * m) for m in (1, 2, 3)]


def column(parts):
    return [swap(parts[m], 8 * m) for m in (1, 2, 3)]


def added(own, got):
    total = own.astype(F32)
    for v in got:
        total = total + v.astype(F32)
    return total.astype(BF)


def joined(own, got):
    return jnp.concatenate([own] + got, 0)


def shards(
    devices, tuned,
    text_tokens, segment_ids, pair_index, image_tokens,
    img_ln1, img_qkv, img_out, img_ln2, img_up, img_down, img_proj,
    txt_ln1, txt_qkv, txt_out, txt_ln2, txt_up, txt_down, txt_proj, log_scale,
):
    total = CAPS * devices
    denom = 2.0 * total
    row_of = jnp.arange(segment_ids.shape[0], dtype=jnp.int32) % (TOK_BLOCK // segment_ids.shape[1])
    lab = (segment_ids + PACK * row_of[:, None]).reshape(BLOCKS, 1, TOK_BLOCK)
    pair = pair_index
    if tuned:
        index = lax.axis_index(AXES)
        mine = ((index & 1) * 16 + ((index >> 1) & 3) * 4 + (index >> 3)).astype(jnp.int32).reshape(1)
        owner, row = pair // CAPS, pair % CAPS
        pair = (((owner & 1) * 16 + ((owner >> 1) & 3) * 4 + (owner >> 3)) ^ mine) * CAPS + row
    else:
        mine = jnp.zeros((1,), jnp.int32)
    pair = pair.reshape(CAPS, 1)
    lab, pair = lax.optimization_barrier((lab, pair))
    emb = image_tower(
        jnp.transpose(image_tokens, (1, 0, 2)), img_ln1, img_qkv, img_out, img_ln2, img_up, img_down, img_proj
    )
    if tuned:
        near = joined(emb, column([emb] * 4))
        o, qkv, p, h1 = text_att(text_tokens, lab, txt_ln1, txt_qkv)
        o, near = lax.optimization_barrier((o, near))
        got = plane([near] * 4)
    else:
        o, qkv, p, h1 = text_att(text_tokens, lab, txt_ln1, txt_qkv)
    h2, c2, gp, pu, pb, e, temb, cnt = text_mlp(text_tokens, o, lab, txt_out, txt_ln2, txt_up, txt_down, txt_proj)
    if tuned:
        near, got, temb = lax.optimization_barrier((near, got, temb))
        near = joined(near, got)
        images = joined(near, [swap(near, 1)])
    else:
        images = lax.all_gather(emb, AXES, axis=0, tiled=True)
    lines = total // 128
    g, sums = simple(
        functools.partial(cosine_kernel, denom),
        [((CAPS, total), F32), ((2 * lines + 8, 128), F32)],
        smem=2,
        us=3,
        name="cosine",
    )(log_scale, mine, temb, images, pair)
    (dt_row,) = simple(functools.partial(rows_kernel, denom), [((CAPS, D), F32)], smem=1, us=2, name="rows")(
        log_scale, g, images, pair
    )
    if tuned:
        for mask in (1, 2, 4, 8, 16):
            sums = sums + swap(sums, mask)
    else:
        sums = lax.psum(sums, AXES)
    send_d, keep_d, send_p, keep_p, du, dy, loss, temp = simple(
        functools.partial(head_kernel, denom),
        [
            ((768, D), BF), ((768, D), BF), ((192, D), BF), ((192, D), BF),
            ((BLOCKS, 48, FF), BF), ((BLOCKS, 48, D), BF), ((1, 1), F32), ((1, 1), F32),
        ],
        [pltpu.VMEM((FF, D), F32), pltpu.VMEM((D, D), F32)],
        smem=2,
        us=5,
        name="head_back",
    )(log_scale, mine, g, images, sums, dt_row, e, pb, cnt, pu, txt_proj, txt_down)
    dx, dxb, send_u, keep_u = mlp_back(mine, lab, h2, gp, c2, du, dy, txt_ln2, txt_up)

    def mlp_parts(d, u):
        return jnp.concatenate([d.reshape(4, 192, D), u.reshape(4, 192, D)], 1)

    def att_parts(a, p):
        return jnp.concatenate([a.reshape(4, 192, D), p.reshape(4, 48, D)], 1)

    def spread_mlp(own, other):
        outs = [((FF, D), F32), ((D, FF), F32), ((1, D), F32)]
        return simple(spread_mlp_kernel, outs, smem=1, us=4, name="spread_mlp")(mine, own, other, txt_up, txt_ln2)

    def spread_att(own, other):
        outs = [((D, D), F32), ((D, 3 * D), F32), ((D, D), F32), ((1, D), F32)]
        return simple(spread_att_kernel, outs, smem=1, us=4, name="spread_att")(mine, own, other, txt_qkv, txt_ln1)

    if not tuned:
        dqkv = att_core(qkv, p, dxb, txt_out)
        send_a, keep_a = att_grads(mine, h1, dqkv, o, dxb)
        grad_tokens = tok_back(text_tokens, dqkv, dx, txt_ln1, txt_qkv)
        sums = [keep_d, send_d, keep_u, send_u, keep_a, send_a, keep_p, send_p]
        d, d2, u, u2, a, a2, p, p2 = [v.astype(BF) for v in lax.psum([v.astype(F32) for v in sums], AXES)]
        grad_down, grad_up, gain2 = spread_mlp(mlp_parts(d, u).reshape(1536, D), mlp_parts(d2, u2).reshape(1536, D))
        grad_out, grad_qkv, grad_proj, gain1 = spread_att(
            att_parts(a, p).reshape(960, D), att_parts(a2, p2).reshape(960, D)
        )
    else:
        d = added(keep_d, [swap(send_d, 1)])
        pr = added(keep_p, [swap(send_p, 1)])
        m = mlp_parts(d, added(keep_u, [swap(send_u, 1)]))
        dxb, m = lax.optimization_barrier((dxb, m))
        got = plane(m)
        dqkv = att_core(qkv, p, dxb, txt_out)
        got, dqkv = lax.optimization_barrier((got, dqkv))
        m = added(m[0], got)
        m, dqkv = lax.optimization_barrier((m, dqkv))
        other = swap(m, 16)
        send_a, keep_a = att_grads(mine, h1, dqkv, o, dxb)
        other, send_a, keep_a = lax.optimization_barrier((other, send_a, keep_a))
        a = att_parts(added(keep_a, [swap(send_a, 1)]), pr)
        a, dqkv = lax.optimization_barrier((a, dqkv))
        grad_tokens = tok_back(text_tokens, dqkv, dx, txt_ln1, txt_qkv)
        m = added(m, [other])
        m = added(m, [swap(m, 8)])
        a = added(a[0], plane(a))
        a = added(a, [swap(a, 16)])
        m = joined(m, plane([m] * 4))
        a = added(a, [swap(a, 8)])
        grad_down, grad_up, gain2 = spread_mlp(m, swap(m, 1))
        got = plane([a] * 4)
        got, grad_up = lax.optimization_barrier((got, grad_up))
        a = joined(a, got)
        grad_out, grad_qkv, grad_proj, gain1 = spread_att(a, swap(a, 1))
    return (
        loss.reshape(1), grad_tokens, gain1.reshape(D), grad_qkv, grad_out, gain2.reshape(D),
        grad_up, grad_down, grad_proj, temp.reshape(1),
    )


def solution(mesh):
    both = ("dp", "replica")
    devices = mesh.shape["dp"] * mesh.shape["replica"]
    tuned = (mesh.shape["dp"], mesh.shape["replica"]) == (8, 4)
    rows = P(both, None)
    return jax.shard_map(
        functools.partial(shards, devices, tuned),
        mesh=mesh,
        in_specs=(rows, rows, P(both), P(both, None, None)) + (P(),) * 15,
        out_specs=(P(), rows) + (P(),) * 8,
        check_vma=False,
    )
```

```python
import functools
import math

import jax
import jax.numpy as jnp
from jax import lax
from jax.experimental import pallas as pl
from jax.experimental.pallas import tpu as pltpu
from jax.sharding import PartitionSpec as P

D = 384
HEADS = 6
HEAD = 64
FF = 1536
IMG_LEN = 50
PACK = 4
CAPS = 64
TOK_BLOCK = 256
CAP_BLOCK = 16
BLOCKS = 4
PAIR = 128
IMG_BLOCK = 16
IMG_ROWS = IMG_BLOCK * IMG_LEN
EPS = 1e-06

BF = jnp.bfloat16
F32 = jnp.float32
GELU_K = math.sqrt(2.0 / math.pi)
GELU_C = 0.044715


def mm(a, b):
    return lax.dot_general(a, b, (((1,), (0,)), ((), ())), preferred_element_type=F32)


def mm_nt(a, b):
    return lax.dot_general(a, b, (((1,), (1,)), ((), ())), preferred_element_type=F32)


def mm_tn(a, b):
    return lax.dot_general(a, b, (((0,), (0,)), ((), ())), preferred_element_type=F32)


def row_mean(v):
    return jnp.sum(v, -1, keepdims=True) * (1.0 / D)


def normalize(v):
    centre = v - row_mean(v)
    return centre * lax.rsqrt(row_mean(centre * centre) + EPS)


def split3(v):
    high = v.astype(BF)
    rest = v - high.astype(F32)
    mid = rest.astype(BF)
    low = (rest - mid.astype(F32)).astype(BF)
    return high, mid, low


def wide_mm(v, w):
    high, mid, low = split3(v)
    n = v.shape[0]
    out = mm(jnp.concatenate([high, mid, low], 0), w)
    return out[:n] + out[n : 2 * n] + out[2 * n :]


def gelu_parts(z):
    z2 = z * z
    t = jnp.tanh(z * (z2 * (GELU_K * GELU_C) + GELU_K))
    hp = t * 0.5 + 0.5
    u = z * hp
    slope = hp + (u * (1.0 - hp)) * (z2 * (6.0 * GELU_K * GELU_C) + 2.0 * GELU_K)
    return u, slope


def lanes_head(shape):
    return lax.broadcasted_iota(jnp.int32, shape, len(shape) - 1) // HEAD


def image_kernel(x_ref, g1, wqkv, wout, g2, wup, wdown, wproj, emb_ref, kv, x0, att):
    step = pl.program_id(0)
    gain = g1[...].reshape(1, D)
    for c in range(2):
        x = x_ref[IMG_LEN // 2 * c : IMG_LEN // 2 * (c + 1)].astype(F32).reshape(IMG_ROWS // 2, D)
        h = (normalize(x) * gain).astype(BF)
        kv[IMG_ROWS // 2 * c : IMG_ROWS // 2 * (c + 1), :] = mm(h, wqkv[:, D:]).astype(BF)
        if c == 0:
            x0[pl.ds(pl.multiple_of(step * IMG_BLOCK, IMG_BLOCK), IMG_BLOCK), :] = x[:IMG_BLOCK]
            h0 = h[:IMG_BLOCK]
    q = mm(h0, wqkv[:, :D]).astype(BF).astype(F32) * (HEAD**-0.5)
    head = lanes_head((IMG_BLOCK, D))
    queries = HEADS * IMG_BLOCK
    rows = lax.broadcasted_iota(jnp.int32, (queries, IMG_ROWS), 0)
    cols = lax.broadcasted_iota(jnp.int32, (queries, IMG_ROWS), 1)
    own = cols % IMG_BLOCK == rows % IMG_BLOCK
    q6 = jnp.concatenate([jnp.where(head == h, q, 0.0) for h in range(HEADS)], 0)
    s = mm_nt(q6.astype(BF), kv[:, :D])
    s = jnp.where(own, s, -1e30)
    e = jnp.exp(s - jnp.max(s, -1, keepdims=True))
    p = (e * (1.0 / jnp.sum(e, -1, keepdims=True))).astype(BF)
    r = mm(p, kv[:, D:])
    o = jnp.where(head == 0, r[0:IMG_BLOCK], 0.0)
    for h in range(1, HEADS):
        o = jnp.where(head == h, r[IMG_BLOCK * h : IMG_BLOCK * (h + 1)], o)
    att[pl.ds(pl.multiple_of(step * IMG_BLOCK, IMG_BLOCK), IMG_BLOCK), :] = o

    @pl.when(step == pl.num_programs(0) - 1)
    def _():
        x1 = x0[...] + mm(att[...].astype(BF), wout[...])
        h2 = (normalize(x1) * g2[...].reshape(1, D)).astype(BF)
        u, _ = gelu_parts(mm(h2, wup[...]))
        y = x1 + mm(u.astype(BF), wdown[...])
        e = mm(y.astype(BF), wproj[...])
        emb_ref[...] = (e * lax.rsqrt(jnp.sum(e * e, -1, keepdims=True) + EPS)).astype(BF)


def cost(us):
    return pl.CostEstimate(flops=int(us * 1e9), bytes_accessed=int(us * 3e6), transcendentals=0)


def const_spec(shape):
    zeros = (0,) * len(shape)
    return pl.BlockSpec(shape, lambda *_: zeros, pipeline_mode=pl.Buffered(1))


def image_tower(x, g1, wqkv, wout, g2, wup, wdown, wproj):
    count = x.shape[1]
    return pl.pallas_call(
        image_kernel,
        grid=(count // IMG_BLOCK,),
        in_specs=[
            pl.BlockSpec((IMG_LEN, IMG_BLOCK, D), lambda i: (0, i, 0)),
            const_spec((D,)),
            const_spec((D, 3 * D)),
            const_spec((D, D)),
            const_spec((D,)),
            const_spec((D, FF)),
            const_spec((FF, D)),
            const_spec((D, D)),
        ],
        out_specs=pl.BlockSpec((count, D), lambda i: (0, 0)),
        out_shape=jax.ShapeDtypeStruct((count, D), BF),
        scratch_shapes=[
            pltpu.VMEM((IMG_ROWS, 2 * D), BF),
            pltpu.VMEM((count, D), F32),
            pltpu.VMEM((count, D), F32),
        ],
        cost_estimate=cost(12),
        name="image_tower",
    )(x, g1, wqkv, wout, g2, wup, wdown, wproj)


def pair_mask(lab_ref, pair):
    lab = lab_ref[0, :, PAIR * pair : PAIR * pair + PAIR].astype(F32)
    wide = jnp.broadcast_to(lab, (PAIR, PAIR))
    return wide == wide.T


def text_att_kernel(tok_ref, lab_ref, g1, wqkv, o_ref, qkv_ref, p_ref, h1_ref):
    x = tok_ref[...].astype(F32)
    h1 = (normalize(x) * g1[...].reshape(1, D)).astype(BF)
    h1_ref[...] = h1
    qkv = mm(h1, wqkv[...]).astype(BF)
    qkv_ref[...] = qkv
    low = lax.broadcasted_iota(jnp.int32, (PAIR, PAIR), 1) < HEAD
    for pair in range(2):
        rows = slice(PAIR * pair, PAIR * pair + PAIR)
        mask = pair_mask(lab_ref, pair)
        mask = jnp.concatenate([mask, mask], 0)
        for j in range(HEADS // 2):
            cols = slice(PAIR * j, PAIR * j + PAIR)
            q2 = qkv[rows, PAIR * j : PAIR * j + PAIR] * jnp.asarray(HEAD**-0.5, BF)
            k2 = qkv[rows, D + PAIR * j : D + PAIR * j + PAIR]
            v2 = qkv[rows, 2 * D + PAIR * j : 2 * D + PAIR * j + PAIR]
            zero = jnp.zeros_like(q2)
            q22 = jnp.concatenate([jnp.where(low, q2, zero), jnp.where(low, zero, q2)], 0)
            s = jnp.where(mask, mm_nt(q22, k2), -1e30)
            ex = jnp.exp(s - jnp.max(s, -1, keepdims=True))
            p = (ex * (1.0 / jnp.sum(ex, -1, keepdims=True))).astype(BF)
            p_ref[pair, j] = p
            v22 = jnp.concatenate([jnp.where(low, v2, zero), jnp.where(low, zero, v2)], 0)
            o = mm(jnp.concatenate([p[:PAIR], p[PAIR:]], 1), v22)
            o_ref[rows, cols] = o.astype(BF)


def text_mlp_kernel(
    tok_ref, o_ref, lab_ref, wout, g2, wup, wdown, wproj,
    h2_ref, c2_ref, gp_ref, pu_ref, pb_ref, e_ref, emb_ref, cnt_ref, pt, po,
):
    step = pl.program_id(0)
    tok = tok_ref[...]
    o = o_ref[...]
    x1 = tok.astype(F32) + mm(o, wout[...])
    c2 = x1 - row_mean(x1)
    c2_ref[...] = c2
    h2 = (c2 * lax.rsqrt(row_mean(c2 * c2) + EPS) * g2[...].reshape(1, D)).astype(BF)
    h2_ref[...] = h2
    hit = lax.broadcasted_iota(jnp.int32, (CAP_BLOCK, TOK_BLOCK), 0) == lab_ref[0]
    member = jnp.where(hit, 1.0, 0.0)
    caps = pl.ds(pl.multiple_of(step * CAP_BLOCK, CAP_BLOCK), CAP_BLOCK)
    member_b = member.astype(BF)
    pt[caps, :] = mm(member_b, tok)
    po[caps, :] = mm(member_b, o)
    cnt_ref[caps, :] = jnp.broadcast_to(jnp.sum(member, -1, keepdims=True), (CAP_BLOCK, 128))
    for k in range(FF // 512):
        cols = slice(512 * k, 512 * (k + 1))
        u, slope = gelu_parts(mm(h2, wup[:, cols]))
        gp_ref[:, cols] = slope.astype(BF)
        pu_ref[caps, cols] = mm(member_b, u.astype(BF))

    @pl.when(step == pl.num_programs(0) - 1)
    def _():
        total = pt[...] + wide_mm(po[...], wout[...]) + wide_mm(pu_ref[...], wdown[...])
        pooled = (total * (1.0 / cnt_ref[:, 0:1])).astype(BF)
        pb_ref[...] = pooled
        e = mm(pooled, wproj[...])
        e_ref[...] = e
        emb_ref[...] = (e * lax.rsqrt(jnp.sum(e * e, -1, keepdims=True) + EPS)).astype(BF)


def token_rows(width):
    return pl.BlockSpec((TOK_BLOCK, width), lambda i: (i, 0))


def block_of(a, b):
    return pl.BlockSpec((1, a, b), lambda i: (i, 0, 0))


def whole(a, b):
    return pl.BlockSpec((a, b), lambda i: (0, 0))


def text_att(tok, lab, g1, wqkv):
    n = tok.shape[0]
    blocks = n // TOK_BLOCK
    shape = jax.ShapeDtypeStruct
    return pl.pallas_call(
        text_att_kernel,
        grid=(blocks,),
        in_specs=[token_rows(D), block_of(1, TOK_BLOCK), const_spec((D,)), const_spec((D, 3 * D))],
        out_specs=[
            token_rows(D),
            token_rows(3 * D),
            pl.BlockSpec((2, 3, 2 * PAIR, PAIR), lambda i: (i, 0, 0, 0)),
            token_rows(D),
        ],
        out_shape=[
            shape((n, D), BF), shape((n, 3 * D), BF), shape((2 * blocks, 3, 2 * PAIR, PAIR), BF), shape((n, D), BF),
        ],
        cost_estimate=cost(9),
        name="text_att",
    )(tok, lab, g1, wqkv)


def text_mlp(tok, o, lab, wout, g2, wup, wdown, wproj):
    n = tok.shape[0]
    shape = jax.ShapeDtypeStruct
    return pl.pallas_call(
        text_mlp_kernel,
        grid=(n // TOK_BLOCK,),
        in_specs=[
            token_rows(D), token_rows(D), block_of(1, TOK_BLOCK),
            const_spec((D, D)), const_spec((D,)), const_spec((D, FF)), const_spec((FF, D)), const_spec((D, D)),
        ],
        out_specs=[
            token_rows(D), token_rows(D), token_rows(FF),
            whole(CAPS, FF), whole(CAPS, D), whole(CAPS, D), whole(CAPS, D), whole(CAPS, 128),
        ],
        out_shape=[
            shape((n, D), BF), shape((n, D), F32), shape((n, FF), BF),
            shape((CAPS, FF), F32), shape((CAPS, D), BF), shape((CAPS, D), F32),
            shape((CAPS, D), BF), shape((CAPS, 128), F32),
        ],
        scratch_shapes=[pltpu.VMEM((CAPS, D), F32), pltpu.VMEM((CAPS, D), F32)],
        cost_estimate=cost(11),
        name="text_mlp",
    )(tok, o, lab, wout, g2, wup, wdown, wproj)


def reorder(mine, row):
    return jnp.where(mine & 1 == 1, pltpu.roll(row, 64, 1), row)


def cosine_kernel(denom, scale_ref, mine_ref, emb, images, pair, g_ref, sum_ref):
    mine = mine_ref[0]
    scale = jnp.exp(jnp.full((1, 1), scale_ref[0], F32))
    g = mm_nt(emb[...], images[...])
    g_ref[...] = g
    e = jnp.exp(g * scale)
    eg = e * g
    total = jnp.sum(e, -1, keepdims=True)
    hit = lax.broadcasted_iota(jnp.int32, g.shape, 1) == pair[...]
    own = jnp.sum(jnp.where(hit, g, 0.0), -1, keepdims=True)
    loss = jnp.sum(jnp.log(total) - 2.0 * scale * own, 0, keepdims=True)
    temp = jnp.sum(jnp.sum(eg, -1, keepdims=True) / total - 2.0 * own, 0, keepdims=True)
    n = g.shape[1] // 128
    for k, v in enumerate((jnp.sum(e, 0, keepdims=True), jnp.sum(eg, 0, keepdims=True))):
        for r in range(n):
            sum_ref[pl.ds(k * n + ((mine >> 1) ^ r), 1), :] = reorder(mine, v[:, 128 * r : 128 * (r + 1)])
    lane = lax.broadcasted_iota(jnp.int32, (8, 128), 1)
    sum_ref[2 * n :, :] = jnp.where(lane == 0, loss, jnp.where(lane == 1, temp, 0.0))


def rows_kernel(denom, scale_ref, g_ref, images, pair, dt_ref):
    scale = jnp.exp(jnp.full((1, 1), scale_ref[0], F32))
    g = g_ref[...]
    e = jnp.exp(g * scale)
    hit = lax.broadcasted_iota(jnp.int32, g.shape, 1) == pair[...]
    p = e * (1.0 / jnp.sum(e, -1, keepdims=True))
    dl = jnp.where(hit, p - 2.0, p) * (scale * (1.0 / denom))
    dt_ref[...] = mm(dl.astype(BF), images[...])


def quarter(mine, base, k, rows=48):
    far = (mine & 3) ^ k
    return pl.multiple_of(base + rows * ((far & 1) * 2 + (far >> 1)), 16)


def halves(mine, rows, send_ref, keep_ref, piece):
    for rel in range(8):
        ref = keep_ref if rel < 4 else send_ref
        at = (rel % 4) * rows
        if rows == 48:
            ref[at : at + 48, :] = piece((mine >> 2) ^ rel, 0).astype(BF)
            continue
        for k in range(4):
            ref[pl.ds(quarter(mine, at, k), 48), :] = piece((mine >> 2) ^ rel, k).astype(BF)


def block(acc, at, rows, col=0):
    return acc[pl.ds(pl.multiple_of(at * rows, 16), rows), D * col : D * (col + 1)]


def head_kernel(
    denom, scale_ref, mine_ref, g_ref, images, sums, dt_row, e_ref, pb, cnt, pu, wproj, wdown,
    sd_ref, kd_ref, sp_ref, kp_ref, du_ref, dy_ref, loss_out, temp_out, down, proj,
):
    mine = mine_ref[0]
    scale = jnp.exp(jnp.full((1, 1), scale_ref[0], F32))
    n = g_ref.shape[1] // 128

    def columns(k):
        return jnp.concatenate([reorder(mine, sums[pl.ds(k * n + ((mine >> 1) ^ r), 1), :]) for r in range(n)], 1)

    temp = jnp.sum(jnp.sum(sums[n : 2 * n, :] / sums[0:n, :], 0, keepdims=True), -1, keepdims=True)
    loss = jnp.sum(jnp.sum(jnp.log(sums[0:n, :]), 0, keepdims=True), -1, keepdims=True)
    loss_out[...] = (sums[2 * n : 2 * n + 1, 0:1] + loss) * (1.0 / denom)
    temp_out[...] = (sums[2 * n : 2 * n + 1, 1:2] + temp) * (scale * (1.0 / denom))
    inverse = 1.0 / columns(0)
    dl = jnp.exp(g_ref[...] * scale) * (inverse * (scale * (1.0 / denom)))
    dt = dt_row[...] + mm(dl.astype(BF), images[...])
    e = e_ref[...]
    r = lax.rsqrt(jnp.sum(e * e, -1, keepdims=True) + EPS)
    de = (dt - e * (r * r * jnp.sum(dt * e, -1, keepdims=True))) * r
    de = de.astype(BF)
    dpooled = mm_nt(de, wproj[...])
    dy = dpooled * (1.0 / cnt[:, 0:1])
    dyb = dy.astype(BF)
    du = mm_nt(dyb, wdown[...])
    for i, piece in enumerate(split3(du)):
        for b in range(BLOCKS):
            du_ref[b, CAP_BLOCK * i : CAP_BLOCK * (i + 1), :] = piece[CAP_BLOCK * b : CAP_BLOCK * (b + 1)]
    for i, piece in enumerate(split3(dy)):
        for b in range(BLOCKS):
            dy_ref[b, CAP_BLOCK * i : CAP_BLOCK * (i + 1), :] = piece[CAP_BLOCK * b : CAP_BLOCK * (b + 1)]
    down[...] = mm_tn(jnp.concatenate(split3(pu[...]), 0), jnp.concatenate([dyb, dyb, dyb], 0))
    proj[...] = mm_tn(pb[...], de)
    halves(mine, 192, sd_ref, kd_ref, lambda at, k: block(down, at * 4 + k, 48))
    halves(mine, 48, sp_ref, kp_ref, lambda at, k: block(proj, at, 48))


def mlp_back_kernel(
    mine_ref, lab_ref, h2_ref, gp_ref, c2_ref, du_ref, dy_ref, g2, wup,
    dx_ref, dxb_ref, send_ref, keep_ref, acc,
):
    step = pl.program_id(0)

    @pl.when(step == 0)
    def _():
        acc[...] = jnp.zeros_like(acc)

    hit = lax.broadcasted_iota(jnp.int32, (3 * CAP_BLOCK, TOK_BLOCK), 0) % CAP_BLOCK == lab_ref[0]
    spread = jnp.where(hit, 1.0, 0.0).astype(BF)
    du = mm_tn(spread, du_ref[0])
    dz = (du * gp_ref[...].astype(F32)).astype(BF)
    dy = mm_tn(spread, dy_ref[0])
    dh = mm_nt(dz, wup[...])
    c2 = c2_ref[...]
    r = lax.rsqrt(row_mean(c2 * c2) + EPS)
    unit = c2 * r
    dn = dh * g2[...].reshape(1, D)
    dx = dy + r * (dn - row_mean(dn) - unit * row_mean(dn * unit))
    dx_ref[...] = dx
    dxb_ref[...] = dx.astype(BF)
    h2 = h2_ref[...]
    acc[...] += mm_tn(h2, dz)

    @pl.when(step == pl.num_programs(0) - 1)
    def _():
        halves(mine_ref[0], 192, send_ref, keep_ref, lambda at, k: block(acc, at, 48, k))


def att_core_kernel(qkv_ref, p_ref, dxb_ref, wout, dqkv_ref):
    do = mm_nt(dxb_ref[...], wout[...]).astype(BF)
    low = lax.broadcasted_iota(jnp.int32, (PAIR, PAIR), 1) < HEAD
    zero = jnp.zeros((PAIR, PAIR), BF)
    half = HEAD**-0.5

    def twice(v):
        return jnp.concatenate([jnp.where(low, v, zero), jnp.where(low, zero, v)], 0)

    for pair in range(2):
        rows = slice(PAIR * pair, PAIR * pair + PAIR)
        for j in range(HEADS // 2):
            cols = slice(PAIR * j, PAIR * j + PAIR)
            q2 = qkv_ref[rows, PAIR * j : PAIR * j + PAIR]
            k2 = qkv_ref[rows, D + PAIR * j : D + PAIR * j + PAIR]
            v2 = qkv_ref[rows, 2 * D + PAIR * j : 2 * D + PAIR * j + PAIR]
            do2 = twice(do[rows, cols])
            pb = p_ref[pair, j]
            p = pb.astype(F32)
            dp = mm_nt(do2, v2)
            ds = (p * (dp - jnp.sum(dp * p, -1, keepdims=True))).astype(BF)
            dq = mm(jnp.concatenate([ds[:PAIR], ds[PAIR:]], 1), twice(k2)) * half
            dk = mm_tn(ds, twice(q2)) * half
            dv = mm_tn(pb, do2)
            dqkv_ref[rows, PAIR * j : PAIR * j + PAIR] = dq.astype(BF)
            dqkv_ref[rows, D + PAIR * j : D + PAIR * j + PAIR] = dk.astype(BF)
            dqkv_ref[rows, 2 * D + PAIR * j : 2 * D + PAIR * j + PAIR] = dv.astype(BF)


def att_grads_kernel(mine_ref, h1_ref, dqkv_ref, o_ref, dxb_ref, send_ref, keep_ref, acc):
    acc[:, :D] = mm_tn(o_ref[...], dxb_ref[...])
    acc[:, D:] = mm_tn(h1_ref[...], dqkv_ref[...])
    halves(mine_ref[0], 192, send_ref, keep_ref, lambda at, k: block(acc, at, 48, k))


def tok_back_kernel(tok_ref, dqkv_ref, dx_ref, g1, wqkv, gtok_ref):
    x = tok_ref[...].astype(F32)
    centre = x - row_mean(x)
    r = lax.rsqrt(row_mean(centre * centre) + EPS)
    unit = centre * r
    dn = mm_nt(dqkv_ref[...], wqkv[...]) * g1[...].reshape(1, D)
    gtok_ref[...] = dx_ref[...] + r * (dn - row_mean(dn) - unit * row_mean(dn * unit))


def gain_of(grad, weight, gain):
    high, mid, _ = split3(grad * weight.astype(F32))
    ones = jnp.ones((8, grad.shape[1]), BF)
    total = mm_nt(ones, high) + mm_nt(ones, mid)
    return total[0:1] / gain.reshape(1, D)


def arrived(mine_ref, own, other, rows):
    for rel in range(8):
        src = own if rel < 4 else other
        yield (mine_ref[0] >> 2) ^ rel, src, (rel % 4) * rows


def spread_mlp_kernel(mine_ref, own, other, wup, g2, down_ref, up_ref, proj_ref, gain_ref):
    for at, src, row in arrived(mine_ref, own, other, 432):
        rows = pl.ds(pl.multiple_of(at * 48, 16), 48)
        for k in range(4):
            part = quarter(mine_ref[0], row, k, 96)
            down_ref[pl.ds(pl.multiple_of(at * 192 + 48 * k, 16), 48), :] = src[pl.ds(part, 48), :].astype(F32)
            up_ref[rows, D * k : D * (k + 1)] = src[pl.ds(pl.multiple_of(part + 48, 16), 48), :].astype(F32)
        proj_ref[rows, :] = src[row + 384 : row + 432, :].astype(F32)
    gain_ref[...] = gain_of(up_ref[...], wup[...], g2[...]).reshape(D)


def spread_att_kernel(mine_ref, own, other, wqkv, g1, out_ref, qkv_ref, gain_ref):
    for at, src, row in arrived(mine_ref, own, other, 192):
        rows = pl.ds(pl.multiple_of(at * 48, 16), 48)
        out_ref[rows, :] = src[pl.ds(quarter(mine_ref[0], row, 0), 48), :].astype(F32)
        for k in range(3):
            qkv_ref[rows, D * k : D * (k + 1)] = src[pl.ds(quarter(mine_ref[0], row, k + 1), 48), :].astype(F32)
    gain_ref[...] = gain_of(qkv_ref[...], wqkv[...], g1[...]).reshape(D)


SMEM = pl.BlockSpec(memory_space=pltpu.SMEM)
VMEM = pl.BlockSpec(memory_space=pltpu.VMEM)


def simple(kernel, outs, scratch=(), smem=0, us=3, name=None):
    def call(*args):
        return pl.pallas_call(
            kernel,
            in_specs=[SMEM] * smem + [VMEM] * (len(args) - smem),
            out_specs=[VMEM] * len(outs),
            out_shape=[jax.ShapeDtypeStruct(s, t) for s, t in outs],
            scratch_shapes=list(scratch),
            cost_estimate=cost(us),
            name=name,
        )(*args)

    return call


def mlp_back(mine, lab, h2, gp, c2, du, dy, g2, wup):
    n = h2.shape[0]

    def rows(width):
        return pl.BlockSpec((TOK_BLOCK, width), lambda i: (i, 0))

    def blk(a, b):
        return pl.BlockSpec((1, a, b), lambda i: (i, 0, 0))

    shape = jax.ShapeDtypeStruct
    return pl.pallas_call(
        mlp_back_kernel,
        grid=(n // TOK_BLOCK,),
        in_specs=[
            SMEM, blk(1, TOK_BLOCK), rows(D), rows(FF), rows(D), blk(3 * CAP_BLOCK, FF), blk(3 * CAP_BLOCK, D),
            const_spec((D,)), const_spec((D, FF)),
        ],
        out_specs=[rows(D), rows(D)] + [pl.BlockSpec((768, D), lambda i: (0, 0))] * 2,
        out_shape=[shape((n, D), F32), shape((n, D), BF), shape((768, D), BF), shape((768, D), BF)],
        scratch_shapes=[pltpu.VMEM((D, FF), F32)],
        cost_estimate=cost(9),
        name="mlp_back",
    )(mine, lab, h2, gp, c2, du, dy, g2, wup)


def att_core(qkv, p, dxb, wout):
    n = dxb.shape[0]
    return pl.pallas_call(
        att_core_kernel,
        grid=(n // TOK_BLOCK,),
        in_specs=[
            token_rows(3 * D),
            pl.BlockSpec((2, 3, 2 * PAIR, PAIR), lambda i: (i, 0, 0, 0)),
            token_rows(D),
            const_spec((D, D)),
        ],
        out_specs=token_rows(3 * D),
        out_shape=jax.ShapeDtypeStruct((n, 3 * D), BF),
        cost_estimate=cost(10),
        name="att_core",
    )(qkv, p, dxb, wout)


def att_grads(mine, h1, dqkv, o, dxb):
    outs = [((768, D), BF)] * 2
    scratch = [pltpu.VMEM((D, 4 * D), F32)]
    return simple(att_grads_kernel, outs, scratch, smem=1, us=4, name="att_grads")(mine, h1, dqkv, o, dxb)


def tok_back(tok, dqkv, dx, g1, wqkv):
    n = tok.shape[0]
    return pl.pallas_call(
        tok_back_kernel,
        grid=(n // TOK_BLOCK,),
        in_specs=[token_rows(D), token_rows(3 * D), token_rows(D), const_spec((D,)), const_spec((D, 3 * D))],
        out_specs=token_rows(D),
        out_shape=jax.ShapeDtypeStruct((n, D), F32),
        cost_estimate=cost(4),
        name="tok_back",
    )(tok, dqkv, dx, g1, wqkv)


AXES = ("dp", "replica")


def swap(v, mask):
    return lax.ppermute(v, AXES, [(i, i ^ mask) for i in range(32)])


def plane(parts):
    return [swap(parts[m], 2 * m) for m in (1, 2, 3)]


def column(parts):
    return [swap(parts[m], 8 * m) for m in (1, 2, 3)]


def total_of(own, got):
    v = [own.astype(F32)] + [x.astype(F32) for x in got]
    return v[0] + v[1] if len(v) == 2 else (v[0] + v[1]) + (v[2] + v[3])


def added(own, got):
    return total_of(own, got).astype(BF)


def joined(own, got):
    return jnp.concatenate([own] + got, 0)


def shards(
    devices, tuned,
    text_tokens, segment_ids, pair_index, image_tokens,
    img_ln1, img_qkv, img_out, img_ln2, img_up, img_down, img_proj,
    txt_ln1, txt_qkv, txt_out, txt_ln2, txt_up, txt_down, txt_proj, log_scale,
):
    total = CAPS * devices
    denom = 2.0 * total
    row_of = jnp.arange(segment_ids.shape[0], dtype=jnp.int32) % (TOK_BLOCK // segment_ids.shape[1])
    lab = (segment_ids + PACK * row_of[:, None]).reshape(BLOCKS, 1, TOK_BLOCK)
    pair = pair_index
    if tuned:
        index = lax.axis_index(AXES)
        mine = ((index & 1) * 16 + ((index >> 1) & 3) * 4 + (index >> 3)).astype(jnp.int32).reshape(1)
        owner, row = pair // CAPS, pair % CAPS
        pair = (((owner & 1) * 16 + ((owner >> 1) & 3) * 4 + (owner >> 3)) ^ mine) * CAPS + row
    else:
        mine = jnp.zeros((1,), jnp.int32)
    pair = pair.reshape(CAPS, 1)
    lab, pair = lax.optimization_barrier((lab, pair))
    emb = image_tower(
        jnp.transpose(image_tokens, (1, 0, 2)), img_ln1, img_qkv, img_out, img_ln2, img_up, img_down, img_proj
    )
    if tuned:
        near = joined(emb, column([emb] * 4))
        o, qkv, p, h1 = text_att(text_tokens, lab, txt_ln1, txt_qkv)
        o, near = lax.optimization_barrier((o, near))
        got = plane([near] * 4)
    else:
        o, qkv, p, h1 = text_att(text_tokens, lab, txt_ln1, txt_qkv)
    h2, c2, gp, pu, pb, e, temb, cnt = text_mlp(text_tokens, o, lab, txt_out, txt_ln2, txt_up, txt_down, txt_proj)
    if tuned:
        near, got, temb = lax.optimization_barrier((near, got, temb))
        near = joined(near, got)
        images = joined(near, [swap(near, 1)])
    else:
        images = lax.all_gather(emb, AXES, axis=0, tiled=True)
    lines = total // 128
    g, sums = simple(
        functools.partial(cosine_kernel, denom),
        [((CAPS, total), F32), ((2 * lines + 8, 128), F32)],
        smem=2,
        us=3,
        name="cosine",
    )(log_scale, mine, temb, images, pair)
    (dt_row,) = simple(functools.partial(rows_kernel, denom), [((CAPS, D), F32)], smem=1, us=2, name="rows")(
        log_scale, g, images, pair
    )
    if tuned:
        sums = total_of(sums, [swap(sums, 1)])
        sums = total_of(sums, plane([sums] * 4))
        sums = total_of(sums, column([sums] * 4))
    else:
        sums = lax.psum(sums, AXES)
    send_d, keep_d, send_p, keep_p, du, dy, loss, temp = simple(
        functools.partial(head_kernel, denom),
        [
            ((768, D), BF), ((768, D), BF), ((192, D), BF), ((192, D), BF),
            ((BLOCKS, 48, FF), BF), ((BLOCKS, 48, D), BF), ((1, 1), F32), ((1, 1), F32),
        ],
        [pltpu.VMEM((FF, D), F32), pltpu.VMEM((D, D), F32)],
        smem=2,
        us=5,
        name="head_back",
    )(log_scale, mine, g, images, sums, dt_row, e, pb, cnt, pu, txt_proj, txt_down)
    dx, dxb, send_u, keep_u = mlp_back(mine, lab, h2, gp, c2, du, dy, txt_ln2, txt_up)

    def mlp_parts(d, u, p):
        both = jnp.concatenate([d.reshape(4, 4, 48, D), u.reshape(4, 4, 48, D)], 2).reshape(4, 384, D)
        return jnp.concatenate([both, p.reshape(4, 48, D)], 1)

    def spread_mlp(own, other):
        outs = [((FF, D), F32), ((D, FF), F32), ((D, D), F32), ((D,), F32)]
        return simple(spread_mlp_kernel, outs, smem=1, us=4, name="spread_mlp")(mine, own, other, txt_up, txt_ln2)

    def spread_att(own, other):
        outs = [((D, D), F32), ((D, 3 * D), F32), ((D,), F32)]
        return simple(spread_att_kernel, outs, smem=1, us=4, name="spread_att")(mine, own, other, txt_qkv, txt_ln1)

    if not tuned:
        dqkv = att_core(qkv, p, dxb, txt_out)
        send_a, keep_a = att_grads(mine, h1, dqkv, o, dxb)
        grad_tokens = tok_back(text_tokens, dqkv, dx, txt_ln1, txt_qkv)
        sums = [keep_d, send_d, keep_u, send_u, keep_a, send_a, keep_p, send_p]
        d, d2, u, u2, a, a2, p, p2 = [v.astype(BF) for v in lax.psum([v.astype(F32) for v in sums], AXES)]
        grad_down, grad_up, grad_proj, gain2 = spread_mlp(
            mlp_parts(d, u, p).reshape(1728, D), mlp_parts(d2, u2, p2).reshape(1728, D)
        )
        grad_out, grad_qkv, gain1 = spread_att(a, a2)
    else:
        d = added(keep_d, [swap(send_d, 1)])
        pr = added(keep_p, [swap(send_p, 1)])
        m = mlp_parts(d, added(keep_u, [swap(send_u, 1)]), pr)
        dxb, m = lax.optimization_barrier((dxb, m))
        got = plane(m)
        dqkv = att_core(qkv, p, dxb, txt_out)
        got, dqkv = lax.optimization_barrier((got, dqkv))
        m = added(m[0], got)
        m, dqkv = lax.optimization_barrier((m, dqkv))
        parts = [jnp.concatenate([m[96 * k : 96 * k + 96], m[384:]], 0) for k in (0, 2, 1, 3)]
        got = column(parts)
        send_a, keep_a = att_grads(mine, h1, dqkv, o, dxb)
        got, send_a, keep_a = lax.optimization_barrier((got, send_a, keep_a))
        q = added(parts[0], got)
        far = swap(q[:96], 16)
        a = added(keep_a, [swap(send_a, 1)]).reshape(4, 192, D)
        got_a = plane(a)
        m = joined(q[:96], [far])
        near = swap(m, 8)
        dqkv, a, m = lax.optimization_barrier((dqkv, a, m))
        grad_tokens = tok_back(text_tokens, dqkv, dx, txt_ln1, txt_qkv)
        got_a, near, grad_tokens = lax.optimization_barrier((got_a, near, grad_tokens))
        a = added(a[0], got_a)
        m = joined(m, [near, q[96:]])
        got_m = plane([m] * 4)
        a = added(a[:96], [swap(a[96:], 8)])
        a = added(a[:48], [swap(a[48:], 16)])
        a, got_m[0], got_m[1] = lax.optimization_barrier((a, got_m[0], got_m[1]))
        a = joined(a, [swap(a, 16)])
        a = joined(a, [swap(a, 8)])
        got_m, a = lax.optimization_barrier((got_m, a))
        got_a = plane([a] * 4)
        m = joined(m, got_m)
        grad_down, grad_up, grad_proj, gain2 = spread_mlp(m, swap(m, 1))
        got_a, grad_up = lax.optimization_barrier((got_a, grad_up))
        a = joined(a, got_a)
        grad_out, grad_qkv, gain1 = spread_att(a, swap(a, 1))
    return (
        loss.reshape(1), grad_tokens, gain1, grad_qkv, grad_out, gain2,
        grad_up, grad_down, grad_proj, temp.reshape(1),
    )


def solution(mesh):
    both = ("dp", "replica")
    devices = mesh.shape["dp"] * mesh.shape["replica"]
    tuned = (mesh.shape["dp"], mesh.shape["replica"]) == (8, 4)
    rows = P(both, None)
    return jax.shard_map(
        functools.partial(shards, devices, tuned),
        mesh=mesh,
        in_specs=(rows, rows, P(both), P(both, None, None)) + (P(),) * 15,
        out_specs=(P(), rows) + (P(),) * 8,
        check_vma=False,
    )
```

```python
import functools
import math

import jax
import jax.numpy as jnp
from jax import lax
from jax.experimental import pallas as pl
from jax.experimental.pallas import tpu as pltpu
from jax.sharding import PartitionSpec as P

D = 384
HEADS = 6
HEAD = 64
FF = 1536
IMG_LEN = 50
PACK = 4
CAPS = 64
TOK_BLOCK = 256
CAP_BLOCK = 16
BLOCKS = 4
PAIR = 128
IMG_BLOCK = 16
IMG_ROWS = IMG_BLOCK * IMG_LEN
EPS = 1e-06

BF = jnp.bfloat16
F32 = jnp.float32
GELU_K = math.sqrt(2.0 / math.pi)
GELU_C = 0.044715


def mm(a, b):
    return lax.dot_general(a, b, (((1,), (0,)), ((), ())), preferred_element_type=F32)


def mm_nt(a, b):
    return lax.dot_general(a, b, (((1,), (1,)), ((), ())), preferred_element_type=F32)


def mm_tn(a, b):
    return lax.dot_general(a, b, (((0,), (0,)), ((), ())), preferred_element_type=F32)


def row_mean(v):
    return jnp.sum(v, -1, keepdims=True) * (1.0 / D)


def normalize(v):
    centre = v - row_mean(v)
    return centre * lax.rsqrt(row_mean(centre * centre) + EPS)


def split3(v):
    high = v.astype(BF)
    rest = v - high.astype(F32)
    mid = rest.astype(BF)
    low = (rest - mid.astype(F32)).astype(BF)
    return high, mid, low


def wide_mm(v, w):
    high, mid, low = split3(v)
    n = v.shape[0]
    out = mm(jnp.concatenate([high, mid, low], 0), w)
    return out[:n] + out[n : 2 * n] + out[2 * n :]


def gelu_parts(z):
    z2 = z * z
    t = jnp.tanh(z * (z2 * (GELU_K * GELU_C) + GELU_K))
    hp = t * 0.5 + 0.5
    u = z * hp
    slope = hp + (u * (1.0 - hp)) * (z2 * (6.0 * GELU_K * GELU_C) + 2.0 * GELU_K)
    return u, slope


def lanes_head(shape):
    return lax.broadcasted_iota(jnp.int32, shape, len(shape) - 1) // HEAD


def image_kernel(x_ref, g1, wqkv, wout, g2, wup, wdown, wproj, emb_ref, kv, x0, att):
    step = pl.program_id(0)
    gain = g1[...].reshape(1, D)
    for c in range(2):
        x = x_ref[IMG_LEN // 2 * c : IMG_LEN // 2 * (c + 1)].astype(F32).reshape(IMG_ROWS // 2, D)
        h = (normalize(x) * gain).astype(BF)
        kv[IMG_ROWS // 2 * c : IMG_ROWS // 2 * (c + 1), :] = mm(h, wqkv[:, D:]).astype(BF)
        if c == 0:
            x0[pl.ds(pl.multiple_of(step * IMG_BLOCK, IMG_BLOCK), IMG_BLOCK), :] = x[:IMG_BLOCK]
            h0 = h[:IMG_BLOCK]
    q = mm(h0, wqkv[:, :D]).astype(BF).astype(F32) * (HEAD**-0.5)
    head = lanes_head((IMG_BLOCK, D))
    queries = HEADS * IMG_BLOCK
    rows = lax.broadcasted_iota(jnp.int32, (queries, IMG_ROWS), 0)
    cols = lax.broadcasted_iota(jnp.int32, (queries, IMG_ROWS), 1)
    own = cols % IMG_BLOCK == rows % IMG_BLOCK
    q6 = jnp.concatenate([jnp.where(head == h, q, 0.0) for h in range(HEADS)], 0)
    s = mm_nt(q6.astype(BF), kv[:, :D])
    s = jnp.where(own, s, -1e30)
    e = jnp.exp(s - jnp.max(s, -1, keepdims=True))
    p = (e * (1.0 / jnp.sum(e, -1, keepdims=True))).astype(BF)
    r = mm(p, kv[:, D:])
    o = jnp.where(head == 0, r[0:IMG_BLOCK], 0.0)
    for h in range(1, HEADS):
        o = jnp.where(head == h, r[IMG_BLOCK * h : IMG_BLOCK * (h + 1)], o)
    att[pl.ds(pl.multiple_of(step * IMG_BLOCK, IMG_BLOCK), IMG_BLOCK), :] = o

    @pl.when(step == pl.num_programs(0) - 1)
    def _():
        x1 = x0[...] + mm(att[...].astype(BF), wout[...])
        h2 = (normalize(x1) * g2[...].reshape(1, D)).astype(BF)
        u, _ = gelu_parts(mm(h2, wup[...]))
        y = x1 + mm(u.astype(BF), wdown[...])
        e = mm(y.astype(BF), wproj[...])
        emb_ref[...] = (e * lax.rsqrt(jnp.sum(e * e, -1, keepdims=True) + EPS)).astype(BF)


def cost(us):
    return pl.CostEstimate(flops=int(us * 1e9), bytes_accessed=int(us * 3e6), transcendentals=0)


def const_spec(shape):
    zeros = (0,) * len(shape)
    return pl.BlockSpec(shape, lambda *_: zeros, pipeline_mode=pl.Buffered(1))


def image_tower(x, g1, wqkv, wout, g2, wup, wdown, wproj):
    count = x.shape[1]
    return pl.pallas_call(
        image_kernel,
        grid=(count // IMG_BLOCK,),
        in_specs=[
            pl.BlockSpec((IMG_LEN, IMG_BLOCK, D), lambda i: (0, i, 0)),
            const_spec((D,)),
            const_spec((D, 3 * D)),
            const_spec((D, D)),
            const_spec((D,)),
            const_spec((D, FF)),
            const_spec((FF, D)),
            const_spec((D, D)),
        ],
        out_specs=pl.BlockSpec((count, D), lambda i: (0, 0)),
        out_shape=jax.ShapeDtypeStruct((count, D), BF),
        scratch_shapes=[
            pltpu.VMEM((IMG_ROWS, 2 * D), BF),
            pltpu.VMEM((count, D), F32),
            pltpu.VMEM((count, D), F32),
        ],
        cost_estimate=cost(12),
        name="image_tower",
    )(x, g1, wqkv, wout, g2, wup, wdown, wproj)


def pair_mask(lab_ref, pair):
    lab = lab_ref[0, :, PAIR * pair : PAIR * pair + PAIR].astype(F32)
    wide = jnp.broadcast_to(lab, (PAIR, PAIR))
    return wide == wide.T


def text_att_kernel(tok_ref, lab_ref, g1, wqkv, o_ref, qkv_ref, p_ref, h1_ref):
    x = tok_ref[...].astype(F32)
    h1 = (normalize(x) * g1[...].reshape(1, D)).astype(BF)
    h1_ref[...] = h1
    qkv = mm(h1, wqkv[...]).astype(BF)
    qkv_ref[...] = qkv
    low = lax.broadcasted_iota(jnp.int32, (PAIR, PAIR), 1) < HEAD
    for pair in range(2):
        rows = slice(PAIR * pair, PAIR * pair + PAIR)
        mask = pair_mask(lab_ref, pair)
        mask = jnp.concatenate([mask, mask], 0)
        for j in range(HEADS // 2):
            cols = slice(PAIR * j, PAIR * j + PAIR)
            q2 = qkv[rows, PAIR * j : PAIR * j + PAIR] * jnp.asarray(HEAD**-0.5, BF)
            k2 = qkv[rows, D + PAIR * j : D + PAIR * j + PAIR]
            v2 = qkv[rows, 2 * D + PAIR * j : 2 * D + PAIR * j + PAIR]
            zero = jnp.zeros_like(q2)
            q22 = jnp.concatenate([jnp.where(low, q2, zero), jnp.where(low, zero, q2)], 0)
            s = jnp.where(mask, mm_nt(q22, k2), -1e30)
            ex = jnp.exp(s - jnp.max(s, -1, keepdims=True))
            p = (ex * (1.0 / jnp.sum(ex, -1, keepdims=True))).astype(BF)
            p_ref[pair, j] = p
            v22 = jnp.concatenate([jnp.where(low, v2, zero), jnp.where(low, zero, v2)], 0)
            o = mm(jnp.concatenate([p[:PAIR], p[PAIR:]], 1), v22)
            o_ref[rows, cols] = o.astype(BF)


def text_mlp_kernel(
    tok_ref, o_ref, lab_ref, wout, g2, wup, wdown, wproj,
    h2_ref, c2_ref, gp_ref, pu_ref, pb_ref, e_ref, emb_ref, cnt_ref, pt, po,
):
    step = pl.program_id(0)
    tok = tok_ref[...]
    o = o_ref[...]
    x1 = tok.astype(F32) + mm(o, wout[...])
    c2 = x1 - row_mean(x1)
    c2_ref[...] = c2
    h2 = (c2 * lax.rsqrt(row_mean(c2 * c2) + EPS) * g2[...].reshape(1, D)).astype(BF)
    h2_ref[...] = h2
    hit = lax.broadcasted_iota(jnp.int32, (CAP_BLOCK, TOK_BLOCK), 0) == lab_ref[0]
    member = jnp.where(hit, 1.0, 0.0)
    caps = pl.ds(pl.multiple_of(step * CAP_BLOCK, CAP_BLOCK), CAP_BLOCK)
    member_b = member.astype(BF)
    pt[caps, :] = mm(member_b, tok)
    po[caps, :] = mm(member_b, o)
    cnt_ref[caps, :] = jnp.broadcast_to(jnp.sum(member, -1, keepdims=True), (CAP_BLOCK, 128))
    for k in range(FF // 512):
        cols = slice(512 * k, 512 * (k + 1))
        u, slope = gelu_parts(mm(h2, wup[:, cols]))
        gp_ref[:, cols] = slope.astype(BF)
        pu_ref[caps, cols] = mm(member_b, u.astype(BF))

    @pl.when(step == pl.num_programs(0) - 1)
    def _():
        total = pt[...] + wide_mm(po[...], wout[...]) + wide_mm(pu_ref[...], wdown[...])
        pooled = (total * (1.0 / cnt_ref[:, 0:1])).astype(BF)
        pb_ref[...] = pooled
        e = mm(pooled, wproj[...])
        e_ref[...] = e
        emb_ref[...] = (e * lax.rsqrt(jnp.sum(e * e, -1, keepdims=True) + EPS)).astype(BF)


def token_rows(width):
    return pl.BlockSpec((TOK_BLOCK, width), lambda i: (i, 0))


def block_of(a, b):
    return pl.BlockSpec((1, a, b), lambda i: (i, 0, 0))


def whole(a, b):
    return pl.BlockSpec((a, b), lambda i: (0, 0))


def text_att(tok, lab, g1, wqkv):
    n = tok.shape[0]
    blocks = n // TOK_BLOCK
    shape = jax.ShapeDtypeStruct
    return pl.pallas_call(
        text_att_kernel,
        grid=(blocks,),
        in_specs=[token_rows(D), block_of(1, TOK_BLOCK), const_spec((D,)), const_spec((D, 3 * D))],
        out_specs=[
            token_rows(D),
            token_rows(3 * D),
            pl.BlockSpec((2, 3, 2 * PAIR, PAIR), lambda i: (i, 0, 0, 0)),
            token_rows(D),
        ],
        out_shape=[
            shape((n, D), BF), shape((n, 3 * D), BF), shape((2 * blocks, 3, 2 * PAIR, PAIR), BF), shape((n, D), BF),
        ],
        cost_estimate=cost(9),
        name="text_att",
    )(tok, lab, g1, wqkv)


def text_mlp(tok, o, lab, wout, g2, wup, wdown, wproj):
    n = tok.shape[0]
    shape = jax.ShapeDtypeStruct
    return pl.pallas_call(
        text_mlp_kernel,
        grid=(n // TOK_BLOCK,),
        in_specs=[
            token_rows(D), token_rows(D), block_of(1, TOK_BLOCK),
            const_spec((D, D)), const_spec((D,)), const_spec((D, FF)), const_spec((FF, D)), const_spec((D, D)),
        ],
        out_specs=[
            token_rows(D), token_rows(D), token_rows(FF),
            whole(CAPS, FF), whole(CAPS, D), whole(CAPS, D), whole(CAPS, D), whole(CAPS, 128),
        ],
        out_shape=[
            shape((n, D), BF), shape((n, D), F32), shape((n, FF), BF),
            shape((CAPS, FF), F32), shape((CAPS, D), BF), shape((CAPS, D), F32),
            shape((CAPS, D), BF), shape((CAPS, 128), F32),
        ],
        scratch_shapes=[pltpu.VMEM((CAPS, D), F32), pltpu.VMEM((CAPS, D), F32)],
        cost_estimate=cost(11),
        name="text_mlp",
    )(tok, o, lab, wout, g2, wup, wdown, wproj)


def reorder(mine, row):
    return jnp.where(mine & 1 == 1, pltpu.roll(row, 64, 1), row)


def cosine_kernel(denom, scale_ref, mine_ref, emb, images, pair, g_ref, sum_ref):
    mine = mine_ref[0]
    scale = jnp.exp(jnp.full((1, 1), scale_ref[0], F32))
    g = mm_nt(emb[...], images[...])
    g_ref[...] = g
    e = jnp.exp(g * scale)
    eg = e * g
    total = jnp.sum(e, -1, keepdims=True)
    hit = lax.broadcasted_iota(jnp.int32, g.shape, 1) == pair[...]
    own = jnp.sum(jnp.where(hit, g, 0.0), -1, keepdims=True)
    loss = jnp.sum(jnp.log(total) - 2.0 * scale * own, 0, keepdims=True)
    temp = jnp.sum(jnp.sum(eg, -1, keepdims=True) / total - 2.0 * own, 0, keepdims=True)
    n = g.shape[1] // 128
    for k, v in enumerate((jnp.sum(e, 0, keepdims=True), jnp.sum(eg, 0, keepdims=True))):
        for r in range(n):
            sum_ref[pl.ds(k * n + ((mine >> 1) ^ r), 1), :] = reorder(mine, v[:, 128 * r : 128 * (r + 1)])
    lane = lax.broadcasted_iota(jnp.int32, (8, 128), 1)
    sum_ref[2 * n :, :] = jnp.where(lane == 0, loss, jnp.where(lane == 1, temp, 0.0))


def rows_kernel(denom, scale_ref, g_ref, images, pair, dt_ref):
    scale = jnp.exp(jnp.full((1, 1), scale_ref[0], F32))
    g = g_ref[...]
    e = jnp.exp(g * scale)
    hit = lax.broadcasted_iota(jnp.int32, g.shape, 1) == pair[...]
    p = e * (1.0 / jnp.sum(e, -1, keepdims=True))
    dl = jnp.where(hit, p - 2.0, p) * (scale * (1.0 / denom))
    dt_ref[...] = mm(dl.astype(BF), images[...])


def quarter(mine, base, k, rows=48):
    far = (mine & 3) ^ k
    return pl.multiple_of(base + rows * ((far & 1) * 2 + (far >> 1)), 16)


def halves(mine, rows, send_ref, keep_ref, piece):
    for rel in range(8):
        ref = keep_ref if rel < 4 else send_ref
        at = (rel % 4) * rows
        if rows == 48:
            ref[at : at + 48, :] = piece((mine >> 2) ^ rel, 0).astype(BF)
            continue
        for k in range(4):
            ref[pl.ds(quarter(mine, at, k), 48), :] = piece((mine >> 2) ^ rel, k).astype(BF)


def block(acc, at, rows, col=0):
    return acc[pl.ds(pl.multiple_of(at * rows, 16), rows), D * col : D * (col + 1)]


def head_kernel(
    denom, scale_ref, mine_ref, g_ref, images, sums, dt_row, e_ref, pb, cnt, pu, wproj, wdown,
    sd_ref, kd_ref, sp_ref, kp_ref, du_ref, dy_ref, loss_out, temp_out, down, proj,
):
    mine = mine_ref[0]
    scale = jnp.exp(jnp.full((1, 1), scale_ref[0], F32))
    n = g_ref.shape[1] // 128

    def columns(k):
        return jnp.concatenate([reorder(mine, sums[pl.ds(k * n + ((mine >> 1) ^ r), 1), :]) for r in range(n)], 1)

    temp = jnp.sum(jnp.sum(sums[n : 2 * n, :] / sums[0:n, :], 0, keepdims=True), -1, keepdims=True)
    loss = jnp.sum(jnp.sum(jnp.log(sums[0:n, :]), 0, keepdims=True), -1, keepdims=True)
    loss_out[...] = (sums[2 * n : 2 * n + 1, 0:1] + loss) * (1.0 / denom)
    temp_out[...] = (sums[2 * n : 2 * n + 1, 1:2] + temp) * (scale * (1.0 / denom))
    inverse = 1.0 / columns(0)
    dl = jnp.exp(g_ref[...] * scale) * (inverse * (scale * (1.0 / denom)))
    dt = dt_row[...] + mm(dl.astype(BF), images[...])
    e = e_ref[...]
    r = lax.rsqrt(jnp.sum(e * e, -1, keepdims=True) + EPS)
    de = (dt - e * (r * r * jnp.sum(dt * e, -1, keepdims=True))) * r
    de = de.astype(BF)
    dpooled = mm_nt(de, wproj[...])
    dy = dpooled * (1.0 / cnt[:, 0:1])
    dyb = dy.astype(BF)
    du = mm_nt(dyb, wdown[...])
    for i, piece in enumerate(split3(du)):
        for b in range(BLOCKS):
            du_ref[b, CAP_BLOCK * i : CAP_BLOCK * (i + 1), :] = piece[CAP_BLOCK * b : CAP_BLOCK * (b + 1)]
    for i, piece in enumerate(split3(dy)):
        for b in range(BLOCKS):
            dy_ref[b, CAP_BLOCK * i : CAP_BLOCK * (i + 1), :] = piece[CAP_BLOCK * b : CAP_BLOCK * (b + 1)]
    down[...] = mm_tn(jnp.concatenate(split3(pu[...]), 0), jnp.concatenate([dyb, dyb, dyb], 0))
    proj[...] = mm_tn(pb[...], de)
    halves(mine, 192, sd_ref, kd_ref, lambda at, k: block(down, at * 4 + k, 48))
    halves(mine, 48, sp_ref, kp_ref, lambda at, k: block(proj, at, 48))


def mlp_back_kernel(
    mine_ref, lab_ref, h2_ref, gp_ref, c2_ref, du_ref, dy_ref, g2, wup,
    dx_ref, dxb_ref, send_ref, keep_ref, acc,
):
    step = pl.program_id(0)

    @pl.when(step == 0)
    def _():
        acc[...] = jnp.zeros_like(acc)

    hit = lax.broadcasted_iota(jnp.int32, (3 * CAP_BLOCK, TOK_BLOCK), 0) % CAP_BLOCK == lab_ref[0]
    spread = jnp.where(hit, 1.0, 0.0).astype(BF)
    du = mm_tn(spread, du_ref[0])
    dz = (du * gp_ref[...].astype(F32)).astype(BF)
    dy = mm_tn(spread, dy_ref[0])
    dh = mm_nt(dz, wup[...])
    c2 = c2_ref[...]
    r = lax.rsqrt(row_mean(c2 * c2) + EPS)
    unit = c2 * r
    dn = dh * g2[...].reshape(1, D)
    dx = dy + r * (dn - row_mean(dn) - unit * row_mean(dn * unit))
    dx_ref[...] = dx
    dxb_ref[...] = dx.astype(BF)
    h2 = h2_ref[...]
    acc[...] += mm_tn(h2, dz)

    @pl.when(step == pl.num_programs(0) - 1)
    def _():
        halves(mine_ref[0], 192, send_ref, keep_ref, lambda at, k: block(acc, at, 48, k))


def att_core_kernel(qkv_ref, p_ref, dxb_ref, wout, dqkv_ref):
    do = mm_nt(dxb_ref[...], wout[...]).astype(BF)
    low = lax.broadcasted_iota(jnp.int32, (PAIR, PAIR), 1) < HEAD
    zero = jnp.zeros((PAIR, PAIR), BF)
    half = HEAD**-0.5

    def twice(v):
        return jnp.concatenate([jnp.where(low, v, zero), jnp.where(low, zero, v)], 0)

    for pair in range(2):
        rows = slice(PAIR * pair, PAIR * pair + PAIR)
        for j in range(HEADS // 2):
            cols = slice(PAIR * j, PAIR * j + PAIR)
            q2 = qkv_ref[rows, PAIR * j : PAIR * j + PAIR]
            k2 = qkv_ref[rows, D + PAIR * j : D + PAIR * j + PAIR]
            v2 = qkv_ref[rows, 2 * D + PAIR * j : 2 * D + PAIR * j + PAIR]
            do2 = twice(do[rows, cols])
            pb = p_ref[pair, j]
            p = pb.astype(F32)
            dp = mm_nt(do2, v2)
            ds = (p * (dp - jnp.sum(dp * p, -1, keepdims=True))).astype(BF)
            dq = mm(jnp.concatenate([ds[:PAIR], ds[PAIR:]], 1), twice(k2)) * half
            dk = mm_tn(ds, twice(q2)) * half
            dv = mm_tn(pb, do2)
            dqkv_ref[rows, PAIR * j : PAIR * j + PAIR] = dq.astype(BF)
            dqkv_ref[rows, D + PAIR * j : D + PAIR * j + PAIR] = dk.astype(BF)
            dqkv_ref[rows, 2 * D + PAIR * j : 2 * D + PAIR * j + PAIR] = dv.astype(BF)


def att_grads_kernel(mine_ref, h1_ref, dqkv_ref, o_ref, dxb_ref, send_ref, keep_ref, acc):
    acc[:, :D] = mm_tn(o_ref[...], dxb_ref[...])
    acc[:, D:] = mm_tn(h1_ref[...], dqkv_ref[...])
    halves(mine_ref[0], 192, send_ref, keep_ref, lambda at, k: block(acc, at, 48, k))


def tok_back_kernel(tok_ref, dqkv_ref, dx_ref, g1, wqkv, gtok_ref):
    x = tok_ref[...].astype(F32)
    centre = x - row_mean(x)
    r = lax.rsqrt(row_mean(centre * centre) + EPS)
    unit = centre * r
    dn = mm_nt(dqkv_ref[...], wqkv[...]) * g1[...].reshape(1, D)
    gtok_ref[...] = dx_ref[...] + r * (dn - row_mean(dn) - unit * row_mean(dn * unit))


def gain_of(grad, weight, gain):
    high, mid, _ = split3(grad * weight.astype(F32))
    ones = jnp.ones((8, grad.shape[1]), BF)
    total = mm_nt(ones, high) + mm_nt(ones, mid)
    return total[0:1] / gain.reshape(1, D)


def arrived(mine_ref, own, other, rows):
    for rel in range(8):
        src = own if rel < 4 else other
        yield (mine_ref[0] >> 2) ^ rel, src, (rel % 4) * rows


def spread_mlp_kernel(mine_ref, own, other, wup, g2, down_ref, up_ref, proj_ref, gain_ref):
    for at, src, row in arrived(mine_ref, own, other, 432):
        rows = pl.ds(pl.multiple_of(at * 48, 16), 48)
        for k in range(4):
            part = quarter(mine_ref[0], row, k, 96)
            down_ref[pl.ds(pl.multiple_of(at * 192 + 48 * k, 16), 48), :] = src[pl.ds(part, 48), :].astype(F32)
            up_ref[rows, D * k : D * (k + 1)] = src[pl.ds(pl.multiple_of(part + 48, 16), 48), :].astype(F32)
        proj_ref[rows, :] = src[row + 384 : row + 432, :].astype(F32)
    gain_ref[...] = gain_of(up_ref[...], wup[...], g2[...]).reshape(D)


def spread_att_kernel(mine_ref, own, other, wqkv, g1, out_ref, qkv_ref, gain_ref):
    for at, src, row in arrived(mine_ref, own, other, 192):
        rows = pl.ds(pl.multiple_of(at * 48, 16), 48)
        out_ref[rows, :] = src[pl.ds(quarter(mine_ref[0], row, 0), 48), :].astype(F32)
        for k in range(3):
            qkv_ref[rows, D * k : D * (k + 1)] = src[pl.ds(quarter(mine_ref[0], row, k + 1), 48), :].astype(F32)
    gain_ref[...] = gain_of(qkv_ref[...], wqkv[...], g1[...]).reshape(D)


SMEM = pl.BlockSpec(memory_space=pltpu.SMEM)
VMEM = pl.BlockSpec(memory_space=pltpu.VMEM)


def simple(kernel, outs, scratch=(), smem=0, us=3, name=None):
    def call(*args):
        return pl.pallas_call(
            kernel,
            in_specs=[SMEM] * smem + [VMEM] * (len(args) - smem),
            out_specs=[VMEM] * len(outs),
            out_shape=[jax.ShapeDtypeStruct(s, t) for s, t in outs],
            scratch_shapes=list(scratch),
            cost_estimate=cost(us),
            name=name,
        )(*args)

    return call


def mlp_back(mine, lab, h2, gp, c2, du, dy, g2, wup):
    n = h2.shape[0]

    def rows(width):
        return pl.BlockSpec((TOK_BLOCK, width), lambda i: (i, 0))

    def blk(a, b):
        return pl.BlockSpec((1, a, b), lambda i: (i, 0, 0))

    shape = jax.ShapeDtypeStruct
    return pl.pallas_call(
        mlp_back_kernel,
        grid=(n // TOK_BLOCK,),
        in_specs=[
            SMEM, blk(1, TOK_BLOCK), rows(D), rows(FF), rows(D), blk(3 * CAP_BLOCK, FF), blk(3 * CAP_BLOCK, D),
            const_spec((D,)), const_spec((D, FF)),
        ],
        out_specs=[rows(D), rows(D)] + [pl.BlockSpec((768, D), lambda i: (0, 0))] * 2,
        out_shape=[shape((n, D), F32), shape((n, D), BF), shape((768, D), BF), shape((768, D), BF)],
        scratch_shapes=[pltpu.VMEM((D, FF), F32)],
        cost_estimate=cost(9),
        name="mlp_back",
    )(mine, lab, h2, gp, c2, du, dy, g2, wup)


def att_core(qkv, p, dxb, wout):
    n = dxb.shape[0]
    return pl.pallas_call(
        att_core_kernel,
        grid=(n // TOK_BLOCK,),
        in_specs=[
            token_rows(3 * D),
            pl.BlockSpec((2, 3, 2 * PAIR, PAIR), lambda i: (i, 0, 0, 0)),
            token_rows(D),
            const_spec((D, D)),
        ],
        out_specs=token_rows(3 * D),
        out_shape=jax.ShapeDtypeStruct((n, 3 * D), BF),
        cost_estimate=cost(10),
        name="att_core",
    )(qkv, p, dxb, wout)


def att_grads(mine, h1, dqkv, o, dxb):
    outs = [((768, D), BF)] * 2
    scratch = [pltpu.VMEM((D, 4 * D), F32)]
    return simple(att_grads_kernel, outs, scratch, smem=1, us=4, name="att_grads")(mine, h1, dqkv, o, dxb)


def tok_back(tok, dqkv, dx, g1, wqkv):
    n = tok.shape[0]
    return pl.pallas_call(
        tok_back_kernel,
        grid=(n // TOK_BLOCK,),
        in_specs=[token_rows(D), token_rows(3 * D), token_rows(D), const_spec((D,)), const_spec((D, 3 * D))],
        out_specs=token_rows(D),
        out_shape=jax.ShapeDtypeStruct((n, D), F32),
        cost_estimate=cost(4),
        name="tok_back",
    )(tok, dqkv, dx, g1, wqkv)


AXES = ("dp", "replica")


def swap(v, mask):
    return lax.ppermute(v, AXES, [(i, i ^ mask) for i in range(32)])


def plane(parts):
    return [swap(parts[m], 2 * m) for m in (1, 2, 3)]


def column(parts):
    return [swap(parts[m], 8 * m) for m in (1, 2, 3)]


def total_of(own, got):
    v = [own.astype(F32)] + [x.astype(F32) for x in got]
    return v[0] + v[1] if len(v) == 2 else (v[0] + v[1]) + (v[2] + v[3])


def added(own, got):
    return total_of(own, got).astype(BF)


def joined(own, got):
    return jnp.concatenate([own] + got, 0)


def shards(
    devices, tuned,
    text_tokens, segment_ids, pair_index, image_tokens,
    img_ln1, img_qkv, img_out, img_ln2, img_up, img_down, img_proj,
    txt_ln1, txt_qkv, txt_out, txt_ln2, txt_up, txt_down, txt_proj, log_scale,
):
    total = CAPS * devices
    denom = 2.0 * total
    row_of = jnp.arange(segment_ids.shape[0], dtype=jnp.int32) % (TOK_BLOCK // segment_ids.shape[1])
    lab = (segment_ids + PACK * row_of[:, None]).reshape(BLOCKS, 1, TOK_BLOCK)
    pair = pair_index
    if tuned:
        index = lax.axis_index(AXES)
        mine = ((index & 1) * 16 + ((index >> 1) & 3) * 4 + (index >> 3)).astype(jnp.int32).reshape(1)
        owner, row = pair // CAPS, pair % CAPS
        pair = (((owner & 1) * 16 + ((owner >> 1) & 3) * 4 + (owner >> 3)) ^ mine) * CAPS + row
    else:
        mine = jnp.zeros((1,), jnp.int32)
    pair = pair.reshape(CAPS, 1)
    lab, pair = lax.optimization_barrier((lab, pair))
    emb = image_tower(
        jnp.transpose(image_tokens, (1, 0, 2)), img_ln1, img_qkv, img_out, img_ln2, img_up, img_down, img_proj
    )
    if tuned:
        near = joined(emb, column([emb] * 4))
        o, qkv, p, h1 = text_att(text_tokens, lab, txt_ln1, txt_qkv)
        o, near = lax.optimization_barrier((o, near))
        got = plane([near] * 4)
    else:
        o, qkv, p, h1 = text_att(text_tokens, lab, txt_ln1, txt_qkv)
    h2, c2, gp, pu, pb, e, temb, cnt = text_mlp(text_tokens, o, lab, txt_out, txt_ln2, txt_up, txt_down, txt_proj)
    if tuned:
        near, got, temb = lax.optimization_barrier((near, got, temb))
        near = joined(near, got)
        images = joined(near, [swap(near, 1)])
    else:
        images = lax.all_gather(emb, AXES, axis=0, tiled=True)
    lines = total // 128
    g, sums = simple(
        functools.partial(cosine_kernel, denom),
        [((CAPS, total), F32), ((2 * lines + 8, 128), F32)],
        smem=2,
        us=3,
        name="cosine",
    )(log_scale, mine, temb, images, pair)
    (dt_row,) = simple(functools.partial(rows_kernel, denom), [((CAPS, D), F32)], smem=1, us=2, name="rows")(
        log_scale, g, images, pair
    )
    if tuned:
        sums = total_of(sums, [swap(sums, 1)])
        sums = total_of(sums, plane([sums] * 4))
        sums = total_of(sums, [swap(sums, 8)])
        sums = total_of(sums, [swap(sums, 16)])
    else:
        sums = lax.psum(sums, AXES)
    send_d, keep_d, send_p, keep_p, du, dy, loss, temp = simple(
        functools.partial(head_kernel, denom),
        [
            ((768, D), BF), ((768, D), BF), ((192, D), BF), ((192, D), BF),
            ((BLOCKS, 48, FF), BF), ((BLOCKS, 48, D), BF), ((1, 1), F32), ((1, 1), F32),
        ],
        [pltpu.VMEM((FF, D), F32), pltpu.VMEM((D, D), F32)],
        smem=2,
        us=5,
        name="head_back",
    )(log_scale, mine, g, images, sums, dt_row, e, pb, cnt, pu, txt_proj, txt_down)
    dx, dxb, send_u, keep_u = mlp_back(mine, lab, h2, gp, c2, du, dy, txt_ln2, txt_up)

    def mlp_parts(d, u, p):
        both = jnp.concatenate([d.reshape(4, 4, 48, D), u.reshape(4, 4, 48, D)], 2).reshape(4, 384, D)
        return jnp.concatenate([both, p.reshape(4, 48, D)], 1)

    def spread_mlp(own, other):
        outs = [((FF, D), F32), ((D, FF), F32), ((D, D), F32), ((D,), F32)]
        return simple(spread_mlp_kernel, outs, smem=1, us=4, name="spread_mlp")(mine, own, other, txt_up, txt_ln2)

    def spread_att(own, other):
        outs = [((D, D), F32), ((D, 3 * D), F32), ((D,), F32)]
        return simple(spread_att_kernel, outs, smem=1, us=4, name="spread_att")(mine, own, other, txt_qkv, txt_ln1)

    if not tuned:
        dqkv = att_core(qkv, p, dxb, txt_out)
        send_a, keep_a = att_grads(mine, h1, dqkv, o, dxb)
        grad_tokens = tok_back(text_tokens, dqkv, dx, txt_ln1, txt_qkv)
        sums = [keep_d, send_d, keep_u, send_u, keep_a, send_a, keep_p, send_p]
        d, d2, u, u2, a, a2, p, p2 = [v.astype(BF) for v in lax.psum([v.astype(F32) for v in sums], AXES)]
        grad_down, grad_up, grad_proj, gain2 = spread_mlp(
            mlp_parts(d, u, p).reshape(1728, D), mlp_parts(d2, u2, p2).reshape(1728, D)
        )
        grad_out, grad_qkv, gain1 = spread_att(a, a2)
    else:
        d = added(keep_d, [swap(send_d, 1)])
        pr = added(keep_p, [swap(send_p, 1)])
        m = mlp_parts(d, added(keep_u, [swap(send_u, 1)]), pr)
        dxb, m = lax.optimization_barrier((dxb, m))
        got = plane(m)
        dqkv = att_core(qkv, p, dxb, txt_out)
        got, dqkv = lax.optimization_barrier((got, dqkv))
        m = added(m[0], got)
        m, dqkv = lax.optimization_barrier((m, dqkv))
        got = swap(m[192:], 8)
        send_a, keep_a = att_grads(mine, h1, dqkv, o, dxb)
        got, send_a, keep_a = lax.optimization_barrier((got, send_a, keep_a))
        m = added(joined(m[:192], [m[384:]]), [got])
        got = swap(m[96:], 16)
        a = added(keep_a, [swap(send_a, 1)]).reshape(4, 192, D)
        got, a = lax.optimization_barrier((got, a))
        m = added(joined(m[:96], [m[192:]]), [got])
        far = swap(m[:96], 16)
        got_a = plane(a)
        dqkv, a, m = lax.optimization_barrier((dqkv, a, m))
        grad_tokens = tok_back(text_tokens, dqkv, dx, txt_ln1, txt_qkv)
        far, grad_tokens = lax.optimization_barrier((far, grad_tokens))
        got_a, grad_tokens = lax.optimization_barrier((got_a, grad_tokens))
        near = joined(m[:96], [far])
        m = joined(near, [swap(near, 8), m[96:]])
        a = added(a[0], got_a)
        got_m = plane([m] * 4)
        a = added(a[:96], [swap(a[96:], 8)])
        a = added(a[:48], [swap(a[48:], 16)])
        a, got_m[0], got_m[1] = lax.optimization_barrier((a, got_m[0], got_m[1]))
        a = joined(a, [swap(a, 16)])
        a = joined(a, [swap(a, 8)])
        got_m, a = lax.optimization_barrier((got_m, a))
        got_a = plane([a] * 4)
        m = joined(m, got_m)
        grad_down, grad_up, grad_proj, gain2 = spread_mlp(m, swap(m, 1))
        got_a, grad_up = lax.optimization_barrier((got_a, grad_up))
        a = joined(a, got_a)
        grad_out, grad_qkv, gain1 = spread_att(a, swap(a, 1))
    return (
        loss.reshape(1), grad_tokens, gain1, grad_qkv, grad_out, gain2,
        grad_up, grad_down, grad_proj, temp.reshape(1),
    )


def solution(mesh):
    both = ("dp", "replica")
    devices = mesh.shape["dp"] * mesh.shape["replica"]
    tuned = (mesh.shape["dp"], mesh.shape["replica"]) == (8, 4)
    rows = P(both, None)
    return jax.shard_map(
        functools.partial(shards, devices, tuned),
        mesh=mesh,
        in_specs=(rows, rows, P(both), P(both, None, None)) + (P(),) * 15,
        out_specs=(P(), rows) + (P(),) * 8,
        check_vma=False,
    )
```

```python
import functools
import math

import jax
import jax.numpy as jnp
from jax import lax
from jax.experimental import pallas as pl
from jax.experimental.pallas import tpu as pltpu
from jax.sharding import PartitionSpec as P

D = 384
HEADS = 6
HEAD = 64
FF = 1536
IMG_LEN = 50
PACK = 4
CAPS = 64
TOK_BLOCK = 256
CAP_BLOCK = 16
BLOCKS = 4
PAIR = 128
IMG_BLOCK = 16
IMG_ROWS = IMG_BLOCK * IMG_LEN
EPS = 1e-06

SMEM = pl.BlockSpec(memory_space=pltpu.SMEM)
VMEM = pl.BlockSpec(memory_space=pltpu.VMEM)
ROOM = pltpu.CompilerParams(vmem_limit_bytes=24 * 2**20)

BF = jnp.bfloat16
F32 = jnp.float32
GELU_K = math.sqrt(2.0 / math.pi)
GELU_C = 0.044715


def mm(a, b):
    return lax.dot_general(a, b, (((1,), (0,)), ((), ())), preferred_element_type=F32)


def mm_nt(a, b):
    return lax.dot_general(a, b, (((1,), (1,)), ((), ())), preferred_element_type=F32)


def mm_tn(a, b):
    return lax.dot_general(a, b, (((0,), (0,)), ((), ())), preferred_element_type=F32)


def row_mean(v):
    return jnp.sum(v, -1, keepdims=True) * (1.0 / D)


def normalize(v):
    centre = v - row_mean(v)
    return centre * lax.rsqrt(row_mean(centre * centre) + EPS)


def split3(v):
    high = v.astype(BF)
    rest = v - high.astype(F32)
    mid = rest.astype(BF)
    low = (rest - mid.astype(F32)).astype(BF)
    return high, mid, low


def wide_mm(v, w):
    high, mid, low = split3(v)
    n = v.shape[0]
    out = mm(jnp.concatenate([high, mid, low], 0), w)
    return out[:n] + out[n : 2 * n] + out[2 * n :]


def gelu_parts(z):
    z2 = z * z
    t = jnp.tanh(z * (z2 * (GELU_K * GELU_C) + GELU_K))
    hp = t * 0.5 + 0.5
    u = z * hp
    slope = hp + (u * (1.0 - hp)) * (z2 * (6.0 * GELU_K * GELU_C) + 2.0 * GELU_K)
    return u, slope


def lanes_head(shape):
    return lax.broadcasted_iota(jnp.int32, shape, len(shape) - 1) // HEAD


def image_kernel(x_ref, g1, wqkv, wout, g2, wup, wdown, wproj, emb_ref, kv, x0, att):
    step = pl.program_id(0)
    gain = g1[...].reshape(1, D)
    for c in range(2):
        x = x_ref[IMG_LEN // 2 * c : IMG_LEN // 2 * (c + 1)].astype(F32).reshape(IMG_ROWS // 2, D)
        h = (normalize(x) * gain).astype(BF)
        kv[IMG_ROWS // 2 * c : IMG_ROWS // 2 * (c + 1), :] = mm(h, wqkv[:, D:]).astype(BF)
        if c == 0:
            x0[pl.ds(pl.multiple_of(step * IMG_BLOCK, IMG_BLOCK), IMG_BLOCK), :] = x[:IMG_BLOCK]
            h0 = h[:IMG_BLOCK]
    q = mm(h0, wqkv[:, :D]).astype(BF).astype(F32) * (HEAD**-0.5)
    head = lanes_head((IMG_BLOCK, D))
    queries = HEADS * IMG_BLOCK
    rows = lax.broadcasted_iota(jnp.int32, (queries, IMG_ROWS), 0)
    cols = lax.broadcasted_iota(jnp.int32, (queries, IMG_ROWS), 1)
    own = cols % IMG_BLOCK == rows % IMG_BLOCK
    q6 = jnp.concatenate([jnp.where(head == h, q, 0.0) for h in range(HEADS)], 0)
    s = mm_nt(q6.astype(BF), kv[:, :D])
    s = jnp.where(own, s, -1e30)
    e = jnp.exp(s - jnp.max(s, -1, keepdims=True))
    p = (e * (1.0 / jnp.sum(e, -1, keepdims=True))).astype(BF)
    r = mm(p, kv[:, D:])
    o = jnp.where(head == 0, r[0:IMG_BLOCK], 0.0)
    for h in range(1, HEADS):
        o = jnp.where(head == h, r[IMG_BLOCK * h : IMG_BLOCK * (h + 1)], o)
    att[pl.ds(pl.multiple_of(step * IMG_BLOCK, IMG_BLOCK), IMG_BLOCK), :] = o

    @pl.when(step == pl.num_programs(0) - 1)
    def _():
        x1 = x0[...] + mm(att[...].astype(BF), wout[...])
        h2 = (normalize(x1) * g2[...].reshape(1, D)).astype(BF)
        u, _ = gelu_parts(mm(h2, wup[...]))
        y = x1 + mm(u.astype(BF), wdown[...])
        e = mm(y.astype(BF), wproj[...])
        emb_ref[...] = (e * lax.rsqrt(jnp.sum(e * e, -1, keepdims=True) + EPS)).astype(BF)


def cost(us):
    return pl.CostEstimate(flops=int(us * 1e9), bytes_accessed=int(us * 3e6), transcendentals=0)


def const_spec(shape):
    zeros = (0,) * len(shape)
    return pl.BlockSpec(shape, lambda *_: zeros, pipeline_mode=pl.Buffered(1))


def image_tower(x, g1, wqkv, wout, g2, wup, wdown, wproj):
    count = x.shape[1]
    return pl.pallas_call(
        image_kernel,
        grid=(count // IMG_BLOCK,),
        in_specs=[
            pl.BlockSpec((IMG_LEN, IMG_BLOCK, D), lambda i: (0, i, 0)),
            const_spec((D,)),
            const_spec((D, 3 * D)),
            const_spec((D, D)),
            const_spec((D,)),
            const_spec((D, FF)),
            const_spec((FF, D)),
            const_spec((D, D)),
        ],
        out_specs=pl.BlockSpec((count, D), lambda i: (0, 0)),
        out_shape=jax.ShapeDtypeStruct((count, D), BF),
        scratch_shapes=[
            pltpu.VMEM((IMG_ROWS, 2 * D), BF),
            pltpu.VMEM((count, D), F32),
            pltpu.VMEM((count, D), F32),
        ],
        compiler_params=ROOM,
        cost_estimate=cost(12),
        name="image_tower",
    )(x, g1, wqkv, wout, g2, wup, wdown, wproj)


def pair_mask(lab_ref, pair):
    lab = lab_ref[0, :, PAIR * pair : PAIR * pair + PAIR].astype(F32)
    wide = jnp.broadcast_to(lab, (PAIR, PAIR))
    return wide == wide.T


def text_att_kernel(tok_ref, lab_ref, g1, wqkv, o_all, qkv_all, p_all, h1_all):
    step = pl.program_id(0)
    o_ref, qkv_ref, h1_ref = o_all.at[held_rows()], qkv_all.at[held_rows()], h1_all.at[held_rows()]
    p_ref = p_all.at[pl.ds(2 * step, 2)]
    x = tok_ref[...].astype(F32)
    h1 = (normalize(x) * g1[...].reshape(1, D)).astype(BF)
    h1_ref[...] = h1
    qkv = mm(h1, wqkv[...]).astype(BF)
    qkv_ref[...] = qkv
    low = lax.broadcasted_iota(jnp.int32, (PAIR, PAIR), 1) < HEAD
    for pair in range(2):
        rows = slice(PAIR * pair, PAIR * pair + PAIR)
        mask = pair_mask(lab_ref, pair)
        mask = jnp.concatenate([mask, mask], 0)
        for j in range(HEADS // 2):
            cols = slice(PAIR * j, PAIR * j + PAIR)
            q2 = qkv[rows, PAIR * j : PAIR * j + PAIR] * jnp.asarray(HEAD**-0.5, BF)
            k2 = qkv[rows, D + PAIR * j : D + PAIR * j + PAIR]
            v2 = qkv[rows, 2 * D + PAIR * j : 2 * D + PAIR * j + PAIR]
            zero = jnp.zeros_like(q2)
            q22 = jnp.concatenate([jnp.where(low, q2, zero), jnp.where(low, zero, q2)], 0)
            s = jnp.where(mask, mm_nt(q22, k2), -1e30)
            ex = jnp.exp(s - jnp.max(s, -1, keepdims=True))
            p = (ex * (1.0 / jnp.sum(ex, -1, keepdims=True))).astype(BF)
            p_ref[pair, j] = p
            v22 = jnp.concatenate([jnp.where(low, v2, zero), jnp.where(low, zero, v2)], 0)
            o = mm(jnp.concatenate([p[:PAIR], p[PAIR:]], 1), v22)
            o_ref[rows, cols] = o.astype(BF)


def text_mlp_kernel(
    tok_ref, o_ref, lab_ref, wout, g2, wup, wdown, wproj,
    h2_all, c2_all, gp_all, pu_ref, pb_ref, e_ref, emb_ref, cnt_ref, pt, po,
):
    step = pl.program_id(0)
    h2_ref, c2_ref, gp_ref = h2_all.at[held_rows()], c2_all.at[held_rows()], gp_all.at[held_rows()]
    tok = tok_ref[...]
    o = o_ref[held_rows(), :]
    x1 = tok.astype(F32) + mm(o, wout[...])
    c2 = x1 - row_mean(x1)
    c2_ref[...] = c2
    h2 = (c2 * lax.rsqrt(row_mean(c2 * c2) + EPS) * g2[...].reshape(1, D)).astype(BF)
    h2_ref[...] = h2
    hit = lax.broadcasted_iota(jnp.int32, (CAP_BLOCK, TOK_BLOCK), 0) == lab_ref[0]
    member = jnp.where(hit, 1.0, 0.0)
    caps = pl.ds(pl.multiple_of(step * CAP_BLOCK, CAP_BLOCK), CAP_BLOCK)
    member_b = member.astype(BF)
    pt[caps, :] = mm(member_b, tok)
    po[caps, :] = mm(member_b, o)
    cnt_ref[caps, :] = jnp.broadcast_to(jnp.sum(member, -1, keepdims=True), (CAP_BLOCK, 128))
    for k in range(FF // 512):
        cols = slice(512 * k, 512 * (k + 1))
        u, slope = gelu_parts(mm(h2, wup[:, cols]))
        gp_ref[:, cols] = slope.astype(BF)
        pu_ref[caps, cols] = mm(member_b, u.astype(BF))

    @pl.when(step == pl.num_programs(0) - 1)
    def _():
        total = pt[...] + wide_mm(po[...], wout[...]) + wide_mm(pu_ref[...], wdown[...])
        pooled = (total * (1.0 / cnt_ref[:, 0:1])).astype(BF)
        pb_ref[...] = pooled
        e = mm(pooled, wproj[...])
        e_ref[...] = e
        emb_ref[...] = (e * lax.rsqrt(jnp.sum(e * e, -1, keepdims=True) + EPS)).astype(BF)


def near(v):
    return pltpu.with_memory_space_constraint(v, pltpu.VMEM)


def held_rows():
    return pl.ds(pl.multiple_of(pl.program_id(0) * TOK_BLOCK, TOK_BLOCK), TOK_BLOCK)


def token_rows(width):
    return pl.BlockSpec((TOK_BLOCK, width), lambda i: (i, 0))


def block_of(a, b):
    return pl.BlockSpec((1, a, b), lambda i: (i, 0, 0))


def whole(a, b):
    return pl.BlockSpec((a, b), lambda i: (0, 0))


def text_att(tok, lab, g1, wqkv):
    n = tok.shape[0]
    blocks = n // TOK_BLOCK
    shape = pltpu.VMEM
    return pl.pallas_call(
        text_att_kernel,
        grid=(blocks,),
        in_specs=[token_rows(D), block_of(1, TOK_BLOCK), const_spec((D,)), const_spec((D, 3 * D))],
        out_specs=[VMEM] * 4,
        out_shape=[
            shape((n, D), BF), shape((n, 3 * D), BF), shape((2 * blocks, 3, 2 * PAIR, PAIR), BF), shape((n, D), BF),
        ],
        compiler_params=ROOM,
        cost_estimate=cost(9),
        name="text_att",
    )(tok, lab, g1, wqkv)


def text_mlp(tok, o, lab, wout, g2, wup, wdown, wproj):
    n = tok.shape[0]
    shape = pltpu.VMEM
    return pl.pallas_call(
        text_mlp_kernel,
        grid=(n // TOK_BLOCK,),
        in_specs=[
            token_rows(D), VMEM, block_of(1, TOK_BLOCK),
            const_spec((D, D)), const_spec((D,)), const_spec((D, FF)), const_spec((FF, D)), const_spec((D, D)),
        ],
        out_specs=[VMEM] * 8,
        out_shape=[
            shape((n, D), BF), shape((n, D), F32), shape((n, FF), BF),
            shape((CAPS, FF), F32), shape((CAPS, D), BF), shape((CAPS, D), F32),
            shape((CAPS, D), BF), shape((CAPS, 128), F32),
        ],
        scratch_shapes=[pltpu.VMEM((CAPS, D), F32), pltpu.VMEM((CAPS, D), F32)],
        compiler_params=ROOM,
        cost_estimate=cost(11),
        name="text_mlp",
    )(tok, near(o), lab, wout, g2, wup, wdown, wproj)


def reorder(mine, row):
    return jnp.where(mine & 1 == 1, pltpu.roll(row, 64, 1), row)


def cosine_kernel(denom, scale_ref, mine_ref, emb, images, pair, g_ref, sum_ref):
    mine = mine_ref[0]
    scale = jnp.exp(jnp.full((1, 1), scale_ref[0], F32))
    g = mm_nt(emb[...], images[...])
    g_ref[...] = g
    e = jnp.exp(g * scale)
    eg = e * g
    total = jnp.sum(e, -1, keepdims=True)
    hit = lax.broadcasted_iota(jnp.int32, g.shape, 1) == pair[...]
    own = jnp.sum(jnp.where(hit, g, 0.0), -1, keepdims=True)
    loss = jnp.sum(jnp.log(total) - 2.0 * scale * own, 0, keepdims=True)
    temp = jnp.sum(jnp.sum(eg, -1, keepdims=True) / total - 2.0 * own, 0, keepdims=True)
    n = g.shape[1] // 128
    for k, v in enumerate((jnp.sum(e, 0, keepdims=True), jnp.sum(eg, 0, keepdims=True))):
        for r in range(n):
            sum_ref[pl.ds(k * n + ((mine >> 1) ^ r), 1), :] = reorder(mine, v[:, 128 * r : 128 * (r + 1)])
    lane = lax.broadcasted_iota(jnp.int32, (8, 128), 1)
    sum_ref[2 * n :, :] = jnp.where(lane == 0, loss, jnp.where(lane == 1, temp, 0.0))


def rows_kernel(denom, scale_ref, g_ref, images, pair, dt_ref):
    scale = jnp.exp(jnp.full((1, 1), scale_ref[0], F32))
    g = g_ref[...]
    e = jnp.exp(g * scale)
    hit = lax.broadcasted_iota(jnp.int32, g.shape, 1) == pair[...]
    p = e * (1.0 / jnp.sum(e, -1, keepdims=True))
    dl = jnp.where(hit, p - 2.0, p) * (scale * (1.0 / denom))
    dt_ref[...] = mm(dl.astype(BF), images[...])


def quarter(mine, base, k, rows=48):
    far = (mine & 3) ^ k
    return pl.multiple_of(base + rows * ((far & 1) * 2 + (far >> 1)), 16)


def halves(mine, rows, send_ref, keep_ref, piece):
    for rel in range(8):
        ref = keep_ref if rel < 4 else send_ref
        at = (rel % 4) * rows
        if rows == 48:
            ref[at : at + 48, :] = piece((mine >> 2) ^ rel, 0).astype(BF)
            continue
        for k in range(4):
            ref[pl.ds(quarter(mine, at, k), 48), :] = piece((mine >> 2) ^ rel, k).astype(BF)


def block(acc, at, rows, col=0):
    return acc[pl.ds(pl.multiple_of(at * rows, 16), rows), D * col : D * (col + 1)]


def head_kernel(
    denom, scale_ref, mine_ref, g_ref, images, sums, dt_row, e_ref, pb, cnt, pu, wproj, wdown,
    sd_ref, kd_ref, sp_ref, kp_ref, du_ref, dy_ref, loss_out, temp_out, down, proj,
):
    mine = mine_ref[0]
    scale = jnp.exp(jnp.full((1, 1), scale_ref[0], F32))
    n = g_ref.shape[1] // 128

    def columns(k):
        return jnp.concatenate([reorder(mine, sums[pl.ds(k * n + ((mine >> 1) ^ r), 1), :]) for r in range(n)], 1)

    temp = jnp.sum(jnp.sum(sums[n : 2 * n, :] / sums[0:n, :], 0, keepdims=True), -1, keepdims=True)
    loss = jnp.sum(jnp.sum(jnp.log(sums[0:n, :]), 0, keepdims=True), -1, keepdims=True)
    loss_out[...] = (sums[2 * n : 2 * n + 1, 0:1] + loss) * (1.0 / denom)
    temp_out[...] = (sums[2 * n : 2 * n + 1, 1:2] + temp) * (scale * (1.0 / denom))
    inverse = 1.0 / columns(0)
    dl = jnp.exp(g_ref[...] * scale) * (inverse * (scale * (1.0 / denom)))
    dt = dt_row[...] + mm(dl.astype(BF), images[...])
    e = e_ref[...]
    r = lax.rsqrt(jnp.sum(e * e, -1, keepdims=True) + EPS)
    de = (dt - e * (r * r * jnp.sum(dt * e, -1, keepdims=True))) * r
    de = de.astype(BF)
    dpooled = mm_nt(de, wproj[...])
    dy = dpooled * (1.0 / cnt[:, 0:1])
    dyb = dy.astype(BF)
    du = mm_nt(dyb, wdown[...])
    for i, piece in enumerate(split3(du)):
        for b in range(BLOCKS):
            du_ref[b, CAP_BLOCK * i : CAP_BLOCK * (i + 1), :] = piece[CAP_BLOCK * b : CAP_BLOCK * (b + 1)]
    for i, piece in enumerate(split3(dy)):
        for b in range(BLOCKS):
            dy_ref[b, CAP_BLOCK * i : CAP_BLOCK * (i + 1), :] = piece[CAP_BLOCK * b : CAP_BLOCK * (b + 1)]
    down[...] = mm_tn(jnp.concatenate(split3(pu[...]), 0), jnp.concatenate([dyb, dyb, dyb], 0))
    proj[...] = mm_tn(pb[...], de)
    halves(mine, 192, sd_ref, kd_ref, lambda at, k: block(down, at * 4 + k, 48))
    halves(mine, 48, sp_ref, kp_ref, lambda at, k: block(proj, at, 48))


def mlp_back_kernel(
    mine_ref, lab_ref, h2_all, gp_all, c2_all, du_ref, dy_ref, g2, wup,
    dx_all, dxb_all, send_ref, keep_ref, acc,
):
    step = pl.program_id(0)
    h2_ref, gp_ref, c2_ref = h2_all.at[held_rows()], gp_all.at[held_rows()], c2_all.at[held_rows()]
    dx_ref, dxb_ref = dx_all.at[held_rows()], dxb_all.at[held_rows()]

    @pl.when(step == 0)
    def _():
        acc[...] = jnp.zeros_like(acc)

    hit = lax.broadcasted_iota(jnp.int32, (3 * CAP_BLOCK, TOK_BLOCK), 0) % CAP_BLOCK == lab_ref[0]
    spread = jnp.where(hit, 1.0, 0.0).astype(BF)
    du = mm_tn(spread, du_ref[step])
    dz = (du * gp_ref[...].astype(F32)).astype(BF)
    dy = mm_tn(spread, dy_ref[step])
    dh = mm_nt(dz, wup[...])
    c2 = c2_ref[...]
    r = lax.rsqrt(row_mean(c2 * c2) + EPS)
    unit = c2 * r
    dn = dh * g2[...].reshape(1, D)
    dx = dy + r * (dn - row_mean(dn) - unit * row_mean(dn * unit))
    dx_ref[...] = dx
    dxb_ref[...] = dx.astype(BF)
    h2 = h2_ref[...]
    acc[...] += mm_tn(h2, dz)

    @pl.when(step == pl.num_programs(0) - 1)
    def _():
        halves(mine_ref[0], 192, send_ref, keep_ref, lambda at, k: block(acc, at, 48, k))


def att_core_kernel(qkv_all, p_all, dxb_all, wout, dqkv_all):
    step = pl.program_id(0)
    qkv_ref, dxb_ref, dqkv_ref = qkv_all.at[held_rows()], dxb_all.at[held_rows()], dqkv_all.at[held_rows()]
    p_ref = p_all.at[pl.ds(2 * step, 2)]
    do = mm_nt(dxb_ref[...], wout[...]).astype(BF)
    low = lax.broadcasted_iota(jnp.int32, (PAIR, PAIR), 1) < HEAD
    zero = jnp.zeros((PAIR, PAIR), BF)
    half = HEAD**-0.5

    def twice(v):
        return jnp.concatenate([jnp.where(low, v, zero), jnp.where(low, zero, v)], 0)

    for pair in range(2):
        rows = slice(PAIR * pair, PAIR * pair + PAIR)
        for j in range(HEADS // 2):
            cols = slice(PAIR * j, PAIR * j + PAIR)
            q2 = qkv_ref[rows, PAIR * j : PAIR * j + PAIR]
            k2 = qkv_ref[rows, D + PAIR * j : D + PAIR * j + PAIR]
            v2 = qkv_ref[rows, 2 * D + PAIR * j : 2 * D + PAIR * j + PAIR]
            do2 = twice(do[rows, cols])
            pb = p_ref[pair, j]
            p = pb.astype(F32)
            dp = mm_nt(do2, v2)
            ds = (p * (dp - jnp.sum(dp * p, -1, keepdims=True))).astype(BF)
            dq = mm(jnp.concatenate([ds[:PAIR], ds[PAIR:]], 1), twice(k2)) * half
            dk = mm_tn(ds, twice(q2)) * half
            dv = mm_tn(pb, do2)
            dqkv_ref[rows, PAIR * j : PAIR * j + PAIR] = dq.astype(BF)
            dqkv_ref[rows, D + PAIR * j : D + PAIR * j + PAIR] = dk.astype(BF)
            dqkv_ref[rows, 2 * D + PAIR * j : 2 * D + PAIR * j + PAIR] = dv.astype(BF)


def att_grads_kernel(mine_ref, h1_ref, dqkv_ref, o_ref, dxb_ref, send_ref, keep_ref, acc):
    acc[:, :D] = mm_tn(o_ref[...], dxb_ref[...])
    acc[:, D:] = mm_tn(h1_ref[...], dqkv_ref[...])
    halves(mine_ref[0], 192, send_ref, keep_ref, lambda at, k: block(acc, at, 48, k))


def tok_back_kernel(tok_ref, dqkv_all, dx_all, g1, wqkv, gtok_ref):
    dqkv_ref, dx_ref = dqkv_all.at[held_rows()], dx_all.at[held_rows()]
    x = tok_ref[...].astype(F32)
    centre = x - row_mean(x)
    r = lax.rsqrt(row_mean(centre * centre) + EPS)
    unit = centre * r
    dn = mm_nt(dqkv_ref[...], wqkv[...]) * g1[...].reshape(1, D)
    gtok_ref[...] = dx_ref[...] + r * (dn - row_mean(dn) - unit * row_mean(dn * unit))


def gain_of(grad, weight, gain):
    high, mid, _ = split3(grad * weight.astype(F32))
    ones = jnp.ones((8, grad.shape[1]), BF)
    total = mm_nt(ones, high) + mm_nt(ones, mid)
    return total[0:1] / gain.reshape(1, D)


def arrived(mine_ref, own, other, rows):
    for rel in range(8):
        src = own if rel < 4 else other
        yield (mine_ref[0] >> 2) ^ rel, src, (rel % 4) * rows


def spread_mlp_kernel(mine_ref, own, other, wup, g2, down_ref, up_ref, proj_ref, gain_ref):
    for at, src, row in arrived(mine_ref, own, other, 432):
        rows = pl.ds(pl.multiple_of(at * 48, 16), 48)
        for k in range(4):
            part = quarter(mine_ref[0], row, k, 96)
            down_ref[pl.ds(pl.multiple_of(at * 192 + 48 * k, 16), 48), :] = src[pl.ds(part, 48), :].astype(F32)
            up_ref[rows, D * k : D * (k + 1)] = src[pl.ds(pl.multiple_of(part + 48, 16), 48), :].astype(F32)
        proj_ref[rows, :] = src[row + 384 : row + 432, :].astype(F32)
    gain_ref[...] = gain_of(up_ref[...], wup[...], g2[...]).reshape(D)


def spread_att_kernel(mine_ref, own, other, wqkv, g1, out_ref, qkv_ref, gain_ref):
    for at, src, row in arrived(mine_ref, own, other, 192):
        rows = pl.ds(pl.multiple_of(at * 48, 16), 48)
        out_ref[rows, :] = src[pl.ds(quarter(mine_ref[0], row, 0), 48), :].astype(F32)
        for k in range(3):
            qkv_ref[rows, D * k : D * (k + 1)] = src[pl.ds(quarter(mine_ref[0], row, k + 1), 48), :].astype(F32)
    gain_ref[...] = gain_of(qkv_ref[...], wqkv[...], g1[...]).reshape(D)


def simple(kernel, outs, scratch=(), smem=0, us=3, name=None, held=(), held_out=True):
    def call(*args):
        args = [near(v) if i in held else v for i, v in enumerate(args)]
        return pl.pallas_call(
            kernel,
            in_specs=[SMEM] * smem + [VMEM] * (len(args) - smem),
            out_specs=[VMEM] * len(outs),
            out_shape=[(pltpu.VMEM if held_out else jax.ShapeDtypeStruct)(s, t) for s, t in outs],
            scratch_shapes=list(scratch),
            compiler_params=ROOM,
            cost_estimate=cost(us),
            name=name,
        )(*args)

    return call


def mlp_back(mine, lab, h2, gp, c2, du, dy, g2, wup):
    n = h2.shape[0]
    shape = pltpu.VMEM
    return pl.pallas_call(
        mlp_back_kernel,
        grid=(n // TOK_BLOCK,),
        in_specs=[SMEM, block_of(1, TOK_BLOCK)] + [VMEM] * 5 + [const_spec((D,)), const_spec((D, FF))],
        out_specs=[VMEM] * 4,
        out_shape=[shape((n, D), F32), shape((n, D), BF), shape((768, D), BF), shape((768, D), BF)],
        scratch_shapes=[pltpu.VMEM((D, FF), F32)],
        compiler_params=ROOM,
        cost_estimate=cost(9),
        name="mlp_back",
    )(mine, lab, near(h2), near(gp), near(c2), near(du), near(dy), g2, wup)


def att_core(qkv, p, dxb, wout):
    n = dxb.shape[0]
    return pl.pallas_call(
        att_core_kernel,
        grid=(n // TOK_BLOCK,),
        in_specs=[VMEM, VMEM, VMEM, const_spec((D, D))],
        out_specs=VMEM,
        out_shape=pltpu.VMEM((n, 3 * D), BF),
        compiler_params=ROOM,
        cost_estimate=cost(10),
        name="att_core",
    )(near(qkv), near(p), near(dxb), wout)


def att_grads(mine, h1, dqkv, o, dxb):
    outs = [((768, D), BF)] * 2
    scratch = [pltpu.VMEM((D, 4 * D), F32)]
    return simple(att_grads_kernel, outs, scratch, smem=1, us=4, name="att_grads", held=(1, 2, 3, 4))(mine, h1, dqkv, o, dxb)


def tok_back(tok, dqkv, dx, g1, wqkv):
    n = tok.shape[0]
    return pl.pallas_call(
        tok_back_kernel,
        grid=(n // TOK_BLOCK,),
        in_specs=[token_rows(D), VMEM, VMEM, const_spec((D,)), const_spec((D, 3 * D))],
        out_specs=token_rows(D),
        out_shape=jax.ShapeDtypeStruct((n, D), F32),
        compiler_params=ROOM,
        cost_estimate=cost(4),
        name="tok_back",
    )(tok, near(dqkv), near(dx), g1, wqkv)


AXES = ("dp", "replica")


def swap(v, mask):
    return lax.ppermute(v, AXES, [(i, i ^ mask) for i in range(32)])


def plane(parts):
    return [swap(parts[m], 2 * m) for m in (1, 2, 3)]


def column(parts):
    return [swap(parts[m], 8 * m) for m in (1, 2, 3)]


def total_of(own, got):
    v = [own.astype(F32)] + [x.astype(F32) for x in got]
    return v[0] + v[1] if len(v) == 2 else (v[0] + v[1]) + (v[2] + v[3])


def added(own, got):
    return total_of(own, got).astype(BF)


def joined(own, got):
    return jnp.concatenate([own] + got, 0)


def shards(
    devices, tuned,
    text_tokens, segment_ids, pair_index, image_tokens,
    img_ln1, img_qkv, img_out, img_ln2, img_up, img_down, img_proj,
    txt_ln1, txt_qkv, txt_out, txt_ln2, txt_up, txt_down, txt_proj, log_scale,
):
    total = CAPS * devices
    denom = 2.0 * total
    row_of = jnp.arange(segment_ids.shape[0], dtype=jnp.int32) % (TOK_BLOCK // segment_ids.shape[1])
    lab = (segment_ids + PACK * row_of[:, None]).reshape(BLOCKS, 1, TOK_BLOCK)
    pair = pair_index
    if tuned:
        index = lax.axis_index(AXES)
        mine = ((index & 1) * 16 + ((index >> 1) & 3) * 4 + (index >> 3)).astype(jnp.int32).reshape(1)
        owner, row = pair // CAPS, pair % CAPS
        pair = (((owner & 1) * 16 + ((owner >> 1) & 3) * 4 + (owner >> 3)) ^ mine) * CAPS + row
    else:
        mine = jnp.zeros((1,), jnp.int32)
    pair = pair.reshape(CAPS, 1)
    lab, pair = lax.optimization_barrier((lab, pair))
    emb = image_tower(
        jnp.transpose(image_tokens, (1, 0, 2)), img_ln1, img_qkv, img_out, img_ln2, img_up, img_down, img_proj
    )
    if tuned:
        near = joined(emb, column([emb] * 4))
        o, qkv, p, h1 = text_att(text_tokens, lab, txt_ln1, txt_qkv)
        o, near = lax.optimization_barrier((o, near))
        got = plane([near] * 4)
    else:
        o, qkv, p, h1 = text_att(text_tokens, lab, txt_ln1, txt_qkv)
    h2, c2, gp, pu, pb, e, temb, cnt = text_mlp(text_tokens, o, lab, txt_out, txt_ln2, txt_up, txt_down, txt_proj)
    if tuned:
        near, got, temb = lax.optimization_barrier((near, got, temb))
        near = joined(near, got)
        images = joined(near, [swap(near, 1)])
    else:
        images = lax.all_gather(emb, AXES, axis=0, tiled=True)
    lines = total // 128
    g, sums = simple(
        functools.partial(cosine_kernel, denom),
        [((CAPS, total), F32), ((2 * lines + 8, 128), F32)],
        smem=2,
        us=3,
        name="cosine",
        held=(3,),
    )(log_scale, mine, temb, images, pair)
    (dt_row,) = simple(functools.partial(rows_kernel, denom), [((CAPS, D), F32)], smem=1, us=2, name="rows", held=(2,))(
        log_scale, g, images, pair
    )
    if tuned:
        sums = total_of(sums, [swap(sums, 1)])
        sums = total_of(sums, plane([sums] * 4))
        sums = total_of(sums, [swap(sums, 8)])
        sums = total_of(sums, [swap(sums, 16)])
    else:
        sums = lax.psum(sums, AXES)
    send_d, keep_d, send_p, keep_p, du, dy, loss, temp = simple(
        functools.partial(head_kernel, denom),
        [
            ((768, D), BF), ((768, D), BF), ((192, D), BF), ((192, D), BF),
            ((BLOCKS, 48, FF), BF), ((BLOCKS, 48, D), BF), ((1, 1), F32), ((1, 1), F32),
        ],
        [pltpu.VMEM((FF, D), F32), pltpu.VMEM((D, D), F32)],
        smem=2,
        us=5,
        name="head_back",
        held=(3, 4),
    )(log_scale, mine, g, images, sums, dt_row, e, pb, cnt, pu, txt_proj, txt_down)
    dx, dxb, send_u, keep_u = mlp_back(mine, lab, h2, gp, c2, du, dy, txt_ln2, txt_up)

    def mlp_parts(d, u, p):
        both = jnp.concatenate([d.reshape(4, 4, 48, D), u.reshape(4, 4, 48, D)], 2).reshape(4, 384, D)
        return jnp.concatenate([both, p.reshape(4, 48, D)], 1)

    def spread_mlp(own, other):
        outs = [((FF, D), F32), ((D, FF), F32), ((D, D), F32), ((D,), F32)]
        return simple(spread_mlp_kernel, outs, smem=1, us=4, name="spread_mlp", held=(1, 2), held_out=False)(mine, own, other, txt_up, txt_ln2)

    def spread_att(own, other):
        outs = [((D, D), F32), ((D, 3 * D), F32), ((D,), F32)]
        return simple(spread_att_kernel, outs, smem=1, us=4, name="spread_att", held=(1, 2), held_out=False)(mine, own, other, txt_qkv, txt_ln1)

    if not tuned:
        dqkv = att_core(qkv, p, dxb, txt_out)
        send_a, keep_a = att_grads(mine, h1, dqkv, o, dxb)
        grad_tokens = tok_back(text_tokens, dqkv, dx, txt_ln1, txt_qkv)
        sums = [keep_d, send_d, keep_u, send_u, keep_a, send_a, keep_p, send_p]
        d, d2, u, u2, a, a2, p, p2 = [v.astype(BF) for v in lax.psum([v.astype(F32) for v in sums], AXES)]
        grad_down, grad_up, grad_proj, gain2 = spread_mlp(
            mlp_parts(d, u, p).reshape(1728, D), mlp_parts(d2, u2, p2).reshape(1728, D)
        )
        grad_out, grad_qkv, gain1 = spread_att(a, a2)
    else:
        d = added(keep_d, [swap(send_d, 1)])
        pr = added(keep_p, [swap(send_p, 1)])
        m = mlp_parts(d, added(keep_u, [swap(send_u, 1)]), pr)
        dxb, m = lax.optimization_barrier((dxb, m))
        got = plane(m)
        dqkv = att_core(qkv, p, dxb, txt_out)
        got, dqkv = lax.optimization_barrier((got, dqkv))
        m = added(m[0], got)
        m, dqkv = lax.optimization_barrier((m, dqkv))
        got = swap(m[192:], 8)
        send_a, keep_a = att_grads(mine, h1, dqkv, o, dxb)
        got, send_a, keep_a = lax.optimization_barrier((got, send_a, keep_a))
        m = added(joined(m[:192], [m[384:]]), [got])
        got = swap(m[96:], 16)
        a = added(keep_a, [swap(send_a, 1)]).reshape(4, 192, D)
        got, a = lax.optimization_barrier((got, a))
        m = added(joined(m[:96], [m[192:]]), [got])
        far = swap(m[:96], 16)
        got_a = plane(a)
        dqkv, a, m = lax.optimization_barrier((dqkv, a, m))
        grad_tokens = tok_back(text_tokens, dqkv, dx, txt_ln1, txt_qkv)
        far, grad_tokens = lax.optimization_barrier((far, grad_tokens))
        got_a, grad_tokens = lax.optimization_barrier((got_a, grad_tokens))
        m = joined(m[:96], [far, m[96:]])
        m = joined(m[:192], [swap(m[:192], 8), m[192:]])
        a = added(a[0], got_a)
        got_m = plane([m] * 4)
        a = added(a[:96], [swap(a[96:], 8)])
        a = added(a[:48], [swap(a[48:], 16)])
        a, got_m[0], got_m[1] = lax.optimization_barrier((a, got_m[0], got_m[1]))
        a = joined(a, [swap(a, 16)])
        a = joined(a, [swap(a, 8)])
        got_m, a = lax.optimization_barrier((got_m, a))
        got_a = plane([a] * 4)
        m = joined(m, got_m)
        grad_down, grad_up, grad_proj, gain2 = spread_mlp(m, swap(m, 1))
        got_a, grad_up = lax.optimization_barrier((got_a, grad_up))
        a = joined(a, got_a)
        grad_out, grad_qkv, gain1 = spread_att(a, swap(a, 1))
    return (
        loss.reshape(1), grad_tokens, gain1, grad_qkv, grad_out, gain2,
        grad_up, grad_down, grad_proj, temp.reshape(1),
    )


def solution(mesh):
    both = ("dp", "replica")
    devices = mesh.shape["dp"] * mesh.shape["replica"]
    tuned = (mesh.shape["dp"], mesh.shape["replica"]) == (8, 4)
    rows = P(both, None)
    return jax.shard_map(
        functools.partial(shards, devices, tuned),
        mesh=mesh,
        in_specs=(rows, rows, P(both), P(both, None, None)) + (P(),) * 15,
        out_specs=(P(), rows) + (P(),) * 8,
        check_vma=False,
    )
```

```python
import functools
import math

import jax
import jax.numpy as jnp
from jax import lax
from jax.experimental import pallas as pl
from jax.experimental.pallas import tpu as pltpu
from jax.sharding import PartitionSpec as P

D = 384
HEADS = 6
HEAD = 64
FF = 1536
IMG_LEN = 50
PACK = 4
CAPS = 64
TOK_BLOCK = 256
CAP_BLOCK = 16
BLOCKS = 4
PAIR = 128
IMG_BLOCK = 16
IMG_ROWS = IMG_BLOCK * IMG_LEN
EPS = 1e-06

SMEM = pl.BlockSpec(memory_space=pltpu.SMEM)
VMEM = pl.BlockSpec(memory_space=pltpu.VMEM)
ROOM = pltpu.CompilerParams(vmem_limit_bytes=24 * 2**20)

BF = jnp.bfloat16
F32 = jnp.float32
GELU_K = math.sqrt(2.0 / math.pi)
GELU_C = 0.044715


def mm(a, b):
    return lax.dot_general(a, b, (((1,), (0,)), ((), ())), preferred_element_type=F32)


def mm_nt(a, b):
    return lax.dot_general(a, b, (((1,), (1,)), ((), ())), preferred_element_type=F32)


def mm_tn(a, b):
    return lax.dot_general(a, b, (((0,), (0,)), ((), ())), preferred_element_type=F32)


def row_mean(v):
    return jnp.sum(v, -1, keepdims=True) * (1.0 / D)


def normalize(v):
    centre = v - row_mean(v)
    return centre * lax.rsqrt(row_mean(centre * centre) + EPS)


def split3(v):
    high = v.astype(BF)
    rest = v - high.astype(F32)
    mid = rest.astype(BF)
    low = (rest - mid.astype(F32)).astype(BF)
    return high, mid, low


def wide_mm(v, w):
    high, mid, low = split3(v)
    n = v.shape[0]
    out = mm(jnp.concatenate([high, mid, low], 0), w)
    return out[:n] + out[n : 2 * n] + out[2 * n :]


def gelu_parts(z):
    z2 = z * z
    t = jnp.tanh(z * (z2 * (GELU_K * GELU_C) + GELU_K))
    hp = t * 0.5 + 0.5
    u = z * hp
    slope = hp + (u * (1.0 - hp)) * (z2 * (6.0 * GELU_K * GELU_C) + 2.0 * GELU_K)
    return u, slope


def lanes_head(shape):
    return lax.broadcasted_iota(jnp.int32, shape, len(shape) - 1) // HEAD


def image_kernel(x_ref, g1, wqkv, wout, g2, wup, wdown, wproj, emb_ref, kv, x0, att):
    step = pl.program_id(0)
    gain = g1[...].reshape(1, D)
    for c in range(2):
        x = x_ref[IMG_LEN // 2 * c : IMG_LEN // 2 * (c + 1)].astype(F32).reshape(IMG_ROWS // 2, D)
        h = (normalize(x) * gain).astype(BF)
        kv[IMG_ROWS // 2 * c : IMG_ROWS // 2 * (c + 1), :] = mm(h, wqkv[:, D:]).astype(BF)
        if c == 0:
            x0[pl.ds(pl.multiple_of(step * IMG_BLOCK, IMG_BLOCK), IMG_BLOCK), :] = x[:IMG_BLOCK]
            h0 = h[:IMG_BLOCK]
    q = mm(h0, wqkv[:, :D]).astype(BF).astype(F32) * (HEAD**-0.5)
    head = lanes_head((IMG_BLOCK, D))
    queries = HEADS * IMG_BLOCK
    rows = lax.broadcasted_iota(jnp.int32, (queries, IMG_ROWS), 0)
    cols = lax.broadcasted_iota(jnp.int32, (queries, IMG_ROWS), 1)
    own = cols % IMG_BLOCK == rows % IMG_BLOCK
    q6 = jnp.concatenate([jnp.where(head == h, q, 0.0) for h in range(HEADS)], 0)
    s = mm_nt(q6.astype(BF), kv[:, :D])
    s = jnp.where(own, s, -1e30)
    e = jnp.exp(s - jnp.max(s, -1, keepdims=True))
    p = (e * (1.0 / jnp.sum(e, -1, keepdims=True))).astype(BF)
    r = mm(p, kv[:, D:])
    o = jnp.where(head == 0, r[0:IMG_BLOCK], 0.0)
    for h in range(1, HEADS):
        o = jnp.where(head == h, r[IMG_BLOCK * h : IMG_BLOCK * (h + 1)], o)
    att[pl.ds(pl.multiple_of(step * IMG_BLOCK, IMG_BLOCK), IMG_BLOCK), :] = o

    @pl.when(step == pl.num_programs(0) - 1)
    def _():
        x1 = x0[...] + mm(att[...].astype(BF), wout[...])
        h2 = (normalize(x1) * g2[...].reshape(1, D)).astype(BF)
        u, _ = gelu_parts(mm(h2, wup[...]))
        y = x1 + mm(u.astype(BF), wdown[...])
        e = mm(y.astype(BF), wproj[...])
        emb_ref[...] = (e * lax.rsqrt(jnp.sum(e * e, -1, keepdims=True) + EPS)).astype(BF)


def near(v):
    return pltpu.with_memory_space_constraint(v, pltpu.VMEM)


def away(v):
    return pltpu.with_memory_space_constraint(v, pltpu.HBM)


def cost(us):
    return pl.CostEstimate(flops=int(us * 1e9), bytes_accessed=int(us * 3e6), transcendentals=0)


def const_spec(shape):
    zeros = (0,) * len(shape)
    return pl.BlockSpec(shape, lambda *_: zeros, pipeline_mode=pl.Buffered(1))


def image_tower(x, g1, wqkv, wout, g2, wup, wdown, wproj):
    count = x.shape[1]
    return pl.pallas_call(
        image_kernel,
        grid=(count // IMG_BLOCK,),
        in_specs=[
            pl.BlockSpec((IMG_LEN, IMG_BLOCK, D), lambda i: (0, i, 0)),
            const_spec((D,)),
            const_spec((D, 3 * D)),
            const_spec((D, D)),
            const_spec((D,)),
            const_spec((D, FF)),
            const_spec((FF, D)),
            const_spec((D, D)),
        ],
        out_specs=pl.BlockSpec((count, D), lambda i: (0, 0)),
        out_shape=jax.ShapeDtypeStruct((count, D), BF),
        scratch_shapes=[
            pltpu.VMEM((IMG_ROWS, 2 * D), BF),
            pltpu.VMEM((count, D), F32),
            pltpu.VMEM((count, D), F32),
        ],
        compiler_params=ROOM,
        cost_estimate=cost(12),
        name="image_tower",
    )(*[away(v) for v in (x, g1, wqkv, wout, g2, wup, wdown, wproj)])


def pair_mask(lab_ref, pair):
    lab = lab_ref[0, :, PAIR * pair : PAIR * pair + PAIR].astype(F32)
    wide = jnp.broadcast_to(lab, (PAIR, PAIR))
    return wide == wide.T


def text_att_kernel(tok_ref, lab_ref, g1, wqkv, o_all, o_ref, qkv_ref, p_ref, h1_ref):
    x = tok_ref[...].astype(F32)
    h1 = (normalize(x) * g1[...].reshape(1, D)).astype(BF)
    h1_ref[...] = h1
    qkv = mm(h1, wqkv[...]).astype(BF)
    qkv_ref[...] = qkv
    low = lax.broadcasted_iota(jnp.int32, (PAIR, PAIR), 1) < HEAD
    for pair in range(2):
        rows = slice(PAIR * pair, PAIR * pair + PAIR)
        mask = pair_mask(lab_ref, pair)
        mask = jnp.concatenate([mask, mask], 0)
        for j in range(HEADS // 2):
            cols = slice(PAIR * j, PAIR * j + PAIR)
            q2 = qkv[rows, PAIR * j : PAIR * j + PAIR] * jnp.asarray(HEAD**-0.5, BF)
            k2 = qkv[rows, D + PAIR * j : D + PAIR * j + PAIR]
            v2 = qkv[rows, 2 * D + PAIR * j : 2 * D + PAIR * j + PAIR]
            zero = jnp.zeros_like(q2)
            q22 = jnp.concatenate([jnp.where(low, q2, zero), jnp.where(low, zero, q2)], 0)
            s = jnp.where(mask, mm_nt(q22, k2), -1e30)
            ex = jnp.exp(s - jnp.max(s, -1, keepdims=True))
            p = (ex * (1.0 / jnp.sum(ex, -1, keepdims=True))).astype(BF)
            p_ref[pair, j] = p
            v22 = jnp.concatenate([jnp.where(low, v2, zero), jnp.where(low, zero, v2)], 0)
            o = mm(jnp.concatenate([p[:PAIR], p[PAIR:]], 1), v22)
            o_ref[rows, cols] = o.astype(BF)
    o_all[held_rows(), :] = o_ref[...]


def text_mlp_kernel(
    tok_ref, o_ref, lab_ref, wout, g2, wup, wdown, wproj,
    h2_ref, c2_ref, gp_ref, pu_ref, pb_ref, e_ref, emb_ref, cnt_ref, pt, po,
):
    step = pl.program_id(0)
    tok = tok_ref[...]
    o = o_ref[held_rows(), :]
    x1 = tok.astype(F32) + mm(o, wout[...])
    c2 = x1 - row_mean(x1)
    c2_ref[...] = c2
    h2 = (c2 * lax.rsqrt(row_mean(c2 * c2) + EPS) * g2[...].reshape(1, D)).astype(BF)
    h2_ref[...] = h2
    hit = lax.broadcasted_iota(jnp.int32, (CAP_BLOCK, TOK_BLOCK), 0) == lab_ref[0]
    member = jnp.where(hit, 1.0, 0.0)
    caps = pl.ds(pl.multiple_of(step * CAP_BLOCK, CAP_BLOCK), CAP_BLOCK)
    member_b = member.astype(BF)
    pt[caps, :] = mm(member_b, tok)
    po[caps, :] = mm(member_b, o)
    cnt_ref[caps, :] = jnp.broadcast_to(jnp.sum(member, -1, keepdims=True), (CAP_BLOCK, 128))
    for k in range(FF // 512):
        cols = slice(512 * k, 512 * (k + 1))
        u, slope = gelu_parts(mm(h2, wup[:, cols]))
        gp_ref[:, cols] = slope.astype(BF)
        pu_ref[caps, cols] = mm(member_b, u.astype(BF))

    @pl.when(step == pl.num_programs(0) - 1)
    def _():
        total = pt[...] + wide_mm(po[...], wout[...]) + wide_mm(pu_ref[...], wdown[...])
        pooled = (total * (1.0 / cnt_ref[:, 0:1])).astype(BF)
        pb_ref[...] = pooled
        e = mm(pooled, wproj[...])
        e_ref[...] = e
        emb_ref[...] = (e * lax.rsqrt(jnp.sum(e * e, -1, keepdims=True) + EPS)).astype(BF)


def held_rows():
    return pl.ds(pl.multiple_of(pl.program_id(0) * TOK_BLOCK, TOK_BLOCK), TOK_BLOCK)


def token_rows(width):
    return pl.BlockSpec((TOK_BLOCK, width), lambda i: (i, 0))


def block_of(a, b):
    return pl.BlockSpec((1, a, b), lambda i: (i, 0, 0))


def whole(a, b):
    return pl.BlockSpec((a, b), lambda i: (0, 0))


def text_att(tok, lab, g1, wqkv):
    n = tok.shape[0]
    blocks = n // TOK_BLOCK
    shape = pltpu.HBM
    return pl.pallas_call(
        text_att_kernel,
        grid=(blocks,),
        in_specs=[token_rows(D), block_of(1, TOK_BLOCK), const_spec((D,)), const_spec((D, 3 * D))],
        out_specs=[
            VMEM,
            token_rows(D),
            token_rows(3 * D),
            pl.BlockSpec((2, 3, 2 * PAIR, PAIR), lambda i: (i, 0, 0, 0)),
            token_rows(D),
        ],
        out_shape=[
            pltpu.VMEM((n, D), BF), shape((n, D), BF), shape((n, 3 * D), BF),
            shape((2 * blocks, 3, 2 * PAIR, PAIR), BF), shape((n, D), BF),
        ],
        compiler_params=ROOM,
        cost_estimate=cost(9),
        name="text_att",
    )(away(tok), lab, g1, away(wqkv))


def text_mlp(tok, o, lab, wout, g2, wup, wdown, wproj):
    n = tok.shape[0]
    shape = pltpu.VMEM
    return pl.pallas_call(
        text_mlp_kernel,
        grid=(n // TOK_BLOCK,),
        in_specs=[
            token_rows(D), VMEM, block_of(1, TOK_BLOCK),
            const_spec((D, D)), const_spec((D,)), const_spec((D, FF)), const_spec((FF, D)), const_spec((D, D)),
        ],
        out_specs=[token_rows(D), token_rows(D), token_rows(FF)] + [VMEM] * 5,
        out_shape=[
            pltpu.HBM((n, D), BF), pltpu.HBM((n, D), F32), pltpu.HBM((n, FF), BF),
            shape((CAPS, FF), F32), shape((CAPS, D), BF), shape((CAPS, D), F32),
            shape((CAPS, D), BF), shape((CAPS, 128), F32),
        ],
        scratch_shapes=[pltpu.VMEM((CAPS, D), F32), pltpu.VMEM((CAPS, D), F32)],
        compiler_params=ROOM,
        cost_estimate=cost(11),
        name="text_mlp",
    )(tok, near(o), lab, wout, g2, wup, wdown, wproj)


def reorder(mine, row):
    return jnp.where(mine & 1 == 1, pltpu.roll(row, 64, 1), row)


def cosine_kernel(denom, scale_ref, mine_ref, emb, own, other, pair, g_ref, sum_ref):
    mine = mine_ref[0]
    scale = jnp.exp(jnp.full((1, 1), scale_ref[0], F32))
    g = jnp.concatenate([mm_nt(emb[...], own[...]), mm_nt(emb[...], other[...])], 1)
    g_ref[...] = g
    e = jnp.exp(g * scale)
    eg = e * g
    total = jnp.sum(e, -1, keepdims=True)
    hit = lax.broadcasted_iota(jnp.int32, g.shape, 1) == pair[...]
    own = jnp.sum(jnp.where(hit, g, 0.0), -1, keepdims=True)
    loss = jnp.sum(jnp.log(total) - 2.0 * scale * own, 0, keepdims=True)
    temp = jnp.sum(jnp.sum(eg, -1, keepdims=True) / total - 2.0 * own, 0, keepdims=True)
    n = g.shape[1] // 128
    for k, v in enumerate((jnp.sum(e, 0, keepdims=True), jnp.sum(eg, 0, keepdims=True))):
        for r in range(n):
            sum_ref[pl.ds(k * n + ((mine >> 1) ^ r), 1), :] = reorder(mine, v[:, 128 * r : 128 * (r + 1)])
    lane = lax.broadcasted_iota(jnp.int32, (8, 128), 1)
    sum_ref[2 * n :, :] = jnp.where(lane == 0, loss, jnp.where(lane == 1, temp, 0.0))


def times_images(dl, own, other):
    half = dl.shape[1] // 2
    return mm(dl[:, :half], own[...]) + mm(dl[:, half:], other[...])


def rows_kernel(denom, scale_ref, g_ref, own, other, pair, dt_ref):
    scale = jnp.exp(jnp.full((1, 1), scale_ref[0], F32))
    g = g_ref[...]
    e = jnp.exp(g * scale)
    hit = lax.broadcasted_iota(jnp.int32, g.shape, 1) == pair[...]
    p = e * (1.0 / jnp.sum(e, -1, keepdims=True))
    dl = jnp.where(hit, p - 2.0, p) * (scale * (1.0 / denom))
    dt_ref[...] = times_images(dl.astype(BF), own, other)


def quarter(mine, base, k, rows=48):
    far = (mine & 3) ^ k
    return pl.multiple_of(base + rows * ((far & 1) * 2 + (far >> 1)), 16)


def halves(mine, rows, send_ref, keep_ref, piece):
    for rel in range(8):
        ref = keep_ref if rel < 4 else send_ref
        at = (rel % 4) * rows
        if rows == 48:
            ref[at : at + 48, :] = piece((mine >> 2) ^ rel, 0).astype(BF)
            continue
        for k in range(4):
            ref[pl.ds(quarter(mine, at, k), 48), :] = piece((mine >> 2) ^ rel, k).astype(BF)


def block(acc, at, rows, col=0):
    return acc[pl.ds(pl.multiple_of(at * rows, 16), rows), D * col : D * (col + 1)]


def head_kernel(
    denom, scale_ref, mine_ref, g_ref, own, other, sums, dt_row, e_ref, pb, cnt, pu, wproj, wdown,
    sd_ref, kd_ref, sp_ref, kp_ref, du_ref, dy_ref, loss_out, temp_out, down, proj,
):
    mine = mine_ref[0]
    scale = jnp.exp(jnp.full((1, 1), scale_ref[0], F32))
    n = g_ref.shape[1] // 128

    def columns(k):
        return jnp.concatenate([reorder(mine, sums[pl.ds(k * n + ((mine >> 1) ^ r), 1), :]) for r in range(n)], 1)

    temp = jnp.sum(jnp.sum(sums[n : 2 * n, :] / sums[0:n, :], 0, keepdims=True), -1, keepdims=True)
    loss = jnp.sum(jnp.sum(jnp.log(sums[0:n, :]), 0, keepdims=True), -1, keepdims=True)
    loss_out[...] = (sums[2 * n : 2 * n + 1, 0:1] + loss) * (1.0 / denom)
    temp_out[...] = (sums[2 * n : 2 * n + 1, 1:2] + temp) * (scale * (1.0 / denom))
    inverse = 1.0 / columns(0)
    dl = jnp.exp(g_ref[...] * scale) * (inverse * (scale * (1.0 / denom)))
    dt = dt_row[...] + times_images(dl.astype(BF), own, other)
    e = e_ref[...]
    r = lax.rsqrt(jnp.sum(e * e, -1, keepdims=True) + EPS)
    de = (dt - e * (r * r * jnp.sum(dt * e, -1, keepdims=True))) * r
    de = de.astype(BF)
    dpooled = mm_nt(de, wproj[...])
    dy = dpooled * (1.0 / cnt[:, 0:1])
    dyb = dy.astype(BF)
    du = mm_nt(dyb, wdown[...])
    for i, piece in enumerate(split3(du)):
        for b in range(BLOCKS):
            du_ref[b, CAP_BLOCK * i : CAP_BLOCK * (i + 1), :] = piece[CAP_BLOCK * b : CAP_BLOCK * (b + 1)]
    for i, piece in enumerate(split3(dy)):
        for b in range(BLOCKS):
            dy_ref[b, CAP_BLOCK * i : CAP_BLOCK * (i + 1), :] = piece[CAP_BLOCK * b : CAP_BLOCK * (b + 1)]
    down[...] = mm_tn(jnp.concatenate(split3(pu[...]), 0), jnp.concatenate([dyb, dyb, dyb], 0))
    proj[...] = mm_tn(pb[...], de)
    halves(mine, 192, sd_ref, kd_ref, lambda at, k: block(down, at * 4 + k, 48))
    halves(mine, 48, sp_ref, kp_ref, lambda at, k: block(proj, at, 48))


def mlp_back_kernel(
    mine_ref, lab_ref, h2_all, gp_all, c2_all, du_ref, dy_ref, g2, wup,
    dx_all, dxb_all, send_ref, keep_ref, acc,
):
    step = pl.program_id(0)
    h2_ref, gp_ref, c2_ref = h2_all.at[held_rows()], gp_all.at[held_rows()], c2_all.at[held_rows()]
    dx_ref, dxb_ref = dx_all.at[held_rows()], dxb_all.at[held_rows()]

    @pl.when(step == 0)
    def _():
        acc[...] = jnp.zeros_like(acc)

    hit = lax.broadcasted_iota(jnp.int32, (3 * CAP_BLOCK, TOK_BLOCK), 0) % CAP_BLOCK == lab_ref[0]
    spread = jnp.where(hit, 1.0, 0.0).astype(BF)
    du = mm_tn(spread, du_ref[step])
    dz = (du * gp_ref[...].astype(F32)).astype(BF)
    dy = mm_tn(spread, dy_ref[step])
    dh = mm_nt(dz, wup[...])
    c2 = c2_ref[...]
    r = lax.rsqrt(row_mean(c2 * c2) + EPS)
    unit = c2 * r
    dn = dh * g2[...].reshape(1, D)
    dx = dy + r * (dn - row_mean(dn) - unit * row_mean(dn * unit))
    dx_ref[...] = dx
    dxb_ref[...] = dx.astype(BF)
    h2 = h2_ref[...]
    acc[...] += mm_tn(h2, dz)

    @pl.when(step == pl.num_programs(0) - 1)
    def _():
        halves(mine_ref[0], 192, send_ref, keep_ref, lambda at, k: block(acc, at, 48, k))


def att_core_kernel(qkv_all, p_all, dxb_all, wout, dqkv_all):
    step = pl.program_id(0)
    qkv_ref, dxb_ref, dqkv_ref = qkv_all.at[held_rows()], dxb_all.at[held_rows()], dqkv_all.at[held_rows()]
    p_ref = p_all.at[pl.ds(2 * step, 2)]
    do = mm_nt(dxb_ref[...], wout[...]).astype(BF)
    low = lax.broadcasted_iota(jnp.int32, (PAIR, PAIR), 1) < HEAD
    zero = jnp.zeros((PAIR, PAIR), BF)
    half = HEAD**-0.5

    def twice(v):
        return jnp.concatenate([jnp.where(low, v, zero), jnp.where(low, zero, v)], 0)

    for pair in range(2):
        rows = slice(PAIR * pair, PAIR * pair + PAIR)
        for j in range(HEADS // 2):
            cols = slice(PAIR * j, PAIR * j + PAIR)
            q2 = qkv_ref[rows, PAIR * j : PAIR * j + PAIR]
            k2 = qkv_ref[rows, D + PAIR * j : D + PAIR * j + PAIR]
            v2 = qkv_ref[rows, 2 * D + PAIR * j : 2 * D + PAIR * j + PAIR]
            do2 = twice(do[rows, cols])
            pb = p_ref[pair, j]
            p = pb.astype(F32)
            dp = mm_nt(do2, v2)
            ds = (p * (dp - jnp.sum(dp * p, -1, keepdims=True))).astype(BF)
            dq = mm(jnp.concatenate([ds[:PAIR], ds[PAIR:]], 1), twice(k2)) * half
            dk = mm_tn(ds, twice(q2)) * half
            dv = mm_tn(pb, do2)
            dqkv_ref[rows, PAIR * j : PAIR * j + PAIR] = dq.astype(BF)
            dqkv_ref[rows, D + PAIR * j : D + PAIR * j + PAIR] = dk.astype(BF)
            dqkv_ref[rows, 2 * D + PAIR * j : 2 * D + PAIR * j + PAIR] = dv.astype(BF)


def att_grads_kernel(mine_ref, h1_ref, dqkv_ref, o_ref, dxb_ref, send_ref, keep_ref, acc):
    acc[:, :D] = mm_tn(o_ref[...], dxb_ref[...])
    acc[:, D:] = mm_tn(h1_ref[...], dqkv_ref[...])
    halves(mine_ref[0], 192, send_ref, keep_ref, lambda at, k: block(acc, at, 48, k))


def tok_back_kernel(tok_ref, dqkv_all, dx_all, g1, wqkv, gtok_ref):
    dqkv_ref, dx_ref = dqkv_all.at[held_rows()], dx_all.at[held_rows()]
    x = tok_ref[...].astype(F32)
    centre = x - row_mean(x)
    r = lax.rsqrt(row_mean(centre * centre) + EPS)
    unit = centre * r
    dn = mm_nt(dqkv_ref[...], wqkv[...]) * g1[...].reshape(1, D)
    gtok_ref[...] = dx_ref[...] + r * (dn - row_mean(dn) - unit * row_mean(dn * unit))


def gain_of(grad, weight, gain):
    high, mid, _ = split3(grad * weight.astype(F32))
    ones = jnp.ones((8, grad.shape[1]), BF)
    total = mm_nt(ones, high) + mm_nt(ones, mid)
    return total[0:1] / gain.reshape(1, D)


def arrived(mine_ref, own, other, rows):
    for rel in range(8):
        src = own if rel < 4 else other
        yield (mine_ref[0] >> 2) ^ rel, src, (rel % 4) * rows


def spread_mlp_kernel(mine_ref, own, other, wup, g2, down_ref, up_ref, proj_ref, gain_ref):
    for at, src, row in arrived(mine_ref, own, other, 432):
        rows = pl.ds(pl.multiple_of(at * 48, 16), 48)
        for k in range(4):
            part = quarter(mine_ref[0], row, k, 96)
            down_ref[pl.ds(pl.multiple_of(at * 192 + 48 * k, 16), 48), :] = src[pl.ds(part, 48), :].astype(F32)
            up_ref[rows, D * k : D * (k + 1)] = src[pl.ds(pl.multiple_of(part + 48, 16), 48), :].astype(F32)
        proj_ref[rows, :] = src[row + 384 : row + 432, :].astype(F32)
    gain_ref[...] = gain_of(up_ref[...], wup[...], g2[...]).reshape(D)


def spread_att_kernel(mine_ref, own, other, wqkv, g1, out_ref, qkv_ref, gain_ref):
    for at, src, row in arrived(mine_ref, own, other, 192):
        rows = pl.ds(pl.multiple_of(at * 48, 16), 48)
        out_ref[rows, :] = src[pl.ds(quarter(mine_ref[0], row, 0), 48), :].astype(F32)
        for k in range(3):
            qkv_ref[rows, D * k : D * (k + 1)] = src[pl.ds(quarter(mine_ref[0], row, k + 1), 48), :].astype(F32)
    gain_ref[...] = gain_of(qkv_ref[...], wqkv[...], g1[...]).reshape(D)


def simple(kernel, outs, scratch=(), smem=0, us=3, name=None, held=(), held_out=True):
    def call(*args):
        args = [near(v) if i in held else v for i, v in enumerate(args)]
        return pl.pallas_call(
            kernel,
            in_specs=[SMEM] * smem + [VMEM] * (len(args) - smem),
            out_specs=[VMEM] * len(outs),
            out_shape=[(pltpu.VMEM if held_out else jax.ShapeDtypeStruct)(s, t) for s, t in outs],
            scratch_shapes=list(scratch),
            compiler_params=ROOM,
            cost_estimate=cost(us),
            name=name,
        )(*args)

    return call


def mlp_back(mine, lab, h2, gp, c2, du, dy, g2, wup):
    n = h2.shape[0]
    shape = pltpu.VMEM
    return pl.pallas_call(
        mlp_back_kernel,
        grid=(n // TOK_BLOCK,),
        in_specs=[SMEM, block_of(1, TOK_BLOCK)] + [VMEM] * 5 + [const_spec((D,)), const_spec((D, FF))],
        out_specs=[VMEM] * 4,
        out_shape=[shape((n, D), F32), shape((n, D), BF), shape((768, D), BF), shape((768, D), BF)],
        scratch_shapes=[pltpu.VMEM((D, FF), F32)],
        compiler_params=ROOM,
        cost_estimate=cost(9),
        name="mlp_back",
    )(mine, lab, near(h2), near(gp), near(c2), near(du), near(dy), g2, wup)


def att_core(qkv, p, dxb, wout):
    n = dxb.shape[0]
    return pl.pallas_call(
        att_core_kernel,
        grid=(n // TOK_BLOCK,),
        in_specs=[VMEM, VMEM, VMEM, const_spec((D, D))],
        out_specs=VMEM,
        out_shape=pltpu.VMEM((n, 3 * D), BF),
        compiler_params=ROOM,
        cost_estimate=cost(10),
        name="att_core",
    )(near(qkv), near(p), near(dxb), wout)


def att_grads(mine, h1, dqkv, o, dxb):
    outs = [((768, D), BF)] * 2
    scratch = [pltpu.VMEM((D, 4 * D), F32)]
    return simple(att_grads_kernel, outs, scratch, smem=1, us=4, name="att_grads", held=(1, 2, 3, 4))(mine, h1, dqkv, o, dxb)


def tok_back(tok, dqkv, dx, g1, wqkv):
    n = tok.shape[0]
    return pl.pallas_call(
        tok_back_kernel,
        grid=(n // TOK_BLOCK,),
        in_specs=[token_rows(D), VMEM, VMEM, const_spec((D,)), const_spec((D, 3 * D))],
        out_specs=token_rows(D),
        out_shape=jax.ShapeDtypeStruct((n, D), F32),
        compiler_params=ROOM,
        cost_estimate=cost(4),
        name="tok_back",
    )(tok, near(dqkv), near(dx), g1, wqkv)


AXES = ("dp", "replica")


def swap(v, mask):
    return lax.ppermute(v, AXES, [(i, i ^ mask) for i in range(32)])


def plane(parts):
    return [swap(parts[m], 2 * m) for m in (1, 2, 3)]


def column(parts):
    return [swap(parts[m], 8 * m) for m in (1, 2, 3)]


def total_of(own, got):
    v = [own.astype(F32)] + [x.astype(F32) for x in got]
    return v[0] + v[1] if len(v) == 2 else (v[0] + v[1]) + (v[2] + v[3])


def added(own, got):
    return total_of(own, got).astype(BF)


def joined(own, got):
    return jnp.concatenate([own] + got, 0)


def shards(
    devices, tuned,
    text_tokens, segment_ids, pair_index, image_tokens,
    img_ln1, img_qkv, img_out, img_ln2, img_up, img_down, img_proj,
    txt_ln1, txt_qkv, txt_out, txt_ln2, txt_up, txt_down, txt_proj, log_scale,
):
    total = CAPS * devices
    denom = 2.0 * total
    row_of = jnp.arange(segment_ids.shape[0], dtype=jnp.int32) % (TOK_BLOCK // segment_ids.shape[1])
    lab = (segment_ids + PACK * row_of[:, None]).reshape(BLOCKS, 1, TOK_BLOCK)
    pair = pair_index
    if tuned:
        index = lax.axis_index(AXES)
        mine = ((index & 1) * 16 + ((index >> 1) & 3) * 4 + (index >> 3)).astype(jnp.int32).reshape(1)
        owner, row = pair // CAPS, pair % CAPS
        pair = (((owner & 1) * 16 + ((owner >> 1) & 3) * 4 + (owner >> 3)) ^ mine) * CAPS + row
    else:
        mine = jnp.zeros((1,), jnp.int32)
    pair = pair.reshape(CAPS, 1)
    lab, pair = lax.optimization_barrier((lab, pair))
    emb = image_tower(
        jnp.transpose(image_tokens, (1, 0, 2)), img_ln1, img_qkv, img_out, img_ln2, img_up, img_down, img_proj
    )
    if tuned:
        near = joined(emb, column([emb] * 4))
        o_now, o, qkv, p, h1 = text_att(text_tokens, lab, txt_ln1, txt_qkv)
        o_now, near = lax.optimization_barrier((o_now, near))
        got = plane([near] * 4)
    else:
        o_now, o, qkv, p, h1 = text_att(text_tokens, lab, txt_ln1, txt_qkv)
    h2, c2, gp, pu, pb, e, temb, cnt = text_mlp(text_tokens, o_now, lab, txt_out, txt_ln2, txt_up, txt_down, txt_proj)
    if tuned:
        near, got, temb = lax.optimization_barrier((near, got, temb))
        near = joined(near, got)
        own, other = near, swap(near, 1)
    else:
        own, other = jnp.split(lax.all_gather(emb, AXES, axis=0, tiled=True), 2)
    lines = total // 128
    g, sums = simple(
        functools.partial(cosine_kernel, denom),
        [((CAPS, total), F32), ((2 * lines + 8, 128), F32)],
        smem=2,
        us=3,
        name="cosine",
        held=(3, 4),
    )(log_scale, mine, temb, own, other, pair)
    (dt_row,) = simple(functools.partial(rows_kernel, denom), [((CAPS, D), F32)], smem=1, us=2, name="rows", held=(2, 3))(
        log_scale, g, own, other, pair
    )
    if tuned:
        sums = total_of(sums, [swap(sums, 1)])
        sums = total_of(sums, plane([sums] * 4))
        sums = total_of(sums, [swap(sums, 8)])
        sums = total_of(sums, [swap(sums, 16)])
    else:
        sums = lax.psum(sums, AXES)
    send_d, keep_d, send_p, keep_p, du, dy, loss, temp = simple(
        functools.partial(head_kernel, denom),
        [
            ((768, D), BF), ((768, D), BF), ((192, D), BF), ((192, D), BF),
            ((BLOCKS, 48, FF), BF), ((BLOCKS, 48, D), BF), ((1, 1), F32), ((1, 1), F32),
        ],
        [pltpu.VMEM((FF, D), F32), pltpu.VMEM((D, D), F32)],
        smem=2,
        us=5,
        name="head_back",
        held=(3, 4, 5),
    )(log_scale, mine, g, own, other, sums, dt_row, e, pb, cnt, pu, txt_proj, txt_down)
    dx, dxb, send_u, keep_u = mlp_back(mine, lab, h2, gp, c2, du, dy, txt_ln2, txt_up)

    def mlp_parts(d, u, p):
        both = jnp.concatenate([d.reshape(4, 4, 48, D), u.reshape(4, 4, 48, D)], 2).reshape(4, 384, D)
        return jnp.concatenate([both, p.reshape(4, 48, D)], 1)

    def spread_mlp(own, other):
        outs = [((FF, D), F32), ((D, FF), F32), ((D, D), F32), ((D,), F32)]
        return simple(spread_mlp_kernel, outs, smem=1, us=4, name="spread_mlp", held=(1, 2), held_out=False)(mine, own, other, txt_up, txt_ln2)

    def spread_att(own, other):
        outs = [((D, D), F32), ((D, 3 * D), F32), ((D,), F32)]
        return simple(spread_att_kernel, outs, smem=1, us=4, name="spread_att", held=(1, 2), held_out=False)(mine, own, other, txt_qkv, txt_ln1)

    if not tuned:
        dqkv = att_core(qkv, p, dxb, txt_out)
        send_a, keep_a = att_grads(mine, h1, dqkv, o, dxb)
        grad_tokens = tok_back(text_tokens, dqkv, dx, txt_ln1, txt_qkv)
        sums = [keep_d, send_d, keep_u, send_u, keep_a, send_a, keep_p, send_p]
        d, d2, u, u2, a, a2, p, p2 = [v.astype(BF) for v in lax.psum([v.astype(F32) for v in sums], AXES)]
        grad_down, grad_up, grad_proj, gain2 = spread_mlp(
            mlp_parts(d, u, p).reshape(1728, D), mlp_parts(d2, u2, p2).reshape(1728, D)
        )
        grad_out, grad_qkv, gain1 = spread_att(a, a2)
    else:
        d = added(keep_d, [swap(send_d, 1)])
        pr = added(keep_p, [swap(send_p, 1)])
        m = mlp_parts(d, added(keep_u, [swap(send_u, 1)]), pr)
        dxb, m = lax.optimization_barrier((dxb, m))
        got = plane(m)
        dqkv = att_core(qkv, p, dxb, txt_out)
        got, dqkv = lax.optimization_barrier((got, dqkv))
        m = added(m[0], got)
        m, dqkv = lax.optimization_barrier((m, dqkv))
        got = swap(m[192:], 8)
        send_a, keep_a = att_grads(mine, h1, dqkv, o, dxb)
        got, send_a, keep_a = lax.optimization_barrier((got, send_a, keep_a))
        m = added(joined(m[:192], [m[384:]]), [got])
        got = swap(m[96:], 16)
        a = added(keep_a, [swap(send_a, 1)]).reshape(4, 192, D)
        got, a = lax.optimization_barrier((got, a))
        m = added(joined(m[:96], [m[192:]]), [got])
        far = swap(m[:96], 16)
        got_a = plane(a)
        dqkv, a, m = lax.optimization_barrier((dqkv, a, m))
        grad_tokens = tok_back(text_tokens, dqkv, dx, txt_ln1, txt_qkv)
        far, grad_tokens = lax.optimization_barrier((far, grad_tokens))
        got_a, grad_tokens = lax.optimization_barrier((got_a, grad_tokens))
        m = joined(m[:96], [far, m[96:]])
        m = joined(m[:192], [swap(m[:192], 8), m[192:]])
        a = added(a[0], got_a)
        got_m = plane([m] * 4)
        a = added(a[:96], [swap(a[96:], 8)])
        a = added(a[:48], [swap(a[48:], 16)])
        a, got_m[0], got_m[1] = lax.optimization_barrier((a, got_m[0], got_m[1]))
        a = joined(a, [swap(a, 16)])
        a = joined(a, [swap(a, 8)])
        got_m, a = lax.optimization_barrier((got_m, a))
        got_a = plane([a] * 4)
        m = joined(m, got_m)
        grad_down, grad_up, grad_proj, gain2 = spread_mlp(m, swap(m, 1))
        got_a, grad_up = lax.optimization_barrier((got_a, grad_up))
        a = joined(a, got_a)
        grad_out, grad_qkv, gain1 = spread_att(a, swap(a, 1))
    return (
        loss.reshape(1), grad_tokens, gain1, grad_qkv, grad_out, gain2,
        grad_up, grad_down, grad_proj, temp.reshape(1),
    )


def solution(mesh):
    both = ("dp", "replica")
    devices = mesh.shape["dp"] * mesh.shape["replica"]
    tuned = (mesh.shape["dp"], mesh.shape["replica"]) == (8, 4)
    rows = P(both, None)
    return jax.shard_map(
        functools.partial(shards, devices, tuned),
        mesh=mesh,
        in_specs=(rows, rows, P(both), P(both, None, None)) + (P(),) * 15,
        out_specs=(P(), rows) + (P(),) * 8,
        check_vma=False,
    )
```

```python
import functools
import math

import jax
import jax.numpy as jnp
from jax import lax
from jax.experimental import pallas as pl
from jax.experimental.pallas import tpu as pltpu
from jax.sharding import PartitionSpec as P

D = 384
HEADS = 6
HEAD = 64
FF = 1536
IMG_LEN = 50
PACK = 4
CAPS = 64
TOK_BLOCK = 256
CAP_BLOCK = 16
BLOCKS = 4
PAIR = 128
IMG_BLOCK = 16
IMG_ROWS = IMG_BLOCK * IMG_LEN
EPS = 1e-06

SMEM = pl.BlockSpec(memory_space=pltpu.SMEM)
VMEM = pl.BlockSpec(memory_space=pltpu.VMEM)
ROOM = pltpu.CompilerParams(vmem_limit_bytes=24 * 2**20)

BF = jnp.bfloat16
F32 = jnp.float32
GELU_K = math.sqrt(2.0 / math.pi)
GELU_C = 0.044715


def mm(a, b):
    return lax.dot_general(a, b, (((1,), (0,)), ((), ())), preferred_element_type=F32)


def mm_nt(a, b):
    return lax.dot_general(a, b, (((1,), (1,)), ((), ())), preferred_element_type=F32)


def mm_tn(a, b):
    return lax.dot_general(a, b, (((0,), (0,)), ((), ())), preferred_element_type=F32)


def row_mean(v):
    return jnp.sum(v, -1, keepdims=True) * (1.0 / D)


def normalize(v):
    centre = v - row_mean(v)
    return centre * lax.rsqrt(row_mean(centre * centre) + EPS)


def split3(v):
    high = v.astype(BF)
    rest = v - high.astype(F32)
    mid = rest.astype(BF)
    low = (rest - mid.astype(F32)).astype(BF)
    return high, mid, low


def wide_mm(v, w):
    high, mid, low = split3(v)
    n = v.shape[0]
    out = mm(jnp.concatenate([high, mid, low], 0), w)
    return out[:n] + out[n : 2 * n] + out[2 * n :]


def gelu_parts(z):
    z2 = z * z
    t = jnp.tanh(z * (z2 * (GELU_K * GELU_C) + GELU_K))
    hp = t * 0.5 + 0.5
    u = z * hp
    slope = hp + (u * (1.0 - hp)) * (z2 * (6.0 * GELU_K * GELU_C) + 2.0 * GELU_K)
    return u, slope


def lanes_head(shape):
    return lax.broadcasted_iota(jnp.int32, shape, len(shape) - 1) // HEAD


def image_kernel(x_ref, g1, wqkv, wout, g2, wup, wdown, wproj, emb_ref, kv, x0, att):
    step = pl.program_id(0)
    gain = g1[...].reshape(1, D)
    for c in range(2):
        x = x_ref[IMG_LEN // 2 * c : IMG_LEN // 2 * (c + 1)].astype(F32).reshape(IMG_ROWS // 2, D)
        h = (normalize(x) * gain).astype(BF)
        kv[IMG_ROWS // 2 * c : IMG_ROWS // 2 * (c + 1), :] = mm(h, wqkv[:, D:]).astype(BF)
        if c == 0:
            x0[pl.ds(pl.multiple_of(step * IMG_BLOCK, IMG_BLOCK), IMG_BLOCK), :] = x[:IMG_BLOCK]
            h0 = h[:IMG_BLOCK]
    q = mm(h0, wqkv[:, :D]).astype(BF).astype(F32) * (HEAD**-0.5)
    head = lanes_head((IMG_BLOCK, D))
    queries = HEADS * IMG_BLOCK
    rows = lax.broadcasted_iota(jnp.int32, (queries, IMG_ROWS), 0)
    cols = lax.broadcasted_iota(jnp.int32, (queries, IMG_ROWS), 1)
    own = cols % IMG_BLOCK == rows % IMG_BLOCK
    q6 = jnp.concatenate([jnp.where(head == h, q, 0.0) for h in range(HEADS)], 0)
    s = mm_nt(q6.astype(BF), kv[:, :D])
    s = jnp.where(own, s, -1e30)
    e = jnp.exp(s - jnp.max(s, -1, keepdims=True))
    p = (e * (1.0 / jnp.sum(e, -1, keepdims=True))).astype(BF)
    r = mm(p, kv[:, D:])
    o = jnp.where(head == 0, r[0:IMG_BLOCK], 0.0)
    for h in range(1, HEADS):
        o = jnp.where(head == h, r[IMG_BLOCK * h : IMG_BLOCK * (h + 1)], o)
    att[pl.ds(pl.multiple_of(step * IMG_BLOCK, IMG_BLOCK), IMG_BLOCK), :] = o

    @pl.when(step == pl.num_programs(0) - 1)
    def _():
        x1 = x0[...] + mm(att[...].astype(BF), wout[...])
        h2 = (normalize(x1) * g2[...].reshape(1, D)).astype(BF)
        u, _ = gelu_parts(mm(h2, wup[...]))
        y = x1 + mm(u.astype(BF), wdown[...])
        e = mm(y.astype(BF), wproj[...])
        emb_ref[...] = (e * lax.rsqrt(jnp.sum(e * e, -1, keepdims=True) + EPS)).astype(BF)


def near(v):
    return pltpu.with_memory_space_constraint(v, pltpu.VMEM)


def away(v):
    return pltpu.with_memory_space_constraint(v, pltpu.HBM)


def cost(us):
    return pl.CostEstimate(flops=int(us * 1e9), bytes_accessed=int(us * 3e6), transcendentals=0)


def const_spec(shape):
    zeros = (0,) * len(shape)
    return pl.BlockSpec(shape, lambda *_: zeros, pipeline_mode=pl.Buffered(1))


def image_tower(x, g1, wqkv, wout, g2, wup, wdown, wproj):
    count = x.shape[1]
    return pl.pallas_call(
        image_kernel,
        grid=(count // IMG_BLOCK,),
        in_specs=[
            pl.BlockSpec((IMG_LEN, IMG_BLOCK, D), lambda i: (0, i, 0)),
            const_spec((D,)),
            const_spec((D, 3 * D)),
            const_spec((D, D)),
            const_spec((D,)),
            const_spec((D, FF)),
            const_spec((FF, D)),
            const_spec((D, D)),
        ],
        out_specs=pl.BlockSpec((count, D), lambda i: (0, 0)),
        out_shape=jax.ShapeDtypeStruct((count, D), BF),
        scratch_shapes=[
            pltpu.VMEM((IMG_ROWS, 2 * D), BF),
            pltpu.VMEM((count, D), F32),
            pltpu.VMEM((count, D), F32),
        ],
        compiler_params=ROOM,
        cost_estimate=cost(12),
        name="image_tower",
    )(*[away(v) for v in (x, g1, wqkv, wout, g2, wup, wdown, wproj)])


def pair_mask(lab_ref, pair):
    lab = lab_ref[0, :, PAIR * pair : PAIR * pair + PAIR].astype(F32)
    wide = jnp.broadcast_to(lab, (PAIR, PAIR))
    return wide == wide.T


def text_att_kernel(tok_ref, lab_ref, g1, wqkv, o_all, o_ref, qkv_ref, p_ref, h1_ref):
    x = tok_ref[...].astype(F32)
    h1 = (normalize(x) * g1[...].reshape(1, D)).astype(BF)
    h1_ref[...] = h1
    qkv = mm(h1, wqkv[...]).astype(BF)
    qkv_ref[...] = qkv
    low = lax.broadcasted_iota(jnp.int32, (PAIR, PAIR), 1) < HEAD
    for pair in range(2):
        rows = slice(PAIR * pair, PAIR * pair + PAIR)
        mask = pair_mask(lab_ref, pair)
        mask = jnp.concatenate([mask, mask], 0)
        for j in range(HEADS // 2):
            cols = slice(PAIR * j, PAIR * j + PAIR)
            q2 = qkv[rows, PAIR * j : PAIR * j + PAIR] * jnp.asarray(HEAD**-0.5, BF)
            k2 = qkv[rows, D + PAIR * j : D + PAIR * j + PAIR]
            v2 = qkv[rows, 2 * D + PAIR * j : 2 * D + PAIR * j + PAIR]
            zero = jnp.zeros_like(q2)
            q22 = jnp.concatenate([jnp.where(low, q2, zero), jnp.where(low, zero, q2)], 0)
            s = jnp.where(mask, mm_nt(q22, k2), -1e30)
            ex = jnp.exp(s - jnp.max(s, -1, keepdims=True))
            p = (ex * (1.0 / jnp.sum(ex, -1, keepdims=True))).astype(BF)
            p_ref[pair, j] = p
            v22 = jnp.concatenate([jnp.where(low, v2, zero), jnp.where(low, zero, v2)], 0)
            o = mm(jnp.concatenate([p[:PAIR], p[PAIR:]], 1), v22)
            o_ref[rows, cols] = o.astype(BF)
    o_all[held_rows(), :] = o_ref[...]


def text_mlp_kernel(
    tok_ref, o_ref, lab_ref, wout, g2, wup, wdown, wproj,
    h2_ref, c2_ref, gp_ref, pu_ref, pb_ref, e_ref, emb_ref, cnt_ref, pt, po,
):
    step = pl.program_id(0)
    tok = tok_ref[...]
    o = o_ref[held_rows(), :]
    x1 = tok.astype(F32) + mm(o, wout[...])
    c2 = x1 - row_mean(x1)
    c2_ref[...] = c2
    h2 = (c2 * lax.rsqrt(row_mean(c2 * c2) + EPS) * g2[...].reshape(1, D)).astype(BF)
    h2_ref[...] = h2
    hit = lax.broadcasted_iota(jnp.int32, (CAP_BLOCK, TOK_BLOCK), 0) == lab_ref[0]
    member = jnp.where(hit, 1.0, 0.0)
    caps = pl.ds(pl.multiple_of(step * CAP_BLOCK, CAP_BLOCK), CAP_BLOCK)
    member_b = member.astype(BF)
    pt[caps, :] = mm(member_b, tok)
    po[caps, :] = mm(member_b, o)
    cnt_ref[caps, :] = jnp.broadcast_to(jnp.sum(member, -1, keepdims=True), (CAP_BLOCK, 128))
    for k in range(FF // 512):
        cols = slice(512 * k, 512 * (k + 1))
        u, slope = gelu_parts(mm(h2, wup[:, cols]))
        gp_ref[:, cols] = slope.astype(BF)
        pu_ref[caps, cols] = mm(member_b, u.astype(BF))

    @pl.when(step == pl.num_programs(0) - 1)
    def _():
        total = pt[...] + wide_mm(po[...], wout[...]) + wide_mm(pu_ref[...], wdown[...])
        pooled = (total * (1.0 / cnt_ref[:, 0:1])).astype(BF)
        pb_ref[...] = pooled
        e = mm(pooled, wproj[...])
        e_ref[...] = e
        emb_ref[...] = (e * lax.rsqrt(jnp.sum(e * e, -1, keepdims=True) + EPS)).astype(BF)


def held_rows():
    return pl.ds(pl.multiple_of(pl.program_id(0) * TOK_BLOCK, TOK_BLOCK), TOK_BLOCK)


def token_rows(width):
    return pl.BlockSpec((TOK_BLOCK, width), lambda i: (i, 0))


def block_of(a, b):
    return pl.BlockSpec((1, a, b), lambda i: (i, 0, 0))


def whole(a, b):
    return pl.BlockSpec((a, b), lambda i: (0, 0))


def text_att(tok, lab, g1, wqkv):
    n = tok.shape[0]
    blocks = n // TOK_BLOCK
    shape = pltpu.HBM
    return pl.pallas_call(
        text_att_kernel,
        grid=(blocks,),
        in_specs=[token_rows(D), block_of(1, TOK_BLOCK), const_spec((D,)), const_spec((D, 3 * D))],
        out_specs=[
            VMEM,
            token_rows(D),
            token_rows(3 * D),
            pl.BlockSpec((2, 3, 2 * PAIR, PAIR), lambda i: (i, 0, 0, 0)),
            token_rows(D),
        ],
        out_shape=[
            pltpu.VMEM((n, D), BF), shape((n, D), BF), shape((n, 3 * D), BF),
            shape((2 * blocks, 3, 2 * PAIR, PAIR), BF), shape((n, D), BF),
        ],
        compiler_params=ROOM,
        cost_estimate=cost(9),
        name="text_att",
    )(away(tok), lab, g1, away(wqkv))


def text_mlp(tok, o, lab, wout, g2, wup, wdown, wproj):
    n = tok.shape[0]
    shape = pltpu.VMEM
    return pl.pallas_call(
        text_mlp_kernel,
        grid=(n // TOK_BLOCK,),
        in_specs=[
            token_rows(D), VMEM, block_of(1, TOK_BLOCK),
            const_spec((D, D)), const_spec((D,)), const_spec((D, FF)), const_spec((FF, D)), const_spec((D, D)),
        ],
        out_specs=[token_rows(D), token_rows(D), token_rows(FF)] + [VMEM] * 5,
        out_shape=[
            pltpu.HBM((n, D), BF), pltpu.HBM((n, D), F32), pltpu.HBM((n, FF), BF),
            shape((CAPS, FF), F32), shape((CAPS, D), BF), shape((CAPS, D), F32),
            shape((CAPS, D), BF), shape((CAPS, 128), F32),
        ],
        scratch_shapes=[pltpu.VMEM((CAPS, D), F32), pltpu.VMEM((CAPS, D), F32)],
        compiler_params=ROOM,
        cost_estimate=cost(11),
        name="text_mlp",
    )(tok, near(o), lab, wout, g2, wup, wdown, wproj)


def reorder(mine, row):
    return jnp.where(mine & 1 == 1, pltpu.roll(row, 64, 1), row)


def cosine_kernel(denom, scale_ref, mine_ref, emb, own, other, pair, g_ref, sum_ref):
    mine = mine_ref[0]
    scale = jnp.exp(jnp.full((1, 1), scale_ref[0], F32))
    g = jnp.concatenate([mm_nt(emb[...], own[...]), mm_nt(emb[...], other[...])], 1)
    g_ref[...] = g
    e = jnp.exp(g * scale)
    eg = e * g
    total = jnp.sum(e, -1, keepdims=True)
    hit = lax.broadcasted_iota(jnp.int32, g.shape, 1) == pair[...]
    own = jnp.sum(jnp.where(hit, g, 0.0), -1, keepdims=True)
    loss = jnp.sum(jnp.log(total) - 2.0 * scale * own, 0, keepdims=True)
    temp = jnp.sum(jnp.sum(eg, -1, keepdims=True) / total - 2.0 * own, 0, keepdims=True)
    n = g.shape[1] // 128
    for k, v in enumerate((jnp.sum(e, 0, keepdims=True), jnp.sum(eg, 0, keepdims=True))):
        for r in range(n):
            sum_ref[pl.ds(k * n + ((mine >> 1) ^ r), 1), :] = reorder(mine, v[:, 128 * r : 128 * (r + 1)])
    lane = lax.broadcasted_iota(jnp.int32, (8, 128), 1)
    sum_ref[2 * n :, :] = jnp.where(lane == 0, loss, jnp.where(lane == 1, temp, 0.0))


def times_images(dl, own, other):
    half = dl.shape[1] // 2
    return mm(dl[:, :half], own[...]) + mm(dl[:, half:], other[...])


def rows_kernel(denom, scale_ref, g_ref, own, other, pair, dt_ref):
    scale = jnp.exp(jnp.full((1, 1), scale_ref[0], F32))
    g = g_ref[...]
    e = jnp.exp(g * scale)
    hit = lax.broadcasted_iota(jnp.int32, g.shape, 1) == pair[...]
    p = e * (1.0 / jnp.sum(e, -1, keepdims=True))
    dl = jnp.where(hit, p - 2.0, p) * (scale * (1.0 / denom))
    dt_ref[...] = times_images(dl.astype(BF), own, other)


def quarter(mine, base, k, rows=48):
    far = (mine & 3) ^ k
    return pl.multiple_of(base + rows * ((far & 1) * 2 + (far >> 1)), 16)


def halves(mine, rows, send_ref, keep_ref, piece):
    for rel in range(8):
        ref = keep_ref if rel < 4 else send_ref
        at = (rel % 4) * rows
        if rows == 48:
            ref[at : at + 48, :] = piece((mine >> 2) ^ rel, 0).astype(BF)
            continue
        for k in range(4):
            ref[pl.ds(quarter(mine, at, k), 48), :] = piece((mine >> 2) ^ rel, k).astype(BF)


def block(acc, at, rows, col=0):
    return acc[pl.ds(pl.multiple_of(at * rows, 16), rows), D * col : D * (col + 1)]


def head_kernel(
    denom, scale_ref, mine_ref, g_ref, own, other, sums, dt_row, e_ref, pb, cnt, pu, wproj, wdown,
    sd_ref, kd_ref, sp_ref, kp_ref, du_ref, dy_ref, loss_out, temp_out, down, proj,
):
    mine = mine_ref[0]
    scale = jnp.exp(jnp.full((1, 1), scale_ref[0], F32))
    n = g_ref.shape[1] // 128

    def columns(k):
        return jnp.concatenate([reorder(mine, sums[pl.ds(k * n + ((mine >> 1) ^ r), 1), :]) for r in range(n)], 1)

    temp = jnp.sum(jnp.sum(sums[n : 2 * n, :] / sums[0:n, :], 0, keepdims=True), -1, keepdims=True)
    loss = jnp.sum(jnp.sum(jnp.log(sums[0:n, :]), 0, keepdims=True), -1, keepdims=True)
    loss_out[...] = (sums[2 * n : 2 * n + 1, 0:1] + loss) * (1.0 / denom)
    temp_out[...] = (sums[2 * n : 2 * n + 1, 1:2] + temp) * (scale * (1.0 / denom))
    inverse = 1.0 / columns(0)
    dl = jnp.exp(g_ref[...] * scale) * (inverse * (scale * (1.0 / denom)))
    dt = dt_row[...] + times_images(dl.astype(BF), own, other)
    e = e_ref[...]
    r = lax.rsqrt(jnp.sum(e * e, -1, keepdims=True) + EPS)
    de = (dt - e * (r * r * jnp.sum(dt * e, -1, keepdims=True))) * r
    de = de.astype(BF)
    dpooled = mm_nt(de, wproj[...])
    dy = dpooled * (1.0 / cnt[:, 0:1])
    dyb = dy.astype(BF)
    du = mm_nt(dyb, wdown[...])
    for i, piece in enumerate(split3(du)):
        for b in range(BLOCKS):
            du_ref[b, CAP_BLOCK * i : CAP_BLOCK * (i + 1), :] = piece[CAP_BLOCK * b : CAP_BLOCK * (b + 1)]
    for i, piece in enumerate(split3(dy)):
        for b in range(BLOCKS):
            dy_ref[b, CAP_BLOCK * i : CAP_BLOCK * (i + 1), :] = piece[CAP_BLOCK * b : CAP_BLOCK * (b + 1)]
    down[...] = mm_tn(jnp.concatenate(split3(pu[...]), 0), jnp.concatenate([dyb, dyb, dyb], 0))
    proj[...] = mm_tn(pb[...], de)
    halves(mine, 192, sd_ref, kd_ref, lambda at, k: block(down, at * 4 + k, 48))
    halves(mine, 48, sp_ref, kp_ref, lambda at, k: block(proj, at, 48))


def mlp_back_kernel(
    mine_ref, lab_ref, h2_all, gp_all, c2_all, du_ref, dy_ref, g2, wup,
    dx_all, dxb_all, send_ref, keep_ref, acc,
):
    step = pl.program_id(0)
    h2_ref, gp_ref, c2_ref = h2_all.at[held_rows()], gp_all.at[held_rows()], c2_all.at[held_rows()]
    dx_ref, dxb_ref = dx_all.at[held_rows()], dxb_all.at[held_rows()]

    @pl.when(step == 0)
    def _():
        acc[...] = jnp.zeros_like(acc)

    hit = lax.broadcasted_iota(jnp.int32, (3 * CAP_BLOCK, TOK_BLOCK), 0) % CAP_BLOCK == lab_ref[0]
    spread = jnp.where(hit, 1.0, 0.0).astype(BF)
    du = mm_tn(spread, du_ref[step])
    dz = (du * gp_ref[...].astype(F32)).astype(BF)
    dy = mm_tn(spread, dy_ref[step])
    dh = mm_nt(dz, wup[...])
    c2 = c2_ref[...]
    r = lax.rsqrt(row_mean(c2 * c2) + EPS)
    unit = c2 * r
    dn = dh * g2[...].reshape(1, D)
    dx = dy + r * (dn - row_mean(dn) - unit * row_mean(dn * unit))
    dx_ref[...] = dx
    dxb_ref[...] = dx.astype(BF)
    h2 = h2_ref[...]
    acc[...] += mm_tn(h2, dz)

    @pl.when(step == pl.num_programs(0) - 1)
    def _():
        halves(mine_ref[0], 192, send_ref, keep_ref, lambda at, k: block(acc, at, 48, k))


def att_back_kernel(
    mine_ref, qkv_all, p_all, dxb_all, dx_all, h1_ref, o_ref, tok_ref, wout, g1, wqkv,
    gtok_ref, send_ref, keep_ref, dqkv_all, acc,
):
    step = pl.program_id(0)
    qkv_ref, dxb_ref, dqkv_ref = qkv_all.at[held_rows()], dxb_all.at[held_rows()], dqkv_all.at[held_rows()]
    p_ref = p_all.at[pl.ds(2 * step, 2)]
    do = mm_nt(dxb_ref[...], wout[...]).astype(BF)
    low = lax.broadcasted_iota(jnp.int32, (PAIR, PAIR), 1) < HEAD
    zero = jnp.zeros((PAIR, PAIR), BF)
    half = HEAD**-0.5

    def twice(v):
        return jnp.concatenate([jnp.where(low, v, zero), jnp.where(low, zero, v)], 0)

    for pair in range(2):
        rows = slice(PAIR * pair, PAIR * pair + PAIR)
        for j in range(HEADS // 2):
            cols = slice(PAIR * j, PAIR * j + PAIR)
            q2 = qkv_ref[rows, PAIR * j : PAIR * j + PAIR]
            k2 = qkv_ref[rows, D + PAIR * j : D + PAIR * j + PAIR]
            v2 = qkv_ref[rows, 2 * D + PAIR * j : 2 * D + PAIR * j + PAIR]
            do2 = twice(do[rows, cols])
            pb = p_ref[pair, j]
            p = pb.astype(F32)
            dp = mm_nt(do2, v2)
            ds = (p * (dp - jnp.sum(dp * p, -1, keepdims=True))).astype(BF)
            dq = mm(jnp.concatenate([ds[:PAIR], ds[PAIR:]], 1), twice(k2)) * half
            dk = mm_tn(ds, twice(q2)) * half
            dv = mm_tn(pb, do2)
            dqkv_ref[rows, PAIR * j : PAIR * j + PAIR] = dq.astype(BF)
            dqkv_ref[rows, D + PAIR * j : D + PAIR * j + PAIR] = dk.astype(BF)
            dqkv_ref[rows, 2 * D + PAIR * j : 2 * D + PAIR * j + PAIR] = dv.astype(BF)
    x = tok_ref[...].astype(F32)
    centre = x - row_mean(x)
    r = lax.rsqrt(row_mean(centre * centre) + EPS)
    unit = centre * r
    dn = mm_nt(dqkv_ref[...], wqkv[...]) * g1[...].reshape(1, D)
    gtok_ref[...] = dx_all[held_rows(), :] + r * (dn - row_mean(dn) - unit * row_mean(dn * unit))

    @pl.when(step == pl.num_programs(0) - 1)
    def _():
        acc[:, :D] = mm_tn(o_ref[...], dxb_all[...])
        acc[:, D:] = mm_tn(h1_ref[...], dqkv_all[...])
        halves(mine_ref[0], 192, send_ref, keep_ref, lambda at, k: block(acc, at, 48, k))


def gain_of(grad, weight, gain):
    high, mid, _ = split3(grad * weight.astype(F32))
    ones = jnp.ones((8, grad.shape[1]), BF)
    total = mm_nt(ones, high) + mm_nt(ones, mid)
    return total[0:1] / gain.reshape(1, D)


def arrived(mine_ref, own, other, rows):
    for rel in range(8):
        src = own if rel < 4 else other
        yield (mine_ref[0] >> 2) ^ rel, src, (rel % 4) * rows


def spread_mlp_kernel(mine_ref, own, other, wup, g2, down_ref, up_ref, proj_ref, gain_ref):
    for at, src, row in arrived(mine_ref, own, other, 432):
        rows = pl.ds(pl.multiple_of(at * 48, 16), 48)
        for k in range(4):
            part = quarter(mine_ref[0], row, k, 96)
            down_ref[pl.ds(pl.multiple_of(at * 192 + 48 * k, 16), 48), :] = src[pl.ds(part, 48), :].astype(F32)
            up_ref[rows, D * k : D * (k + 1)] = src[pl.ds(pl.multiple_of(part + 48, 16), 48), :].astype(F32)
        proj_ref[rows, :] = src[row + 384 : row + 432, :].astype(F32)
    gain_ref[...] = gain_of(up_ref[...], wup[...], g2[...]).reshape(D)


def spread_att_kernel(mine_ref, own, other, wqkv, g1, out_ref, qkv_ref, gain_ref):
    for at, src, row in arrived(mine_ref, own, other, 192):
        rows = pl.ds(pl.multiple_of(at * 48, 16), 48)
        out_ref[rows, :] = src[pl.ds(quarter(mine_ref[0], row, 0), 48), :].astype(F32)
        for k in range(3):
            qkv_ref[rows, D * k : D * (k + 1)] = src[pl.ds(quarter(mine_ref[0], row, k + 1), 48), :].astype(F32)
    gain_ref[...] = gain_of(qkv_ref[...], wqkv[...], g1[...]).reshape(D)


def simple(kernel, outs, scratch=(), smem=0, us=3, name=None, held=(), held_out=True):
    def call(*args):
        args = [near(v) if i in held else v for i, v in enumerate(args)]
        return pl.pallas_call(
            kernel,
            in_specs=[SMEM] * smem + [VMEM] * (len(args) - smem),
            out_specs=[VMEM] * len(outs),
            out_shape=[(pltpu.VMEM if held_out else jax.ShapeDtypeStruct)(s, t) for s, t in outs],
            scratch_shapes=list(scratch),
            compiler_params=ROOM,
            cost_estimate=cost(us),
            name=name,
        )(*args)

    return call


def mlp_back(mine, lab, h2, gp, c2, du, dy, g2, wup):
    n = h2.shape[0]
    shape = pltpu.VMEM
    return pl.pallas_call(
        mlp_back_kernel,
        grid=(n // TOK_BLOCK,),
        in_specs=[SMEM, block_of(1, TOK_BLOCK)] + [VMEM] * 5 + [const_spec((D,)), const_spec((D, FF))],
        out_specs=[VMEM] * 4,
        out_shape=[shape((n, D), F32), shape((n, D), BF), shape((768, D), BF), shape((768, D), BF)],
        scratch_shapes=[pltpu.VMEM((D, FF), F32)],
        compiler_params=ROOM,
        cost_estimate=cost(9),
        name="mlp_back",
    )(mine, lab, near(h2), near(gp), near(c2), near(du), near(dy), g2, wup)


def att_back(mine, qkv, p, dxb, dx, h1, o, tok, wout, g1, wqkv):
    n = dxb.shape[0]
    return pl.pallas_call(
        att_back_kernel,
        grid=(n // TOK_BLOCK,),
        in_specs=[SMEM] + [VMEM] * 6 + [token_rows(D), const_spec((D, D)), const_spec((D,)), const_spec((D, 3 * D))],
        out_specs=[token_rows(D), VMEM, VMEM],
        out_shape=[pltpu.HBM((n, D), F32), pltpu.VMEM((768, D), BF), pltpu.VMEM((768, D), BF)],
        scratch_shapes=[pltpu.VMEM((n, 3 * D), BF), pltpu.VMEM((D, 4 * D), F32)],
        compiler_params=ROOM,
        cost_estimate=cost(14),
        name="att_back",
    )(mine, *[near(v) for v in (qkv, p, dxb, dx, h1, o)], tok, wout, g1, wqkv)


AXES = ("dp", "replica")


def swap(v, mask):
    return lax.ppermute(v, AXES, [(i, i ^ mask) for i in range(32)])


def plane(parts):
    return [swap(parts[m], 2 * m) for m in (1, 2, 3)]


def column(parts):
    return [swap(parts[m], 8 * m) for m in (1, 2, 3)]


def total_of(own, got):
    v = [own.astype(F32)] + [x.astype(F32) for x in got]
    return v[0] + v[1] if len(v) == 2 else (v[0] + v[1]) + (v[2] + v[3])


def added(own, got):
    return total_of(own, got).astype(BF)


def joined(own, got):
    return jnp.concatenate([own] + got, 0)


def shards(
    devices, tuned,
    text_tokens, segment_ids, pair_index, image_tokens,
    img_ln1, img_qkv, img_out, img_ln2, img_up, img_down, img_proj,
    txt_ln1, txt_qkv, txt_out, txt_ln2, txt_up, txt_down, txt_proj, log_scale,
):
    total = CAPS * devices
    denom = 2.0 * total
    row_of = jnp.arange(segment_ids.shape[0], dtype=jnp.int32) % (TOK_BLOCK // segment_ids.shape[1])
    lab = (segment_ids + PACK * row_of[:, None]).reshape(BLOCKS, 1, TOK_BLOCK)
    pair = pair_index
    if tuned:
        index = lax.axis_index(AXES)
        mine = ((index & 1) * 16 + ((index >> 1) & 3) * 4 + (index >> 3)).astype(jnp.int32).reshape(1)
        owner, row = pair // CAPS, pair % CAPS
        pair = (((owner & 1) * 16 + ((owner >> 1) & 3) * 4 + (owner >> 3)) ^ mine) * CAPS + row
    else:
        mine = jnp.zeros((1,), jnp.int32)
    pair = pair.reshape(CAPS, 1)
    lab, pair = lax.optimization_barrier((lab, pair))
    emb = image_tower(
        jnp.transpose(image_tokens, (1, 0, 2)), img_ln1, img_qkv, img_out, img_ln2, img_up, img_down, img_proj
    )
    if tuned:
        near = joined(emb, column([emb] * 4))
        o_now, o, qkv, p, h1 = text_att(text_tokens, lab, txt_ln1, txt_qkv)
        o_now, near = lax.optimization_barrier((o_now, near))
        got = plane([near] * 4)
    else:
        o_now, o, qkv, p, h1 = text_att(text_tokens, lab, txt_ln1, txt_qkv)
    h2, c2, gp, pu, pb, e, temb, cnt = text_mlp(text_tokens, o_now, lab, txt_out, txt_ln2, txt_up, txt_down, txt_proj)
    if tuned:
        near, got, temb = lax.optimization_barrier((near, got, temb))
        near = joined(near, got)
        own, other = near, swap(near, 1)
    else:
        own, other = jnp.split(lax.all_gather(emb, AXES, axis=0, tiled=True), 2)
    lines = total // 128
    g, sums = simple(
        functools.partial(cosine_kernel, denom),
        [((CAPS, total), F32), ((2 * lines + 8, 128), F32)],
        smem=2,
        us=3,
        name="cosine",
        held=(3, 4),
    )(log_scale, mine, temb, own, other, pair)
    (dt_row,) = simple(functools.partial(rows_kernel, denom), [((CAPS, D), F32)], smem=1, us=2, name="rows", held=(2, 3))(
        log_scale, g, own, other, pair
    )
    if tuned:
        sums = total_of(sums, [swap(sums, 1)])
        sums = total_of(sums, plane([sums] * 4))
        sums = total_of(sums, [swap(sums, 8)])
        sums = total_of(sums, [swap(sums, 16)])
    else:
        sums = lax.psum(sums, AXES)
    send_d, keep_d, send_p, keep_p, du, dy, loss, temp = simple(
        functools.partial(head_kernel, denom),
        [
            ((768, D), BF), ((768, D), BF), ((192, D), BF), ((192, D), BF),
            ((BLOCKS, 48, FF), BF), ((BLOCKS, 48, D), BF), ((1, 1), F32), ((1, 1), F32),
        ],
        [pltpu.VMEM((FF, D), F32), pltpu.VMEM((D, D), F32)],
        smem=2,
        us=5,
        name="head_back",
        held=(3, 4, 5),
    )(log_scale, mine, g, own, other, sums, dt_row, e, pb, cnt, pu, txt_proj, txt_down)
    dx, dxb, send_u, keep_u = mlp_back(mine, lab, h2, gp, c2, du, dy, txt_ln2, txt_up)

    def mlp_parts(d, u, p):
        both = jnp.concatenate([d.reshape(4, 4, 48, D), u.reshape(4, 4, 48, D)], 2).reshape(4, 384, D)
        return jnp.concatenate([both, p.reshape(4, 48, D)], 1)

    def spread_mlp(own, other):
        outs = [((FF, D), F32), ((D, FF), F32), ((D, D), F32), ((D,), F32)]
        return simple(spread_mlp_kernel, outs, smem=1, us=4, name="spread_mlp", held=(1, 2), held_out=False)(mine, own, other, txt_up, txt_ln2)

    def spread_att(own, other):
        outs = [((D, D), F32), ((D, 3 * D), F32), ((D,), F32)]
        return simple(spread_att_kernel, outs, smem=1, us=4, name="spread_att", held=(1, 2), held_out=False)(mine, own, other, txt_qkv, txt_ln1)

    if not tuned:
        grad_tokens, send_a, keep_a = att_back(
            mine, qkv, p, dxb, dx, h1, o, text_tokens, txt_out, txt_ln1, txt_qkv
        )
        sums = [keep_d, send_d, keep_u, send_u, keep_a, send_a, keep_p, send_p]
        d, d2, u, u2, a, a2, p, p2 = [v.astype(BF) for v in lax.psum([v.astype(F32) for v in sums], AXES)]
        grad_down, grad_up, grad_proj, gain2 = spread_mlp(
            mlp_parts(d, u, p).reshape(1728, D), mlp_parts(d2, u2, p2).reshape(1728, D)
        )
        grad_out, grad_qkv, gain1 = spread_att(a, a2)
    else:
        d = added(keep_d, [swap(send_d, 1)])
        pr = added(keep_p, [swap(send_p, 1)])
        m = mlp_parts(d, added(keep_u, [swap(send_u, 1)]), pr)
        dxb, m = lax.optimization_barrier((dxb, m))
        got = plane(m)
        grad_tokens, send_a, keep_a = att_back(
            mine, qkv, p, dxb, dx, h1, o, text_tokens, txt_out, txt_ln1, txt_qkv
        )
        other = swap(send_a, 1)
        got, keep_a = lax.optimization_barrier((got, keep_a))
        m = added(m[0], got)
        got = swap(m[192:], 8)
        a = added(keep_a, [other]).reshape(4, 192, D)
        got_a = plane(a)
        got, got_a[0], got_a[1] = lax.optimization_barrier((got, got_a[0], got_a[1]))
        m = added(joined(m[:192], [m[384:]]), [got])
        got = swap(m[96:], 16)
        got, got_a = lax.optimization_barrier((got, got_a))
        a = added(a[0], got_a)
        got_a = swap(a[96:], 8)
        m = added(joined(m[:96], [m[192:]]), [got])
        far = swap(m[:96], 16)
        a = added(a[:96], [got_a])
        got_a = swap(a[48:], 16)
        m = joined(m[:96], [far, m[96:]])
        m = joined(m[:192], [swap(m[:192], 8), m[192:]])
        got_m = plane([m] * 4)
        a = added(a[:48], [got_a])
        a = joined(a, [swap(a, 16)])
        a = joined(a, [swap(a, 8)])
        got_m[0], got_m[1], a = lax.optimization_barrier((got_m[0], got_m[1], a))
        got_a = plane([a] * 4)
        got_m[2], got_a[0], got_a[1] = lax.optimization_barrier((got_m[2], got_a[0], got_a[1]))
        m = joined(m, got_m)
        grad_down, grad_up, grad_proj, gain2 = spread_mlp(m, swap(m, 1))
        got_a, grad_up = lax.optimization_barrier((got_a, grad_up))
        a = joined(a, got_a)
        grad_out, grad_qkv, gain1 = spread_att(a, swap(a, 1))
    return (
        loss.reshape(1), grad_tokens, gain1, grad_qkv, grad_out, gain2,
        grad_up, grad_down, grad_proj, temp.reshape(1),
    )


def solution(mesh):
    both = ("dp", "replica")
    devices = mesh.shape["dp"] * mesh.shape["replica"]
    tuned = (mesh.shape["dp"], mesh.shape["replica"]) == (8, 4)
    rows = P(both, None)
    return jax.shard_map(
        functools.partial(shards, devices, tuned),
        mesh=mesh,
        in_specs=(rows, rows, P(both), P(both, None, None)) + (P(),) * 15,
        out_specs=(P(), rows) + (P(),) * 8,
        check_vma=False,
    )
```

```python
import functools
import math

import jax
import jax.numpy as jnp
from jax import lax
from jax.experimental import pallas as pl
from jax.experimental.pallas import tpu as pltpu
from jax.sharding import PartitionSpec as P

D = 384
HEADS = 6
HEAD = 64
FF = 1536
IMG_LEN = 50
PACK = 4
CAPS = 64
TOK_BLOCK = 256
CAP_BLOCK = 16
BLOCKS = 4
PAIR = 128
IMG_BLOCK = 16
IMG_ROWS = IMG_BLOCK * IMG_LEN
EPS = 1e-06

SMEM = pl.BlockSpec(memory_space=pltpu.SMEM)
VMEM = pl.BlockSpec(memory_space=pltpu.VMEM)
ROOM = pltpu.CompilerParams(vmem_limit_bytes=24 * 2**20)

BF = jnp.bfloat16
F32 = jnp.float32
GELU_K = math.sqrt(2.0 / math.pi)
GELU_C = 0.044715


def mm(a, b):
    return lax.dot_general(a, b, (((1,), (0,)), ((), ())), preferred_element_type=F32)


def mm_nt(a, b):
    return lax.dot_general(a, b, (((1,), (1,)), ((), ())), preferred_element_type=F32)


def mm_tn(a, b):
    return lax.dot_general(a, b, (((0,), (0,)), ((), ())), preferred_element_type=F32)


def row_mean(v):
    return jnp.sum(v, -1, keepdims=True) * (1.0 / D)


def normalize(v):
    centre = v - row_mean(v)
    return centre * lax.rsqrt(row_mean(centre * centre) + EPS)


def split3(v):
    high = v.astype(BF)
    rest = v - high.astype(F32)
    mid = rest.astype(BF)
    low = (rest - mid.astype(F32)).astype(BF)
    return high, mid, low


def wide_mm(v, w):
    high, mid, low = split3(v)
    n = v.shape[0]
    out = mm(jnp.concatenate([high, mid, low], 0), w)
    return out[:n] + out[n : 2 * n] + out[2 * n :]


def gelu_parts(z):
    z2 = z * z
    t = jnp.tanh(z * (z2 * (GELU_K * GELU_C) + GELU_K))
    hp = t * 0.5 + 0.5
    u = z * hp
    slope = hp + (u * (1.0 - hp)) * (z2 * (6.0 * GELU_K * GELU_C) + 2.0 * GELU_K)
    return u, slope


def lanes_head(shape):
    return lax.broadcasted_iota(jnp.int32, shape, len(shape) - 1) // HEAD


def image_kernel(x_ref, g1, wqkv, wout, g2, wup, wdown, wproj, emb_ref, kv, x0, att):
    step = pl.program_id(0)
    gain = g1[...].reshape(1, D)
    for c in range(2):
        x = x_ref[IMG_LEN // 2 * c : IMG_LEN // 2 * (c + 1)].astype(F32).reshape(IMG_ROWS // 2, D)
        h = (normalize(x) * gain).astype(BF)
        kv[IMG_ROWS // 2 * c : IMG_ROWS // 2 * (c + 1), :] = mm(h, wqkv[:, D:]).astype(BF)
        if c == 0:
            x0[pl.ds(pl.multiple_of(step * IMG_BLOCK, IMG_BLOCK), IMG_BLOCK), :] = x[:IMG_BLOCK]
            h0 = h[:IMG_BLOCK]
    q = mm(h0, wqkv[:, :D]).astype(BF).astype(F32) * (HEAD**-0.5)
    head = lanes_head((IMG_BLOCK, D))
    queries = HEADS * IMG_BLOCK
    rows = lax.broadcasted_iota(jnp.int32, (queries, IMG_ROWS), 0)
    cols = lax.broadcasted_iota(jnp.int32, (queries, IMG_ROWS), 1)
    own = cols % IMG_BLOCK == rows % IMG_BLOCK
    q6 = jnp.concatenate([jnp.where(head == h, q, 0.0) for h in range(HEADS)], 0)
    s = mm_nt(q6.astype(BF), kv[:, :D])
    s = jnp.where(own, s, -1e30)
    e = jnp.exp(s - jnp.max(s, -1, keepdims=True))
    p = (e * (1.0 / jnp.sum(e, -1, keepdims=True))).astype(BF)
    r = mm(p, kv[:, D:])
    o = jnp.where(head == 0, r[0:IMG_BLOCK], 0.0)
    for h in range(1, HEADS):
        o = jnp.where(head == h, r[IMG_BLOCK * h : IMG_BLOCK * (h + 1)], o)
    att[pl.ds(pl.multiple_of(step * IMG_BLOCK, IMG_BLOCK), IMG_BLOCK), :] = o

    @pl.when(step == pl.num_programs(0) - 1)
    def _():
        x1 = x0[...] + mm(att[...].astype(BF), wout[...])
        h2 = (normalize(x1) * g2[...].reshape(1, D)).astype(BF)
        u, _ = gelu_parts(mm(h2, wup[...]))
        y = x1 + mm(u.astype(BF), wdown[...])
        e = mm(y.astype(BF), wproj[...])
        emb_ref[...] = (e * lax.rsqrt(jnp.sum(e * e, -1, keepdims=True) + EPS)).astype(BF)


def near(v):
    return pltpu.with_memory_space_constraint(v, pltpu.VMEM)


def away(v):
    return pltpu.with_memory_space_constraint(v, pltpu.HBM)


def cost(us):
    return pl.CostEstimate(flops=int(us * 1e9), bytes_accessed=int(us * 3e6), transcendentals=0)


def const_spec(shape):
    zeros = (0,) * len(shape)
    return pl.BlockSpec(shape, lambda *_: zeros, pipeline_mode=pl.Buffered(1))


def image_tower(x, g1, wqkv, wout, g2, wup, wdown, wproj):
    count = x.shape[1]
    return pl.pallas_call(
        image_kernel,
        grid=(count // IMG_BLOCK,),
        in_specs=[
            pl.BlockSpec((IMG_LEN, IMG_BLOCK, D), lambda i: (0, i, 0)),
            const_spec((D,)),
            const_spec((D, 3 * D)),
            const_spec((D, D)),
            const_spec((D,)),
            const_spec((D, FF)),
            const_spec((FF, D)),
            const_spec((D, D)),
        ],
        out_specs=pl.BlockSpec((count, D), lambda i: (0, 0)),
        out_shape=jax.ShapeDtypeStruct((count, D), BF),
        scratch_shapes=[
            pltpu.VMEM((IMG_ROWS, 2 * D), BF),
            pltpu.VMEM((count, D), F32),
            pltpu.VMEM((count, D), F32),
        ],
        compiler_params=ROOM,
        cost_estimate=cost(12),
        name="image_tower",
    )(*[away(v) for v in (x, g1, wqkv, wout, g2, wup, wdown, wproj)])


def pair_mask(lab_ref, pair):
    lab = lab_ref[0, :, PAIR * pair : PAIR * pair + PAIR].astype(F32)
    wide = jnp.broadcast_to(lab, (PAIR, PAIR))
    return wide == wide.T


def text_att_kernel(tok_ref, lab_ref, g1, wqkv, o_all, o_ref, qkv_ref, p_ref, h1_ref):
    x = tok_ref[...].astype(F32)
    h1 = (normalize(x) * g1[...].reshape(1, D)).astype(BF)
    h1_ref[...] = h1
    qkv = mm(h1, wqkv[...]).astype(BF)
    qkv_ref[...] = qkv
    low = lax.broadcasted_iota(jnp.int32, (PAIR, PAIR), 1) < HEAD
    for pair in range(2):
        rows = slice(PAIR * pair, PAIR * pair + PAIR)
        mask = pair_mask(lab_ref, pair)
        mask = jnp.concatenate([mask, mask], 0)
        for j in range(HEADS // 2):
            cols = slice(PAIR * j, PAIR * j + PAIR)
            q2 = qkv[rows, PAIR * j : PAIR * j + PAIR] * jnp.asarray(HEAD**-0.5, BF)
            k2 = qkv[rows, D + PAIR * j : D + PAIR * j + PAIR]
            v2 = qkv[rows, 2 * D + PAIR * j : 2 * D + PAIR * j + PAIR]
            zero = jnp.zeros_like(q2)
            q22 = jnp.concatenate([jnp.where(low, q2, zero), jnp.where(low, zero, q2)], 0)
            s = jnp.where(mask, mm_nt(q22, k2), -1e30)
            ex = jnp.exp(s - jnp.max(s, -1, keepdims=True))
            p = (ex * (1.0 / jnp.sum(ex, -1, keepdims=True))).astype(BF)
            p_ref[pair, j] = p
            v22 = jnp.concatenate([jnp.where(low, v2, zero), jnp.where(low, zero, v2)], 0)
            o = mm(jnp.concatenate([p[:PAIR], p[PAIR:]], 1), v22)
            o_ref[rows, cols] = o.astype(BF)
    o_all[held_rows(), :] = o_ref[...]


def text_mlp_kernel(
    tok_ref, o_ref, lab_ref, wout, g2, wup, wdown, wproj,
    h2_ref, c2_ref, gp_ref, pu_ref, pb_ref, e_ref, emb_ref, cnt_ref, pt, po,
):
    step = pl.program_id(0)
    tok = tok_ref[...]
    o = o_ref[held_rows(), :]
    x1 = tok.astype(F32) + mm(o, wout[...])
    c2 = x1 - row_mean(x1)
    c2_ref[...] = c2
    h2 = (c2 * lax.rsqrt(row_mean(c2 * c2) + EPS) * g2[...].reshape(1, D)).astype(BF)
    h2_ref[...] = h2
    hit = lax.broadcasted_iota(jnp.int32, (CAP_BLOCK, TOK_BLOCK), 0) == lab_ref[0]
    member = jnp.where(hit, 1.0, 0.0)
    caps = pl.ds(pl.multiple_of(step * CAP_BLOCK, CAP_BLOCK), CAP_BLOCK)
    member_b = member.astype(BF)
    pt[caps, :] = mm(member_b, tok)
    po[caps, :] = mm(member_b, o)
    cnt_ref[caps, :] = jnp.broadcast_to(jnp.sum(member, -1, keepdims=True), (CAP_BLOCK, 128))
    for k in range(FF // 512):
        cols = slice(512 * k, 512 * (k + 1))
        u, slope = gelu_parts(mm(h2, wup[:, cols]))
        gp_ref[:, cols] = slope.astype(BF)
        pu_ref[caps, cols] = mm(member_b, u.astype(BF))

    @pl.when(step == pl.num_programs(0) - 1)
    def _():
        total = pt[...] + wide_mm(po[...], wout[...]) + wide_mm(pu_ref[...], wdown[...])
        pooled = (total * (1.0 / cnt_ref[:, 0:1])).astype(BF)
        pb_ref[...] = pooled
        e = mm(pooled, wproj[...])
        e_ref[...] = e
        emb_ref[...] = (e * lax.rsqrt(jnp.sum(e * e, -1, keepdims=True) + EPS)).astype(BF)


def held_rows():
    return pl.ds(pl.multiple_of(pl.program_id(0) * TOK_BLOCK, TOK_BLOCK), TOK_BLOCK)


def token_rows(width):
    return pl.BlockSpec((TOK_BLOCK, width), lambda i: (i, 0))


def block_of(a, b):
    return pl.BlockSpec((1, a, b), lambda i: (i, 0, 0))


def whole(a, b):
    return pl.BlockSpec((a, b), lambda i: (0, 0))


def text_att(tok, lab, g1, wqkv):
    n = tok.shape[0]
    blocks = n // TOK_BLOCK
    shape = pltpu.HBM
    return pl.pallas_call(
        text_att_kernel,
        grid=(blocks,),
        in_specs=[token_rows(D), block_of(1, TOK_BLOCK), const_spec((D,)), const_spec((D, 3 * D))],
        out_specs=[
            VMEM,
            token_rows(D),
            token_rows(3 * D),
            pl.BlockSpec((2, 3, 2 * PAIR, PAIR), lambda i: (i, 0, 0, 0)),
            token_rows(D),
        ],
        out_shape=[
            pltpu.VMEM((n, D), BF), shape((n, D), BF), shape((n, 3 * D), BF),
            shape((2 * blocks, 3, 2 * PAIR, PAIR), BF), shape((n, D), BF),
        ],
        compiler_params=ROOM,
        cost_estimate=cost(9),
        name="text_att",
    )(away(tok), lab, g1, away(wqkv))


def text_mlp(tok, o, lab, wout, g2, wup, wdown, wproj):
    n = tok.shape[0]
    shape = pltpu.VMEM
    return pl.pallas_call(
        text_mlp_kernel,
        grid=(n // TOK_BLOCK,),
        in_specs=[
            token_rows(D), VMEM, block_of(1, TOK_BLOCK),
            const_spec((D, D)), const_spec((D,)), const_spec((D, FF)), const_spec((FF, D)), const_spec((D, D)),
        ],
        out_specs=[token_rows(D), token_rows(D), token_rows(FF)] + [VMEM] * 5,
        out_shape=[
            pltpu.HBM((n, D), BF), pltpu.HBM((n, D), F32), pltpu.HBM((n, FF), BF),
            shape((CAPS, FF), F32), shape((CAPS, D), BF), shape((CAPS, D), F32),
            shape((CAPS, D), BF), shape((CAPS, 128), F32),
        ],
        scratch_shapes=[pltpu.VMEM((CAPS, D), F32), pltpu.VMEM((CAPS, D), F32)],
        compiler_params=ROOM,
        cost_estimate=cost(11),
        name="text_mlp",
    )(tok, near(o), lab, wout, g2, wup, wdown, wproj)


def reorder(mine, row):
    return jnp.where(mine & 1 == 1, pltpu.roll(row, 64, 1), row)


def cosine_kernel(denom, scale_ref, mine_ref, emb, own, other, pair, g_ref, sum_ref):
    mine = mine_ref[0]
    scale = jnp.exp(jnp.full((1, 1), scale_ref[0], F32))
    g = jnp.concatenate([mm_nt(emb[...], own[...]), mm_nt(emb[...], other[...])], 1)
    g_ref[...] = g
    e = jnp.exp(g * scale)
    eg = e * g
    total = jnp.sum(e, -1, keepdims=True)
    hit = lax.broadcasted_iota(jnp.int32, g.shape, 1) == pair[...]
    own = jnp.sum(jnp.where(hit, g, 0.0), -1, keepdims=True)
    loss = jnp.sum(jnp.log(total) - 2.0 * scale * own, 0, keepdims=True)
    temp = jnp.sum(jnp.sum(eg, -1, keepdims=True) / total - 2.0 * own, 0, keepdims=True)
    n = g.shape[1] // 128
    for k, v in enumerate((jnp.sum(e, 0, keepdims=True), jnp.sum(eg, 0, keepdims=True))):
        for r in range(n):
            sum_ref[pl.ds(k * n + ((mine >> 1) ^ r), 1), :] = reorder(mine, v[:, 128 * r : 128 * (r + 1)])
    lane = lax.broadcasted_iota(jnp.int32, (8, 128), 1)
    sum_ref[2 * n :, :] = jnp.where(lane == 0, loss, jnp.where(lane == 1, temp, 0.0))


def times_images(dl, own, other):
    half = dl.shape[1] // 2
    return mm(dl[:, :half], own[...]) + mm(dl[:, half:], other[...])


def rows_kernel(denom, scale_ref, g_ref, own, other, pair, dt_ref):
    scale = jnp.exp(jnp.full((1, 1), scale_ref[0], F32))
    g = g_ref[...]
    e = jnp.exp(g * scale)
    hit = lax.broadcasted_iota(jnp.int32, g.shape, 1) == pair[...]
    p = e * (1.0 / jnp.sum(e, -1, keepdims=True))
    dl = jnp.where(hit, p - 2.0, p) * (scale * (1.0 / denom))
    dt_ref[...] = times_images(dl.astype(BF), own, other)


def quarter(mine, base, k, rows=48):
    far = (mine & 3) ^ k
    return pl.multiple_of(base + rows * ((far & 1) * 2 + (far >> 1)), 16)


def halves(mine, rows, send_ref, keep_ref, piece):
    for rel in range(8):
        ref = keep_ref if rel < 4 else send_ref
        at = (rel % 4) * rows
        if rows == 48:
            ref[at : at + 48, :] = piece((mine >> 2) ^ rel, 0).astype(BF)
            continue
        for k in range(4):
            ref[pl.ds(quarter(mine, at, k), 48), :] = piece((mine >> 2) ^ rel, k).astype(BF)


def block(acc, at, rows, col=0):
    return acc[pl.ds(pl.multiple_of(at * rows, 16), rows), D * col : D * (col + 1)]


def head_kernel(
    denom, scale_ref, mine_ref, g_ref, own, other, sums, dt_row, e_ref, pb, cnt, pu, wproj, wdown,
    sd_ref, kd_ref, sp_ref, kp_ref, du_ref, dy_ref, loss_out, temp_out, down, proj,
):
    mine = mine_ref[0]
    scale = jnp.exp(jnp.full((1, 1), scale_ref[0], F32))
    n = g_ref.shape[1] // 128

    def columns(k):
        return jnp.concatenate([reorder(mine, sums[pl.ds(k * n + ((mine >> 1) ^ r), 1), :]) for r in range(n)], 1)

    temp = jnp.sum(jnp.sum(sums[n : 2 * n, :] / sums[0:n, :], 0, keepdims=True), -1, keepdims=True)
    loss = jnp.sum(jnp.sum(jnp.log(sums[0:n, :]), 0, keepdims=True), -1, keepdims=True)
    loss_out[...] = (sums[2 * n : 2 * n + 1, 0:1] + loss) * (1.0 / denom)
    temp_out[...] = (sums[2 * n : 2 * n + 1, 1:2] + temp) * (scale * (1.0 / denom))
    inverse = 1.0 / columns(0)
    dl = jnp.exp(g_ref[...] * scale) * (inverse * (scale * (1.0 / denom)))
    dt = dt_row[...] + times_images(dl.astype(BF), own, other)
    e = e_ref[...]
    r = lax.rsqrt(jnp.sum(e * e, -1, keepdims=True) + EPS)
    de = (dt - e * (r * r * jnp.sum(dt * e, -1, keepdims=True))) * r
    de = de.astype(BF)
    dpooled = mm_nt(de, wproj[...])
    dy = dpooled * (1.0 / cnt[:, 0:1])
    dyb = dy.astype(BF)
    du = mm_nt(dyb, wdown[...])
    for i, piece in enumerate(split3(du)):
        for b in range(BLOCKS):
            du_ref[b, CAP_BLOCK * i : CAP_BLOCK * (i + 1), :] = piece[CAP_BLOCK * b : CAP_BLOCK * (b + 1)]
    for i, piece in enumerate(split3(dy)):
        for b in range(BLOCKS):
            dy_ref[b, CAP_BLOCK * i : CAP_BLOCK * (i + 1), :] = piece[CAP_BLOCK * b : CAP_BLOCK * (b + 1)]
    down[...] = mm_tn(jnp.concatenate(split3(pu[...]), 0), jnp.concatenate([dyb, dyb, dyb], 0))
    proj[...] = mm_tn(pb[...], de)
    halves(mine, 192, sd_ref, kd_ref, lambda at, k: block(down, at * 4 + k, 48))
    halves(mine, 48, sp_ref, kp_ref, lambda at, k: block(proj, at, 48))


def mlp_back_kernel(
    mine_ref, lab_ref, h2_all, gp_all, c2_all, du_ref, dy_ref, g2, wup,
    dx_all, dxb_all, send_ref, keep_ref, acc,
):
    step = pl.program_id(0)
    h2_ref, gp_ref, c2_ref = h2_all.at[held_rows()], gp_all.at[held_rows()], c2_all.at[held_rows()]
    dx_ref, dxb_ref = dx_all.at[held_rows()], dxb_all.at[held_rows()]

    @pl.when(step == 0)
    def _():
        acc[...] = jnp.zeros_like(acc)

    hit = lax.broadcasted_iota(jnp.int32, (3 * CAP_BLOCK, TOK_BLOCK), 0) % CAP_BLOCK == lab_ref[0]
    spread = jnp.where(hit, 1.0, 0.0).astype(BF)
    du = mm_tn(spread, du_ref[step])
    dz = (du * gp_ref[...].astype(F32)).astype(BF)
    dy = mm_tn(spread, dy_ref[step])
    dh = mm_nt(dz, wup[...])
    c2 = c2_ref[...]
    r = lax.rsqrt(row_mean(c2 * c2) + EPS)
    unit = c2 * r
    dn = dh * g2[...].reshape(1, D)
    dx = dy + r * (dn - row_mean(dn) - unit * row_mean(dn * unit))
    dx_ref[...] = dx
    dxb_ref[...] = dx.astype(BF)
    h2 = h2_ref[...]
    acc[...] += mm_tn(h2, dz)

    @pl.when(step == pl.num_programs(0) - 1)
    def _():
        halves(mine_ref[0], 192, send_ref, keep_ref, lambda at, k: block(acc, at, 48, k))


def att_back_kernel(
    mine_ref, qkv_all, p_all, dxb_all, dx_all, h1_ref, o_ref, tok_ref, wout, g1, wqkv,
    gtok_ref, send_ref, keep_ref, dqkv_all, acc,
):
    step = pl.program_id(0)
    qkv_ref, dxb_ref, dqkv_ref = qkv_all.at[held_rows()], dxb_all.at[held_rows()], dqkv_all.at[held_rows()]
    p_ref = p_all.at[pl.ds(2 * step, 2)]
    do = mm_nt(dxb_ref[...], wout[...]).astype(BF)
    low = lax.broadcasted_iota(jnp.int32, (PAIR, PAIR), 1) < HEAD
    zero = jnp.zeros((PAIR, PAIR), BF)
    half = HEAD**-0.5

    def twice(v):
        return jnp.concatenate([jnp.where(low, v, zero), jnp.where(low, zero, v)], 0)

    for pair in range(2):
        rows = slice(PAIR * pair, PAIR * pair + PAIR)
        for j in range(HEADS // 2):
            cols = slice(PAIR * j, PAIR * j + PAIR)
            q2 = qkv_ref[rows, PAIR * j : PAIR * j + PAIR]
            k2 = qkv_ref[rows, D + PAIR * j : D + PAIR * j + PAIR]
            v2 = qkv_ref[rows, 2 * D + PAIR * j : 2 * D + PAIR * j + PAIR]
            do2 = twice(do[rows, cols])
            pb = p_ref[pair, j]
            p = pb.astype(F32)
            dp = mm_nt(do2, v2)
            ds = (p * (dp - jnp.sum(dp * p, -1, keepdims=True))).astype(BF)
            dq = mm(jnp.concatenate([ds[:PAIR], ds[PAIR:]], 1), twice(k2)) * half
            dk = mm_tn(ds, twice(q2)) * half
            dv = mm_tn(pb, do2)
            dqkv_ref[rows, PAIR * j : PAIR * j + PAIR] = dq.astype(BF)
            dqkv_ref[rows, D + PAIR * j : D + PAIR * j + PAIR] = dk.astype(BF)
            dqkv_ref[rows, 2 * D + PAIR * j : 2 * D + PAIR * j + PAIR] = dv.astype(BF)
    x = tok_ref[...].astype(F32)
    centre = x - row_mean(x)
    r = lax.rsqrt(row_mean(centre * centre) + EPS)
    unit = centre * r
    dn = mm_nt(dqkv_ref[...], wqkv[...]) * g1[...].reshape(1, D)
    gtok_ref[...] = dx_all[held_rows(), :] + r * (dn - row_mean(dn) - unit * row_mean(dn * unit))

    @pl.when(step == pl.num_programs(0) - 1)
    def _():
        acc[:, :D] = mm_tn(o_ref[...], dxb_all[...])
        acc[:, D:] = mm_tn(h1_ref[...], dqkv_all[...])
        halves(mine_ref[0], 192, send_ref, keep_ref, lambda at, k: block(acc, at, 48, k))


def gain_of(grad, weight, gain):
    high, mid, _ = split3(grad * weight.astype(F32))
    ones = jnp.ones((8, grad.shape[1]), BF)
    total = mm_nt(ones, high) + mm_nt(ones, mid)
    return total[0:1] / gain.reshape(1, D)


def arrived(mine_ref, own, other, rows):
    for rel in range(8):
        src = own if rel < 4 else other
        yield (mine_ref[0] >> 2) ^ rel, src, (rel % 4) * rows


def spread_mlp_kernel(mine_ref, own, other, wup, g2, down_ref, up_ref, proj_ref, gain_ref):
    for at, src, row in arrived(mine_ref, own, other, 432):
        rows = pl.ds(pl.multiple_of(at * 48, 16), 48)
        for k in range(4):
            part = quarter(mine_ref[0], row, k, 96)
            down_ref[pl.ds(pl.multiple_of(at * 192 + 48 * k, 16), 48), :] = src[pl.ds(part, 48), :].astype(F32)
            up_ref[rows, D * k : D * (k + 1)] = src[pl.ds(pl.multiple_of(part + 48, 16), 48), :].astype(F32)
        proj_ref[rows, :] = src[row + 384 : row + 432, :].astype(F32)
    gain_ref[...] = gain_of(up_ref[...], wup[...], g2[...]).reshape(D)


def spread_att_kernel(mine_ref, own, other, wqkv, g1, out_ref, qkv_ref, gain_ref):
    for at, src, row in arrived(mine_ref, own, other, 192):
        rows = pl.ds(pl.multiple_of(at * 48, 16), 48)
        out_ref[rows, :] = src[pl.ds(quarter(mine_ref[0], row, 0), 48), :].astype(F32)
        for k in range(3):
            qkv_ref[rows, D * k : D * (k + 1)] = src[pl.ds(quarter(mine_ref[0], row, k + 1), 48), :].astype(F32)
    gain_ref[...] = gain_of(qkv_ref[...], wqkv[...], g1[...]).reshape(D)


def simple(kernel, outs, scratch=(), smem=0, us=3, name=None, held=(), held_out=True):
    def call(*args):
        args = [near(v) if i in held else v for i, v in enumerate(args)]
        return pl.pallas_call(
            kernel,
            in_specs=[SMEM] * smem + [VMEM] * (len(args) - smem),
            out_specs=[VMEM] * len(outs),
            out_shape=[(pltpu.VMEM if held_out else jax.ShapeDtypeStruct)(s, t) for s, t in outs],
            scratch_shapes=list(scratch),
            compiler_params=ROOM,
            cost_estimate=cost(us),
            name=name,
        )(*args)

    return call


def mlp_back(mine, lab, h2, gp, c2, du, dy, g2, wup):
    n = h2.shape[0]
    shape = pltpu.VMEM
    return pl.pallas_call(
        mlp_back_kernel,
        grid=(n // TOK_BLOCK,),
        in_specs=[SMEM, block_of(1, TOK_BLOCK)] + [VMEM] * 5 + [const_spec((D,)), const_spec((D, FF))],
        out_specs=[VMEM] * 4,
        out_shape=[shape((n, D), F32), shape((n, D), BF), shape((768, D), BF), shape((768, D), BF)],
        scratch_shapes=[pltpu.VMEM((D, FF), F32)],
        compiler_params=ROOM,
        cost_estimate=cost(9),
        name="mlp_back",
    )(mine, lab, near(h2), near(gp), near(c2), near(du), near(dy), g2, wup)


def att_back(mine, qkv, p, dxb, dx, h1, o, tok, wout, g1, wqkv):
    n = dxb.shape[0]
    return pl.pallas_call(
        att_back_kernel,
        grid=(n // TOK_BLOCK,),
        in_specs=[SMEM] + [VMEM] * 6 + [token_rows(D), const_spec((D, D)), const_spec((D,)), const_spec((D, 3 * D))],
        out_specs=[token_rows(D), VMEM, VMEM],
        out_shape=[pltpu.HBM((n, D), F32), pltpu.VMEM((768, D), BF), pltpu.VMEM((768, D), BF)],
        scratch_shapes=[pltpu.VMEM((n, 3 * D), BF), pltpu.VMEM((D, 4 * D), F32)],
        compiler_params=ROOM,
        cost_estimate=cost(14),
        name="att_back",
    )(mine, *[near(v) for v in (qkv, p, dxb, dx, h1, o)], tok, wout, g1, wqkv)


AXES = ("dp", "replica")


def swap(v, mask):
    return lax.ppermute(v, AXES, [(i, i ^ mask) for i in range(32)])


def plane(parts):
    return [swap(parts[m], 2 * m) for m in (1, 2, 3)]


def column(parts):
    return [swap(parts[m], 8 * m) for m in (1, 2, 3)]


def total_of(own, got):
    v = [own.astype(F32)] + [x.astype(F32) for x in got]
    return v[0] + v[1] if len(v) == 2 else (v[0] + v[1]) + (v[2] + v[3])


def added(own, got):
    return total_of(own, got).astype(BF)


def joined(own, got):
    return jnp.concatenate([own] + got, 0)


def shards(
    devices, tuned,
    text_tokens, segment_ids, pair_index, image_tokens,
    img_ln1, img_qkv, img_out, img_ln2, img_up, img_down, img_proj,
    txt_ln1, txt_qkv, txt_out, txt_ln2, txt_up, txt_down, txt_proj, log_scale,
):
    total = CAPS * devices
    denom = 2.0 * total
    row_of = jnp.arange(segment_ids.shape[0], dtype=jnp.int32) % (TOK_BLOCK // segment_ids.shape[1])
    lab = (segment_ids + PACK * row_of[:, None]).reshape(BLOCKS, 1, TOK_BLOCK)
    pair = pair_index
    if tuned:
        index = lax.axis_index(AXES)
        mine = ((index & 1) * 16 + ((index >> 1) & 3) * 4 + (index >> 3)).astype(jnp.int32).reshape(1)
        owner, row = pair // CAPS, pair % CAPS
        pair = (((owner & 1) * 16 + ((owner >> 1) & 3) * 4 + (owner >> 3)) ^ mine) * CAPS + row
    else:
        mine = jnp.zeros((1,), jnp.int32)
    pair = pair.reshape(CAPS, 1)
    lab, pair = lax.optimization_barrier((lab, pair))
    emb = image_tower(
        jnp.transpose(image_tokens, (1, 0, 2)), img_ln1, img_qkv, img_out, img_ln2, img_up, img_down, img_proj
    )
    if tuned:
        near = joined(emb, column([emb] * 4))
        o_now, o, qkv, p, h1 = text_att(text_tokens, lab, txt_ln1, txt_qkv)
        o_now, near = lax.optimization_barrier((o_now, near))
        got = plane([near] * 4)
    else:
        o_now, o, qkv, p, h1 = text_att(text_tokens, lab, txt_ln1, txt_qkv)
    h2, c2, gp, pu, pb, e, temb, cnt = text_mlp(text_tokens, o_now, lab, txt_out, txt_ln2, txt_up, txt_down, txt_proj)
    if tuned:
        near, got, temb = lax.optimization_barrier((near, got, temb))
        near = joined(near, got)
        own, other = near, swap(near, 1)
    else:
        own, other = jnp.split(lax.all_gather(emb, AXES, axis=0, tiled=True), 2)
    lines = total // 128
    g, sums = simple(
        functools.partial(cosine_kernel, denom),
        [((CAPS, total), F32), ((2 * lines + 8, 128), F32)],
        smem=2,
        us=3,
        name="cosine",
        held=(3, 4),
    )(log_scale, mine, temb, own, other, pair)
    (dt_row,) = simple(functools.partial(rows_kernel, denom), [((CAPS, D), F32)], smem=1, us=2, name="rows", held=(2, 3))(
        log_scale, g, own, other, pair
    )
    if tuned:
        sums = total_of(sums, [swap(sums, 1)])
        sums = total_of(sums, plane([sums] * 4))
        sums = total_of(sums, [swap(sums, 8)])
        sums = total_of(sums, [swap(sums, 16)])
    else:
        sums = lax.psum(sums, AXES)
    send_d, keep_d, send_p, keep_p, du, dy, loss, temp = simple(
        functools.partial(head_kernel, denom),
        [
            ((768, D), BF), ((768, D), BF), ((192, D), BF), ((192, D), BF),
            ((BLOCKS, 48, FF), BF), ((BLOCKS, 48, D), BF), ((1, 1), F32), ((1, 1), F32),
        ],
        [pltpu.VMEM((FF, D), F32), pltpu.VMEM((D, D), F32)],
        smem=2,
        us=5,
        name="head_back",
        held=(3, 4, 5),
    )(log_scale, mine, g, own, other, sums, dt_row, e, pb, cnt, pu, txt_proj, txt_down)
    dx, dxb, send_u, keep_u = mlp_back(mine, lab, h2, gp, c2, du, dy, txt_ln2, txt_up)

    def mlp_parts(d, u, p):
        both = jnp.concatenate([d.reshape(4, 4, 48, D), u.reshape(4, 4, 48, D)], 2).reshape(4, 384, D)
        return jnp.concatenate([both, p.reshape(4, 48, D)], 1)

    def spread_mlp(own, other):
        outs = [((FF, D), F32), ((D, FF), F32), ((D, D), F32), ((D,), F32)]
        return simple(spread_mlp_kernel, outs, smem=1, us=4, name="spread_mlp", held=(1, 2), held_out=False)(mine, own, other, txt_up, txt_ln2)

    def spread_att(own, other):
        outs = [((D, D), F32), ((D, 3 * D), F32), ((D,), F32)]
        return simple(spread_att_kernel, outs, smem=1, us=4, name="spread_att", held=(1, 2), held_out=False)(mine, own, other, txt_qkv, txt_ln1)

    if not tuned:
        grad_tokens, send_a, keep_a = att_back(
            mine, qkv, p, dxb, dx, h1, o, text_tokens, txt_out, txt_ln1, txt_qkv
        )
        sums = [keep_d, send_d, keep_u, send_u, keep_a, send_a, keep_p, send_p]
        d, d2, u, u2, a, a2, p, p2 = [v.astype(BF) for v in lax.psum([v.astype(F32) for v in sums], AXES)]
        grad_down, grad_up, grad_proj, gain2 = spread_mlp(
            mlp_parts(d, u, p).reshape(1728, D), mlp_parts(d2, u2, p2).reshape(1728, D)
        )
        grad_out, grad_qkv, gain1 = spread_att(a, a2)
    else:
        d = added(keep_d, [swap(send_d, 1)])
        pr = added(keep_p, [swap(send_p, 1)])
        m = mlp_parts(d, added(keep_u, [swap(send_u, 1)]), pr)
        dxb, m = lax.optimization_barrier((dxb, m))
        got = plane(m)
        grad_tokens, send_a, keep_a = att_back(
            mine, qkv, p, dxb, dx, h1, o, text_tokens, txt_out, txt_ln1, txt_qkv
        )
        other = swap(send_a, 1)
        got, keep_a = lax.optimization_barrier((got, keep_a))
        m = added(m[0], got)
        got = swap(m[192:], 8)
        a = added(keep_a, [other]).reshape(4, 192, D)
        got_a = plane(a)
        got, got_a[0] = lax.optimization_barrier((got, got_a[0]))
        m = added(joined(m[:192], [m[384:]]), [got])
        got = swap(m[96:], 16)
        got, got_a[1], got_a[2] = lax.optimization_barrier((got, got_a[1], got_a[2]))
        a = added(a[0], got_a)
        got_a = swap(a[96:], 8)
        m = added(joined(m[:96], [m[192:]]), [got])
        far = swap(m[:96], 16)
        a = added(a[:96], [got_a])
        got_a = swap(a[48:], 16)
        m = joined(m[:96], [far, m[96:]])
        m = joined(m[:192], [swap(m[:192], 8), m[192:]])
        got_m = plane([m] * 4)
        a = added(a[:48], [got_a])
        a = joined(a, [swap(a, 16)])
        a = joined(a, [swap(a, 8)])
        last, got_m[0], got_m[1] = lax.optimization_barrier((a, got_m[0], got_m[1]))
        got_a = plane([a, a, a, last])
        got_m[2], got_a[0], got_a[1] = lax.optimization_barrier((got_m[2], got_a[0], got_a[1]))
        m = joined(m, got_m)
        grad_down, grad_up, grad_proj, gain2 = spread_mlp(m, swap(m, 1))
        got_a, grad_up = lax.optimization_barrier((got_a, grad_up))
        a = joined(a, got_a)
        grad_out, grad_qkv, gain1 = spread_att(a, swap(a, 1))
    return (
        loss.reshape(1), grad_tokens, gain1, grad_qkv, grad_out, gain2,
        grad_up, grad_down, grad_proj, temp.reshape(1),
    )


def solution(mesh):
    both = ("dp", "replica")
    devices = mesh.shape["dp"] * mesh.shape["replica"]
    tuned = (mesh.shape["dp"], mesh.shape["replica"]) == (8, 4)
    rows = P(both, None)
    return jax.shard_map(
        functools.partial(shards, devices, tuned),
        mesh=mesh,
        in_specs=(rows, rows, P(both), P(both, None, None)) + (P(),) * 15,
        out_specs=(P(), rows) + (P(),) * 8,
        check_vma=False,
    )
```

```python
import functools
import math

import jax
import jax.numpy as jnp
from jax import lax
from jax.experimental import pallas as pl
from jax.experimental.pallas import tpu as pltpu
from jax.sharding import PartitionSpec as P

D = 384
HEADS = 6
HEAD = 64
FF = 1536
IMG_LEN = 50
PACK = 4
CAPS = 64
TOK_BLOCK = 256
CAP_BLOCK = 16
BLOCKS = 4
PAIR = 128
IMG_BLOCK = 16
IMG_ROWS = IMG_BLOCK * IMG_LEN
EPS = 1e-06

SMEM = pl.BlockSpec(memory_space=pltpu.SMEM)
VMEM = pl.BlockSpec(memory_space=pltpu.VMEM)
ROOM = pltpu.CompilerParams(vmem_limit_bytes=24 * 2**20)

BF = jnp.bfloat16
F32 = jnp.float32
GELU_K = math.sqrt(2.0 / math.pi)
GELU_C = 0.044715


def mm(a, b):
    return lax.dot_general(a, b, (((1,), (0,)), ((), ())), preferred_element_type=F32)


def mm_nt(a, b):
    return lax.dot_general(a, b, (((1,), (1,)), ((), ())), preferred_element_type=F32)


def mm_tn(a, b):
    return lax.dot_general(a, b, (((0,), (0,)), ((), ())), preferred_element_type=F32)


def row_mean(v):
    return jnp.sum(v, -1, keepdims=True) * (1.0 / D)


def normalize(v):
    centre = v - row_mean(v)
    return centre * lax.rsqrt(row_mean(centre * centre) + EPS)


def split3(v):
    high = v.astype(BF)
    rest = v - high.astype(F32)
    mid = rest.astype(BF)
    low = (rest - mid.astype(F32)).astype(BF)
    return high, mid, low


def wide_mm(v, w):
    high, mid, low = split3(v)
    n = v.shape[0]
    out = mm(jnp.concatenate([high, mid, low], 0), w)
    return out[:n] + out[n : 2 * n] + out[2 * n :]


def gelu_parts(z):
    z2 = z * z
    t = jnp.tanh(z * (z2 * (GELU_K * GELU_C) + GELU_K))
    hp = t * 0.5 + 0.5
    u = z * hp
    slope = hp + (u * (1.0 - hp)) * (z2 * (6.0 * GELU_K * GELU_C) + 2.0 * GELU_K)
    return u, slope


def lanes_head(shape):
    return lax.broadcasted_iota(jnp.int32, shape, len(shape) - 1) // HEAD


def image_kernel(x_ref, g1, wqkv, wout, g2, wup, wdown, wproj, emb_ref, kv, x0, att):
    step = pl.program_id(0)
    gain = g1[...].reshape(1, D)
    for c in range(2):
        x = x_ref[IMG_LEN // 2 * c : IMG_LEN // 2 * (c + 1)].astype(F32).reshape(IMG_ROWS // 2, D)
        h = (normalize(x) * gain).astype(BF)
        kv[IMG_ROWS // 2 * c : IMG_ROWS // 2 * (c + 1), :] = mm(h, wqkv[:, D:]).astype(BF)
        if c == 0:
            x0[pl.ds(pl.multiple_of(step * IMG_BLOCK, IMG_BLOCK), IMG_BLOCK), :] = x[:IMG_BLOCK]
            h0 = h[:IMG_BLOCK]
    q = mm(h0, wqkv[:, :D]).astype(BF).astype(F32) * (HEAD**-0.5)
    head = lanes_head((IMG_BLOCK, D))
    queries = HEADS * IMG_BLOCK
    rows = lax.broadcasted_iota(jnp.int32, (queries, IMG_ROWS), 0)
    cols = lax.broadcasted_iota(jnp.int32, (queries, IMG_ROWS), 1)
    own = cols % IMG_BLOCK == rows % IMG_BLOCK
    q6 = jnp.concatenate([jnp.where(head == h, q, 0.0) for h in range(HEADS)], 0)
    s = mm_nt(q6.astype(BF), kv[:, :D])
    s = jnp.where(own, s, -1e30)
    e = jnp.exp(s - jnp.max(s, -1, keepdims=True))
    p = (e * (1.0 / jnp.sum(e, -1, keepdims=True))).astype(BF)
    r = mm(p, kv[:, D:])
    o = jnp.where(head == 0, r[0:IMG_BLOCK], 0.0)
    for h in range(1, HEADS):
        o = jnp.where(head == h, r[IMG_BLOCK * h : IMG_BLOCK * (h + 1)], o)
    att[pl.ds(pl.multiple_of(step * IMG_BLOCK, IMG_BLOCK), IMG_BLOCK), :] = o

    @pl.when(step == pl.num_programs(0) - 1)
    def _():
        x1 = x0[...] + mm(att[...].astype(BF), wout[...])
        h2 = (normalize(x1) * g2[...].reshape(1, D)).astype(BF)
        u, _ = gelu_parts(mm(h2, wup[...]))
        y = x1 + mm(u.astype(BF), wdown[...])
        e = mm(y.astype(BF), wproj[...])
        emb_ref[...] = (e * lax.rsqrt(jnp.sum(e * e, -1, keepdims=True) + EPS)).astype(BF)


def near(v):
    return pltpu.with_memory_space_constraint(v, pltpu.VMEM)


def away(v):
    return pltpu.with_memory_space_constraint(v, pltpu.HBM)


def cost(us):
    return pl.CostEstimate(flops=int(us * 1e9), bytes_accessed=int(us * 3e6), transcendentals=0)


def const_spec(shape):
    zeros = (0,) * len(shape)
    return pl.BlockSpec(shape, lambda *_: zeros, pipeline_mode=pl.Buffered(1))


def image_tower(x, g1, wqkv, wout, g2, wup, wdown, wproj):
    count = x.shape[1]
    return pl.pallas_call(
        image_kernel,
        grid=(count // IMG_BLOCK,),
        in_specs=[
            pl.BlockSpec((IMG_LEN, IMG_BLOCK, D), lambda i: (0, i, 0)),
            const_spec((D,)),
            const_spec((D, 3 * D)),
            const_spec((D, D)),
            const_spec((D,)),
            const_spec((D, FF)),
            const_spec((FF, D)),
            const_spec((D, D)),
        ],
        out_specs=pl.BlockSpec((count, D), lambda i: (0, 0)),
        out_shape=jax.ShapeDtypeStruct((count, D), BF),
        scratch_shapes=[
            pltpu.VMEM((IMG_ROWS, 2 * D), BF),
            pltpu.VMEM((count, D), F32),
            pltpu.VMEM((count, D), F32),
        ],
        compiler_params=ROOM,
        cost_estimate=cost(12),
        name="image_tower",
    )(*[away(v) for v in (x, g1, wqkv, wout, g2, wup, wdown, wproj)])


def pair_mask(lab_ref, pair):
    lab = lab_ref[0, :, PAIR * pair : PAIR * pair + PAIR].astype(F32)
    wide = jnp.broadcast_to(lab, (PAIR, PAIR))
    return wide == wide.T


def text_att_kernel(tok_ref, lab_ref, g1, wqkv, o_all, o_ref, qkv_ref, p_ref, h1_ref):
    x = tok_ref[...].astype(F32)
    h1 = (normalize(x) * g1[...].reshape(1, D)).astype(BF)
    h1_ref[...] = h1
    qkv = mm(h1, wqkv[...]).astype(BF)
    qkv_ref[...] = qkv
    low = lax.broadcasted_iota(jnp.int32, (PAIR, PAIR), 1) < HEAD
    for pair in range(2):
        rows = slice(PAIR * pair, PAIR * pair + PAIR)
        mask = pair_mask(lab_ref, pair)
        mask = jnp.concatenate([mask, mask], 0)
        for j in range(HEADS // 2):
            cols = slice(PAIR * j, PAIR * j + PAIR)
            q2 = qkv[rows, PAIR * j : PAIR * j + PAIR] * jnp.asarray(HEAD**-0.5, BF)
            k2 = qkv[rows, D + PAIR * j : D + PAIR * j + PAIR]
            v2 = qkv[rows, 2 * D + PAIR * j : 2 * D + PAIR * j + PAIR]
            zero = jnp.zeros_like(q2)
            q22 = jnp.concatenate([jnp.where(low, q2, zero), jnp.where(low, zero, q2)], 0)
            s = jnp.where(mask, mm_nt(q22, k2), -1e30)
            ex = jnp.exp(s - jnp.max(s, -1, keepdims=True))
            p = (ex * (1.0 / jnp.sum(ex, -1, keepdims=True))).astype(BF)
            p_ref[pair, j] = p
            v22 = jnp.concatenate([jnp.where(low, v2, zero), jnp.where(low, zero, v2)], 0)
            o = mm(jnp.concatenate([p[:PAIR], p[PAIR:]], 1), v22)
            o_ref[rows, cols] = o.astype(BF)
    o_all[held_rows(), :] = o_ref[...]


def text_mlp_kernel(
    tok_ref, o_ref, lab_ref, wout, g2, wup, wdown, wproj,
    h2_ref, c2_ref, gp_ref, pu_ref, pb_ref, e_ref, emb_ref, cnt_ref, pt, po,
):
    step = pl.program_id(0)
    tok = tok_ref[...]
    o = o_ref[held_rows(), :]
    x1 = tok.astype(F32) + mm(o, wout[...])
    c2 = x1 - row_mean(x1)
    c2_ref[...] = c2
    h2 = (c2 * lax.rsqrt(row_mean(c2 * c2) + EPS) * g2[...].reshape(1, D)).astype(BF)
    h2_ref[...] = h2
    hit = lax.broadcasted_iota(jnp.int32, (CAP_BLOCK, TOK_BLOCK), 0) == lab_ref[0]
    member = jnp.where(hit, 1.0, 0.0)
    caps = pl.ds(pl.multiple_of(step * CAP_BLOCK, CAP_BLOCK), CAP_BLOCK)
    member_b = member.astype(BF)
    pt[caps, :] = mm(member_b, tok)
    po[caps, :] = mm(member_b, o)
    cnt_ref[caps, :] = jnp.broadcast_to(jnp.sum(member, -1, keepdims=True), (CAP_BLOCK, 128))
    for k in range(FF // 512):
        cols = slice(512 * k, 512 * (k + 1))
        u, slope = gelu_parts(mm(h2, wup[:, cols]))
        gp_ref[:, cols] = slope.astype(BF)
        pu_ref[caps, cols] = mm(member_b, u.astype(BF))

    @pl.when(step == pl.num_programs(0) - 1)
    def _():
        total = pt[...] + wide_mm(po[...], wout[...]) + wide_mm(pu_ref[...], wdown[...])
        pooled = (total * (1.0 / cnt_ref[:, 0:1])).astype(BF)
        pb_ref[...] = pooled
        e = mm(pooled, wproj[...])
        e_ref[...] = e
        emb_ref[...] = (e * lax.rsqrt(jnp.sum(e * e, -1, keepdims=True) + EPS)).astype(BF)


def held_rows():
    return pl.ds(pl.multiple_of(pl.program_id(0) * TOK_BLOCK, TOK_BLOCK), TOK_BLOCK)


def token_rows(width):
    return pl.BlockSpec((TOK_BLOCK, width), lambda i: (i, 0))


def block_of(a, b):
    return pl.BlockSpec((1, a, b), lambda i: (i, 0, 0))


def whole(a, b):
    return pl.BlockSpec((a, b), lambda i: (0, 0))


def text_att(tok, lab, g1, wqkv):
    n = tok.shape[0]
    blocks = n // TOK_BLOCK
    shape = pltpu.HBM
    return pl.pallas_call(
        text_att_kernel,
        grid=(blocks,),
        in_specs=[token_rows(D), block_of(1, TOK_BLOCK), const_spec((D,)), const_spec((D, 3 * D))],
        out_specs=[
            VMEM,
            token_rows(D),
            token_rows(3 * D),
            pl.BlockSpec((2, 3, 2 * PAIR, PAIR), lambda i: (i, 0, 0, 0)),
            token_rows(D),
        ],
        out_shape=[
            pltpu.VMEM((n, D), BF), shape((n, D), BF), shape((n, 3 * D), BF),
            shape((2 * blocks, 3, 2 * PAIR, PAIR), BF), shape((n, D), BF),
        ],
        compiler_params=ROOM,
        cost_estimate=cost(9),
        name="text_att",
    )(away(tok), lab, g1, away(wqkv))


def text_mlp(tok, o, lab, wout, g2, wup, wdown, wproj):
    n = tok.shape[0]
    shape = pltpu.VMEM
    return pl.pallas_call(
        text_mlp_kernel,
        grid=(n // TOK_BLOCK,),
        in_specs=[
            token_rows(D), VMEM, block_of(1, TOK_BLOCK),
            const_spec((D, D)), const_spec((D,)), const_spec((D, FF)), const_spec((FF, D)), const_spec((D, D)),
        ],
        out_specs=[token_rows(D), token_rows(D), token_rows(FF)] + [VMEM] * 5,
        out_shape=[
            pltpu.HBM((n, D), BF), pltpu.HBM((n, D), F32), pltpu.HBM((n, FF), BF),
            shape((CAPS, FF), F32), shape((CAPS, D), BF), shape((CAPS, D), F32),
            shape((CAPS, D), BF), shape((CAPS, 128), F32),
        ],
        scratch_shapes=[pltpu.VMEM((CAPS, D), F32), pltpu.VMEM((CAPS, D), F32)],
        compiler_params=ROOM,
        cost_estimate=cost(11),
        name="text_mlp",
    )(tok, near(o), lab, wout, g2, wup, wdown, wproj)


def reorder(mine, row):
    return jnp.where(mine & 1 == 1, pltpu.roll(row, 64, 1), row)


def cosine_kernel(denom, scale_ref, mine_ref, emb, own, other, pair, g_ref, sum_ref):
    mine = mine_ref[0]
    scale = jnp.exp(jnp.full((1, 1), scale_ref[0], F32))
    g = jnp.concatenate([mm_nt(emb[...], own[...]), mm_nt(emb[...], other[...])], 1)
    g_ref[...] = g
    e = jnp.exp(g * scale)
    eg = e * g
    total = jnp.sum(e, -1, keepdims=True)
    hit = lax.broadcasted_iota(jnp.int32, g.shape, 1) == pair[...]
    own = jnp.sum(jnp.where(hit, g, 0.0), -1, keepdims=True)
    loss = jnp.sum(jnp.log(total) - 2.0 * scale * own, 0, keepdims=True)
    temp = jnp.sum(jnp.sum(eg, -1, keepdims=True) / total - 2.0 * own, 0, keepdims=True)
    n = g.shape[1] // 128
    for k, v in enumerate((jnp.sum(e, 0, keepdims=True), jnp.sum(eg, 0, keepdims=True))):
        for r in range(n):
            sum_ref[pl.ds(k * n + ((mine >> 1) ^ r), 1), :] = reorder(mine, v[:, 128 * r : 128 * (r + 1)])
    lane = lax.broadcasted_iota(jnp.int32, (8, 128), 1)
    sum_ref[2 * n :, :] = jnp.where(lane == 0, loss, jnp.where(lane == 1, temp, 0.0))


def times_images(dl, own, other):
    half = dl.shape[1] // 2
    return mm(dl[:, :half], own[...]) + mm(dl[:, half:], other[...])


def rows_kernel(denom, scale_ref, g_ref, own, other, pair, dt_ref):
    scale = jnp.exp(jnp.full((1, 1), scale_ref[0], F32))
    g = g_ref[...]
    e = jnp.exp(g * scale)
    hit = lax.broadcasted_iota(jnp.int32, g.shape, 1) == pair[...]
    p = e * (1.0 / jnp.sum(e, -1, keepdims=True))
    dl = jnp.where(hit, p - 2.0, p) * (scale * (1.0 / denom))
    dt_ref[...] = times_images(dl.astype(BF), own, other)


def quarter(mine, base, k, rows=48):
    far = (mine & 3) ^ k
    return pl.multiple_of(base + rows * ((far & 1) * 2 + (far >> 1)), 16)


def halves(mine, rows, send_ref, keep_ref, piece):
    for rel in range(8):
        ref = keep_ref if rel < 4 else send_ref
        at = (rel % 4) * rows
        if rows == 48:
            ref[at : at + 48, :] = piece((mine >> 2) ^ rel, 0).astype(BF)
            continue
        for k in range(4):
            ref[pl.ds(quarter(mine, at, k), 48), :] = piece((mine >> 2) ^ rel, k).astype(BF)


def block(acc, at, rows, col=0):
    return acc[pl.ds(pl.multiple_of(at * rows, 16), rows), D * col : D * (col + 1)]


def head_kernel(
    denom, scale_ref, mine_ref, g_ref, own, other, sums, dt_row, e_ref, pb, cnt, pu, wproj, wdown,
    sd_ref, kd_ref, sp_ref, kp_ref, du_ref, dy_ref, loss_out, temp_out, down, proj,
):
    mine = mine_ref[0]
    scale = jnp.exp(jnp.full((1, 1), scale_ref[0], F32))
    n = g_ref.shape[1] // 128

    def columns(k):
        return jnp.concatenate([reorder(mine, sums[pl.ds(k * n + ((mine >> 1) ^ r), 1), :]) for r in range(n)], 1)

    temp = jnp.sum(jnp.sum(sums[n : 2 * n, :] / sums[0:n, :], 0, keepdims=True), -1, keepdims=True)
    loss = jnp.sum(jnp.sum(jnp.log(sums[0:n, :]), 0, keepdims=True), -1, keepdims=True)
    loss_out[...] = (sums[2 * n : 2 * n + 1, 0:1] + loss) * (1.0 / denom)
    temp_out[...] = (sums[2 * n : 2 * n + 1, 1:2] + temp) * (scale * (1.0 / denom))
    inverse = 1.0 / columns(0)
    dl = jnp.exp(g_ref[...] * scale) * (inverse * (scale * (1.0 / denom)))
    dt = dt_row[...] + times_images(dl.astype(BF), own, other)
    e = e_ref[...]
    r = lax.rsqrt(jnp.sum(e * e, -1, keepdims=True) + EPS)
    de = (dt - e * (r * r * jnp.sum(dt * e, -1, keepdims=True))) * r
    de = de.astype(BF)
    dpooled = mm_nt(de, wproj[...])
    dy = dpooled * (1.0 / cnt[:, 0:1])
    dyb = dy.astype(BF)
    du = mm_nt(dyb, wdown[...])
    for i, piece in enumerate(split3(du)):
        for b in range(BLOCKS):
            du_ref[b, CAP_BLOCK * i : CAP_BLOCK * (i + 1), :] = piece[CAP_BLOCK * b : CAP_BLOCK * (b + 1)]
    for i, piece in enumerate(split3(dy)):
        for b in range(BLOCKS):
            dy_ref[b, CAP_BLOCK * i : CAP_BLOCK * (i + 1), :] = piece[CAP_BLOCK * b : CAP_BLOCK * (b + 1)]
    down[...] = mm_tn(jnp.concatenate(split3(pu[...]), 0), jnp.concatenate([dyb, dyb, dyb], 0))
    proj[...] = mm_tn(pb[...], de)
    halves(mine, 192, sd_ref, kd_ref, lambda at, k: block(down, at * 4 + k, 48))
    halves(mine, 48, sp_ref, kp_ref, lambda at, k: block(proj, at, 48))


def mlp_back_kernel(
    mine_ref, lab_ref, h2_all, gp_all, c2_all, du_ref, dy_ref, g2, wup,
    dx_all, dxb_all, send_ref, keep_ref, acc,
):
    step = pl.program_id(0)
    h2_ref, gp_ref, c2_ref = h2_all.at[held_rows()], gp_all.at[held_rows()], c2_all.at[held_rows()]
    dx_ref, dxb_ref = dx_all.at[held_rows()], dxb_all.at[held_rows()]

    @pl.when(step == 0)
    def _():
        acc[...] = jnp.zeros_like(acc)

    hit = lax.broadcasted_iota(jnp.int32, (3 * CAP_BLOCK, TOK_BLOCK), 0) % CAP_BLOCK == lab_ref[0]
    spread = jnp.where(hit, 1.0, 0.0).astype(BF)
    du = mm_tn(spread, du_ref[step])
    dz = (du * gp_ref[...].astype(F32)).astype(BF)
    dy = mm_tn(spread, dy_ref[step])
    dh = mm_nt(dz, wup[...])
    c2 = c2_ref[...]
    r = lax.rsqrt(row_mean(c2 * c2) + EPS)
    unit = c2 * r
    dn = dh * g2[...].reshape(1, D)
    dx = dy + r * (dn - row_mean(dn) - unit * row_mean(dn * unit))
    dx_ref[...] = dx
    dxb_ref[...] = dx.astype(BF)
    h2 = h2_ref[...]
    acc[...] += mm_tn(h2, dz)

    @pl.when(step == pl.num_programs(0) - 1)
    def _():
        halves(mine_ref[0], 192, send_ref, keep_ref, lambda at, k: block(acc, at, 48, k))


def att_back_kernel(
    mine_ref, qkv_all, p_all, dxb_all, dx_all, h1_ref, o_ref, tok_ref, wout, g1, wqkv,
    gtok_ref, send_ref, keep_ref, dqkv_all, acc,
):
    step = pl.program_id(0)
    qkv_ref, dxb_ref, dqkv_ref = qkv_all.at[held_rows()], dxb_all.at[held_rows()], dqkv_all.at[held_rows()]
    p_ref = p_all.at[pl.ds(2 * step, 2)]
    do = mm_nt(dxb_ref[...], wout[...]).astype(BF)
    low = lax.broadcasted_iota(jnp.int32, (PAIR, PAIR), 1) < HEAD
    zero = jnp.zeros((PAIR, PAIR), BF)
    half = HEAD**-0.5

    def twice(v):
        return jnp.concatenate([jnp.where(low, v, zero), jnp.where(low, zero, v)], 0)

    for pair in range(2):
        rows = slice(PAIR * pair, PAIR * pair + PAIR)
        for j in range(HEADS // 2):
            cols = slice(PAIR * j, PAIR * j + PAIR)
            q2 = qkv_ref[rows, PAIR * j : PAIR * j + PAIR]
            k2 = qkv_ref[rows, D + PAIR * j : D + PAIR * j + PAIR]
            v2 = qkv_ref[rows, 2 * D + PAIR * j : 2 * D + PAIR * j + PAIR]
            do2 = twice(do[rows, cols])
            pb = p_ref[pair, j]
            p = pb.astype(F32)
            dp = mm_nt(do2, v2)
            ds = (p * (dp - jnp.sum(dp * p, -1, keepdims=True))).astype(BF)
            dq = mm(jnp.concatenate([ds[:PAIR], ds[PAIR:]], 1), twice(k2)) * half
            dk = mm_tn(ds, twice(q2)) * half
            dv = mm_tn(pb, do2)
            dqkv_ref[rows, PAIR * j : PAIR * j + PAIR] = dq.astype(BF)
            dqkv_ref[rows, D + PAIR * j : D + PAIR * j + PAIR] = dk.astype(BF)
            dqkv_ref[rows, 2 * D + PAIR * j : 2 * D + PAIR * j + PAIR] = dv.astype(BF)
    x = tok_ref[...].astype(F32)
    centre = x - row_mean(x)
    r = lax.rsqrt(row_mean(centre * centre) + EPS)
    unit = centre * r
    dn = mm_nt(dqkv_ref[...], wqkv[...]) * g1[...].reshape(1, D)
    gtok_ref[...] = dx_all[held_rows(), :] + r * (dn - row_mean(dn) - unit * row_mean(dn * unit))

    @pl.when(step == pl.num_programs(0) - 1)
    def _():
        acc[:, :D] = mm_tn(o_ref[...], dxb_all[...])
        acc[:, D:] = mm_tn(h1_ref[...], dqkv_all[...])
        halves(mine_ref[0], 192, send_ref, keep_ref, lambda at, k: block(acc, at, 48, k))


def gain_of(grad, weight, gain):
    high, mid, _ = split3(grad * weight.astype(F32))
    ones = jnp.ones((8, grad.shape[1]), BF)
    total = mm_nt(ones, high) + mm_nt(ones, mid)
    return total[0:1] / gain.reshape(1, D)


def arrived(mine_ref, own, other, rows):
    for rel in range(8):
        src = own if rel < 4 else other
        yield (mine_ref[0] >> 2) ^ rel, src, (rel % 4) * rows


def spread_mlp_kernel(mine_ref, own, other, wup, g2, down_ref, up_ref, proj_ref, gain_ref):
    for at, src, row in arrived(mine_ref, own, other, 432):
        rows = pl.ds(pl.multiple_of(at * 48, 16), 48)
        for k in range(4):
            part = quarter(mine_ref[0], row, k, 96)
            down_ref[pl.ds(pl.multiple_of(at * 192 + 48 * k, 16), 48), :] = src[pl.ds(part, 48), :].astype(F32)
            up_ref[rows, D * k : D * (k + 1)] = src[pl.ds(pl.multiple_of(part + 48, 16), 48), :].astype(F32)
        proj_ref[rows, :] = src[row + 384 : row + 432, :].astype(F32)
    gain_ref[...] = gain_of(up_ref[...], wup[...], g2[...]).reshape(D)


def spread_att_kernel(mine_ref, own, other, wqkv, g1, out_ref, qkv_ref, gain_ref):
    for at, src, row in arrived(mine_ref, own, other, 192):
        rows = pl.ds(pl.multiple_of(at * 48, 16), 48)
        out_ref[rows, :] = src[pl.ds(quarter(mine_ref[0], row, 0), 48), :].astype(F32)
        for k in range(3):
            qkv_ref[rows, D * k : D * (k + 1)] = src[pl.ds(quarter(mine_ref[0], row, k + 1), 48), :].astype(F32)
    gain_ref[...] = gain_of(qkv_ref[...], wqkv[...], g1[...]).reshape(D)


def simple(kernel, outs, scratch=(), smem=0, us=3, name=None, held=(), held_out=True):
    def call(*args):
        args = [near(v) if i in held else v for i, v in enumerate(args)]
        return pl.pallas_call(
            kernel,
            in_specs=[SMEM] * smem + [VMEM] * (len(args) - smem),
            out_specs=[VMEM] * len(outs),
            out_shape=[(pltpu.VMEM if held_out else jax.ShapeDtypeStruct)(s, t) for s, t in outs],
            scratch_shapes=list(scratch),
            compiler_params=ROOM,
            cost_estimate=cost(us),
            name=name,
        )(*args)

    return call


def mlp_back(mine, lab, h2, gp, c2, du, dy, g2, wup):
    n = h2.shape[0]
    shape = pltpu.VMEM
    return pl.pallas_call(
        mlp_back_kernel,
        grid=(n // TOK_BLOCK,),
        in_specs=[SMEM, block_of(1, TOK_BLOCK)] + [VMEM] * 5 + [const_spec((D,)), const_spec((D, FF))],
        out_specs=[VMEM] * 4,
        out_shape=[shape((n, D), F32), shape((n, D), BF), shape((768, D), BF), shape((768, D), BF)],
        scratch_shapes=[pltpu.VMEM((D, FF), F32)],
        compiler_params=ROOM,
        cost_estimate=cost(9),
        name="mlp_back",
    )(mine, lab, near(h2), near(gp), near(c2), near(du), near(dy), g2, wup)


def att_back(mine, qkv, p, dxb, dx, h1, o, tok, wout, g1, wqkv):
    n = dxb.shape[0]
    return pl.pallas_call(
        att_back_kernel,
        grid=(n // TOK_BLOCK,),
        in_specs=[SMEM] + [VMEM] * 6 + [token_rows(D), const_spec((D, D)), const_spec((D,)), const_spec((D, 3 * D))],
        out_specs=[token_rows(D), VMEM, VMEM],
        out_shape=[pltpu.HBM((n, D), F32), pltpu.VMEM((768, D), BF), pltpu.VMEM((768, D), BF)],
        scratch_shapes=[pltpu.VMEM((n, 3 * D), BF), pltpu.VMEM((D, 4 * D), F32)],
        compiler_params=ROOM,
        cost_estimate=cost(14),
        name="att_back",
    )(mine, *[near(v) for v in (qkv, p, dxb, dx, h1, o)], tok, wout, g1, wqkv)


AXES = ("dp", "replica")


def swap(v, mask):
    return lax.ppermute(v, AXES, [(i, i ^ mask) for i in range(32)])


def plane(parts):
    return [swap(parts[m], 2 * m) for m in (1, 2, 3)]


def column(parts):
    return [swap(parts[m], 8 * m) for m in (1, 2, 3)]


def total_of(own, got):
    v = [own.astype(F32)] + [x.astype(F32) for x in got]
    return v[0] + v[1] if len(v) == 2 else (v[0] + v[1]) + (v[2] + v[3])


def added(own, got):
    return total_of(own, got).astype(BF)


def joined(own, got):
    return jnp.concatenate([own] + got, 0)


def shards(
    devices, tuned,
    text_tokens, segment_ids, pair_index, image_tokens,
    img_ln1, img_qkv, img_out, img_ln2, img_up, img_down, img_proj,
    txt_ln1, txt_qkv, txt_out, txt_ln2, txt_up, txt_down, txt_proj, log_scale,
):
    total = CAPS * devices
    denom = 2.0 * total
    row_of = jnp.arange(segment_ids.shape[0], dtype=jnp.int32) % (TOK_BLOCK // segment_ids.shape[1])
    lab = (segment_ids + PACK * row_of[:, None]).reshape(BLOCKS, 1, TOK_BLOCK)
    pair = pair_index
    if tuned:
        index = lax.axis_index(AXES)
        mine = ((index & 1) * 16 + ((index >> 1) & 3) * 4 + (index >> 3)).astype(jnp.int32).reshape(1)
        owner, row = pair // CAPS, pair % CAPS
        pair = (((owner & 1) * 16 + ((owner >> 1) & 3) * 4 + (owner >> 3)) ^ mine) * CAPS + row
    else:
        mine = jnp.zeros((1,), jnp.int32)
    pair = pair.reshape(CAPS, 1)
    lab, pair = lax.optimization_barrier((lab, pair))
    emb = image_tower(
        jnp.transpose(image_tokens, (1, 0, 2)), img_ln1, img_qkv, img_out, img_ln2, img_up, img_down, img_proj
    )
    if tuned:
        near = joined(emb, column([emb] * 4))
        o_now, o, qkv, p, h1 = text_att(text_tokens, lab, txt_ln1, txt_qkv)
        o_now, near = lax.optimization_barrier((o_now, near))
        got = plane([near] * 4)
    else:
        o_now, o, qkv, p, h1 = text_att(text_tokens, lab, txt_ln1, txt_qkv)
    h2, c2, gp, pu, pb, e, temb, cnt = text_mlp(text_tokens, o_now, lab, txt_out, txt_ln2, txt_up, txt_down, txt_proj)
    if tuned:
        near, got, temb = lax.optimization_barrier((near, got, temb))
        near = joined(near, got)
        own, other = near, swap(near, 1)
    else:
        own, other = jnp.split(lax.all_gather(emb, AXES, axis=0, tiled=True), 2)
    lines = total // 128
    g, sums = simple(
        functools.partial(cosine_kernel, denom),
        [((CAPS, total), F32), ((2 * lines + 8, 128), F32)],
        smem=2,
        us=3,
        name="cosine",
        held=(3, 4),
    )(log_scale, mine, temb, own, other, pair)
    (dt_row,) = simple(functools.partial(rows_kernel, denom), [((CAPS, D), F32)], smem=1, us=2, name="rows", held=(2, 3))(
        log_scale, g, own, other, pair
    )
    if tuned:
        sums = total_of(sums, [swap(sums, 1)])
        sums = total_of(sums, plane([sums] * 4))
        sums = total_of(sums, [swap(sums, 8)])
        sums = total_of(sums, [swap(sums, 16)])
    else:
        sums = lax.psum(sums, AXES)
    send_d, keep_d, send_p, keep_p, du, dy, loss, temp = simple(
        functools.partial(head_kernel, denom),
        [
            ((768, D), BF), ((768, D), BF), ((192, D), BF), ((192, D), BF),
            ((BLOCKS, 48, FF), BF), ((BLOCKS, 48, D), BF), ((1, 1), F32), ((1, 1), F32),
        ],
        [pltpu.VMEM((FF, D), F32), pltpu.VMEM((D, D), F32)],
        smem=2,
        us=5,
        name="head_back",
        held=(3, 4, 5),
    )(log_scale, mine, g, own, other, sums, dt_row, e, pb, cnt, pu, txt_proj, txt_down)
    dx, dxb, send_u, keep_u = mlp_back(mine, lab, h2, gp, c2, du, dy, txt_ln2, txt_up)

    def mlp_parts(d, u, p):
        both = jnp.concatenate([d.reshape(4, 4, 48, D), u.reshape(4, 4, 48, D)], 2).reshape(4, 384, D)
        return jnp.concatenate([both, p.reshape(4, 48, D)], 1)

    def spread_mlp(own, other):
        outs = [((FF, D), F32), ((D, FF), F32), ((D, D), F32), ((D,), F32)]
        return simple(spread_mlp_kernel, outs, smem=1, us=4, name="spread_mlp", held=(1, 2), held_out=False)(mine, own, other, txt_up, txt_ln2)

    def spread_att(own, other):
        outs = [((D, D), F32), ((D, 3 * D), F32), ((D,), F32)]
        return simple(spread_att_kernel, outs, smem=1, us=4, name="spread_att", held=(1, 2), held_out=False)(mine, own, other, txt_qkv, txt_ln1)

    if not tuned:
        grad_tokens, send_a, keep_a = att_back(
            mine, qkv, p, dxb, dx, h1, o, text_tokens, txt_out, txt_ln1, txt_qkv
        )
        sums = [keep_d, send_d, keep_u, send_u, keep_a, send_a, keep_p, send_p]
        d, d2, u, u2, a, a2, p, p2 = [v.astype(BF) for v in lax.psum([v.astype(F32) for v in sums], AXES)]
        grad_down, grad_up, grad_proj, gain2 = spread_mlp(
            mlp_parts(d, u, p).reshape(1728, D), mlp_parts(d2, u2, p2).reshape(1728, D)
        )
        grad_out, grad_qkv, gain1 = spread_att(a, a2)
    else:
        d = added(keep_d, [swap(send_d, 1)])
        pr = added(keep_p, [swap(send_p, 1)])
        m = mlp_parts(d, added(keep_u, [swap(send_u, 1)]), pr)
        dxb, m = lax.optimization_barrier((dxb, m))
        got = plane(m)
        grad_tokens, send_a, keep_a = att_back(
            mine, qkv, p, dxb, dx, h1, o, text_tokens, txt_out, txt_ln1, txt_qkv
        )
        other = swap(send_a, 1)
        got, keep_a = lax.optimization_barrier((got, keep_a))
        m = added(m[0], got)
        got = swap(m[192:], 8)
        a = added(keep_a, [other]).reshape(4, 192, D)
        got_a = plane(a)
        got, got_a[0] = lax.optimization_barrier((got, got_a[0]))
        m = added(joined(m[:192], [m[384:]]), [got])
        got = swap(m[96:], 16)
        got, got_a[1], got_a[2] = lax.optimization_barrier((got, got_a[1], got_a[2]))
        a = added(a[0], got_a)
        got_a = swap(a[96:], 8)
        m = added(joined(m[:96], [m[192:]]), [got])
        far = swap(m[:96], 16)
        a = added(a[:96], [got_a])
        got_a = swap(a[48:], 16)
        m = joined(m[:96], [far, m[96:]])
        m = joined(m[:192], [swap(m[:192], 8), m[192:]])
        got_m = plane([m] * 4)
        a, m = lax.optimization_barrier((added(a[:48], [got_a]), m))
        a = joined(a, [swap(a, 16)])
        a = joined(a, [swap(a, 8)])
        last, got_m[0], got_m[1] = lax.optimization_barrier((a, got_m[0], got_m[1]))
        got_a = plane([a, a, a, last])
        got_m[2], got_a[0], got_a[1] = lax.optimization_barrier((got_m[2], got_a[0], got_a[1]))
        m = joined(m, got_m)
        grad_down, grad_up, grad_proj, gain2 = spread_mlp(m, swap(m, 1))
        got_a, grad_up = lax.optimization_barrier((got_a, grad_up))
        a = joined(a, got_a)
        grad_out, grad_qkv, gain1 = spread_att(a, swap(a, 1))
    return (
        loss.reshape(1), grad_tokens, gain1, grad_qkv, grad_out, gain2,
        grad_up, grad_down, grad_proj, temp.reshape(1),
    )


def solution(mesh):
    both = ("dp", "replica")
    devices = mesh.shape["dp"] * mesh.shape["replica"]
    tuned = (mesh.shape["dp"], mesh.shape["replica"]) == (8, 4)
    rows = P(both, None)
    return jax.shard_map(
        functools.partial(shards, devices, tuned),
        mesh=mesh,
        in_specs=(rows, rows, P(both), P(both, None, None)) + (P(),) * 15,
        out_specs=(P(), rows) + (P(),) * 8,
        check_vma=False,
    )
```

```python
import functools
import math

import jax
import jax.numpy as jnp
from jax import lax
from jax.experimental import pallas as pl
from jax.experimental.pallas import tpu as pltpu
from jax.sharding import PartitionSpec as P

D = 384
HEADS = 6
HEAD = 64
FF = 1536
IMG_LEN = 50
PACK = 4
CAPS = 64
TOK_BLOCK = 256
CAP_BLOCK = 16
BLOCKS = 4
PAIR = 128
IMG_BLOCK = 16
IMG_ROWS = IMG_BLOCK * IMG_LEN
EPS = 1e-06

SMEM = pl.BlockSpec(memory_space=pltpu.SMEM)
VMEM = pl.BlockSpec(memory_space=pltpu.VMEM)
ROOM = pltpu.CompilerParams(vmem_limit_bytes=24 * 2**20)

BF = jnp.bfloat16
F32 = jnp.float32
GELU_K = math.sqrt(2.0 / math.pi)
GELU_C = 0.044715


def mm(a, b):
    return lax.dot_general(a, b, (((1,), (0,)), ((), ())), preferred_element_type=F32)


def mm_nt(a, b):
    return lax.dot_general(a, b, (((1,), (1,)), ((), ())), preferred_element_type=F32)


def mm_tn(a, b):
    return lax.dot_general(a, b, (((0,), (0,)), ((), ())), preferred_element_type=F32)


def row_mean(v):
    return jnp.sum(v, -1, keepdims=True) * (1.0 / D)


def normalize(v):
    centre = v - row_mean(v)
    return centre * lax.rsqrt(row_mean(centre * centre) + EPS)


def split3(v):
    high = v.astype(BF)
    rest = v - high.astype(F32)
    mid = rest.astype(BF)
    low = (rest - mid.astype(F32)).astype(BF)
    return high, mid, low


def wide_mm(v, w):
    high, mid, low = split3(v)
    n = v.shape[0]
    out = mm(jnp.concatenate([high, mid, low], 0), w)
    return out[:n] + out[n : 2 * n] + out[2 * n :]


def gelu_parts(z):
    z2 = z * z
    t = jnp.tanh(z * (z2 * (GELU_K * GELU_C) + GELU_K))
    hp = t * 0.5 + 0.5
    u = z * hp
    slope = hp + (u * (1.0 - hp)) * (z2 * (6.0 * GELU_K * GELU_C) + 2.0 * GELU_K)
    return u, slope


def lanes_head(shape):
    return lax.broadcasted_iota(jnp.int32, shape, len(shape) - 1) // HEAD


def image_kernel(x_ref, g1, wqkv, wout, g2, wup, wdown, wproj, emb_ref, kv, x0, att):
    step = pl.program_id(0)
    gain = g1[...].reshape(1, D)
    for c in range(2):
        x = x_ref[IMG_LEN // 2 * c : IMG_LEN // 2 * (c + 1)].astype(F32).reshape(IMG_ROWS // 2, D)
        h = (normalize(x) * gain).astype(BF)
        kv[IMG_ROWS // 2 * c : IMG_ROWS // 2 * (c + 1), :] = mm(h, wqkv[:, D:]).astype(BF)
        if c == 0:
            x0[pl.ds(pl.multiple_of(step * IMG_BLOCK, IMG_BLOCK), IMG_BLOCK), :] = x[:IMG_BLOCK]
            h0 = h[:IMG_BLOCK]
    q = mm(h0, wqkv[:, :D]).astype(BF).astype(F32) * (HEAD**-0.5)
    head = lanes_head((IMG_BLOCK, D))
    queries = HEADS * IMG_BLOCK
    rows = lax.broadcasted_iota(jnp.int32, (queries, IMG_ROWS), 0)
    cols = lax.broadcasted_iota(jnp.int32, (queries, IMG_ROWS), 1)
    own = cols % IMG_BLOCK == rows % IMG_BLOCK
    q6 = jnp.concatenate([jnp.where(head == h, q, 0.0) for h in range(HEADS)], 0)
    s = mm_nt(q6.astype(BF), kv[:, :D])
    s = jnp.where(own, s, -1e30)
    e = jnp.exp(s - jnp.max(s, -1, keepdims=True))
    p = (e * (1.0 / jnp.sum(e, -1, keepdims=True))).astype(BF)
    r = mm(p, kv[:, D:])
    o = jnp.where(head == 0, r[0:IMG_BLOCK], 0.0)
    for h in range(1, HEADS):
        o = jnp.where(head == h, r[IMG_BLOCK * h : IMG_BLOCK * (h + 1)], o)
    att[pl.ds(pl.multiple_of(step * IMG_BLOCK, IMG_BLOCK), IMG_BLOCK), :] = o

    @pl.when(step == pl.num_programs(0) - 1)
    def _():
        x1 = x0[...] + mm(att[...].astype(BF), wout[...])
        h2 = (normalize(x1) * g2[...].reshape(1, D)).astype(BF)
        u, _ = gelu_parts(mm(h2, wup[...]))
        y = x1 + mm(u.astype(BF), wdown[...])
        e = mm(y.astype(BF), wproj[...])
        emb_ref[...] = (e * lax.rsqrt(jnp.sum(e * e, -1, keepdims=True) + EPS)).astype(BF)


def near(v):
    return pltpu.with_memory_space_constraint(v, pltpu.VMEM)


def away(v):
    return pltpu.with_memory_space_constraint(v, pltpu.HBM)


def cost(us):
    return pl.CostEstimate(flops=int(us * 1e9), bytes_accessed=int(us * 3e6), transcendentals=0)


def const_spec(shape):
    zeros = (0,) * len(shape)
    return pl.BlockSpec(shape, lambda *_: zeros, pipeline_mode=pl.Buffered(1))


def image_tower(x, g1, wqkv, wout, g2, wup, wdown, wproj):
    count = x.shape[1]
    return pl.pallas_call(
        image_kernel,
        grid=(count // IMG_BLOCK,),
        in_specs=[
            pl.BlockSpec((IMG_LEN, IMG_BLOCK, D), lambda i: (0, i, 0)),
            const_spec((D,)),
            const_spec((D, 3 * D)),
            const_spec((D, D)),
            const_spec((D,)),
            const_spec((D, FF)),
            const_spec((FF, D)),
            const_spec((D, D)),
        ],
        out_specs=pl.BlockSpec((count, D), lambda i: (0, 0)),
        out_shape=jax.ShapeDtypeStruct((count, D), BF),
        scratch_shapes=[
            pltpu.VMEM((IMG_ROWS, 2 * D), BF),
            pltpu.VMEM((count, D), F32),
            pltpu.VMEM((count, D), F32),
        ],
        compiler_params=ROOM,
        cost_estimate=cost(12),
        name="image_tower",
    )(*[away(v) for v in (x, g1, wqkv, wout, g2, wup, wdown, wproj)])


def pair_mask(lab_ref, pair):
    lab = lab_ref[0, :, PAIR * pair : PAIR * pair + PAIR].astype(F32)
    wide = jnp.broadcast_to(lab, (PAIR, PAIR))
    return wide == wide.T


def text_att_kernel(tok_ref, lab_ref, g1, wqkv, o_all, o_ref, qkv_ref, p_ref, h1_ref):
    x = tok_ref[...].astype(F32)
    h1 = (normalize(x) * g1[...].reshape(1, D)).astype(BF)
    h1_ref[...] = h1
    qkv = mm(h1, wqkv[...]).astype(BF)
    qkv_ref[...] = qkv
    low = lax.broadcasted_iota(jnp.int32, (PAIR, PAIR), 1) < HEAD
    for pair in range(2):
        rows = slice(PAIR * pair, PAIR * pair + PAIR)
        mask = pair_mask(lab_ref, pair)
        mask = jnp.concatenate([mask, mask], 0)
        for j in range(HEADS // 2):
            cols = slice(PAIR * j, PAIR * j + PAIR)
            q2 = qkv[rows, PAIR * j : PAIR * j + PAIR] * jnp.asarray(HEAD**-0.5, BF)
            k2 = qkv[rows, D + PAIR * j : D + PAIR * j + PAIR]
            v2 = qkv[rows, 2 * D + PAIR * j : 2 * D + PAIR * j + PAIR]
            zero = jnp.zeros_like(q2)
            q22 = jnp.concatenate([jnp.where(low, q2, zero), jnp.where(low, zero, q2)], 0)
            s = jnp.where(mask, mm_nt(q22, k2), -1e30)
            ex = jnp.exp(s - jnp.max(s, -1, keepdims=True))
            p = (ex * (1.0 / jnp.sum(ex, -1, keepdims=True))).astype(BF)
            p_ref[pair, j] = p
            v22 = jnp.concatenate([jnp.where(low, v2, zero), jnp.where(low, zero, v2)], 0)
            o = mm(jnp.concatenate([p[:PAIR], p[PAIR:]], 1), v22)
            o_ref[rows, cols] = o.astype(BF)
    o_all[held_rows(), :] = o_ref[...]


def text_mlp_kernel(
    tok_ref, o_ref, lab_ref, wout, g2, wup, wdown, wproj,
    h2_ref, c2_ref, gp_ref, pu_ref, pb_ref, e_ref, emb_ref, cnt_ref, pt, po,
):
    step = pl.program_id(0)
    tok = tok_ref[...]
    o = o_ref[held_rows(), :]
    x1 = tok.astype(F32) + mm(o, wout[...])
    c2 = x1 - row_mean(x1)
    c2_ref[...] = c2
    h2 = (c2 * lax.rsqrt(row_mean(c2 * c2) + EPS) * g2[...].reshape(1, D)).astype(BF)
    h2_ref[...] = h2
    hit = lax.broadcasted_iota(jnp.int32, (CAP_BLOCK, TOK_BLOCK), 0) == lab_ref[0]
    member = jnp.where(hit, 1.0, 0.0)
    caps = pl.ds(pl.multiple_of(step * CAP_BLOCK, CAP_BLOCK), CAP_BLOCK)
    member_b = member.astype(BF)
    pt[caps, :] = mm(member_b, tok)
    po[caps, :] = mm(member_b, o)
    cnt_ref[caps, :] = jnp.broadcast_to(jnp.sum(member, -1, keepdims=True), (CAP_BLOCK, 128))
    for k in range(FF // 512):
        cols = slice(512 * k, 512 * (k + 1))
        u, slope = gelu_parts(mm(h2, wup[:, cols]))
        gp_ref[:, cols] = slope.astype(BF)
        pu_ref[caps, cols] = mm(member_b, u.astype(BF))

    @pl.when(step == pl.num_programs(0) - 1)
    def _():
        total = pt[...] + wide_mm(po[...], wout[...]) + wide_mm(pu_ref[...], wdown[...])
        pooled = (total * (1.0 / cnt_ref[:, 0:1])).astype(BF)
        pb_ref[...] = pooled
        e = mm(pooled, wproj[...])
        e_ref[...] = e
        emb_ref[...] = (e * lax.rsqrt(jnp.sum(e * e, -1, keepdims=True) + EPS)).astype(BF)


def held_rows():
    return pl.ds(pl.multiple_of(pl.program_id(0) * TOK_BLOCK, TOK_BLOCK), TOK_BLOCK)


def token_rows(width):
    return pl.BlockSpec((TOK_BLOCK, width), lambda i: (i, 0))


def block_of(a, b):
    return pl.BlockSpec((1, a, b), lambda i: (i, 0, 0))


def whole(a, b):
    return pl.BlockSpec((a, b), lambda i: (0, 0))


def text_att(tok, lab, g1, wqkv):
    n = tok.shape[0]
    blocks = n // TOK_BLOCK
    shape = pltpu.HBM
    return pl.pallas_call(
        text_att_kernel,
        grid=(blocks,),
        in_specs=[token_rows(D), block_of(1, TOK_BLOCK), const_spec((D,)), const_spec((D, 3 * D))],
        out_specs=[
            VMEM,
            token_rows(D),
            token_rows(3 * D),
            pl.BlockSpec((2, 3, 2 * PAIR, PAIR), lambda i: (i, 0, 0, 0)),
            token_rows(D),
        ],
        out_shape=[
            pltpu.VMEM((n, D), BF), shape((n, D), BF), shape((n, 3 * D), BF),
            shape((2 * blocks, 3, 2 * PAIR, PAIR), BF), shape((n, D), BF),
        ],
        compiler_params=ROOM,
        cost_estimate=cost(9),
        name="text_att",
    )(away(tok), lab, g1, away(wqkv))


def text_mlp(tok, o, lab, wout, g2, wup, wdown, wproj):
    n = tok.shape[0]
    shape = pltpu.VMEM
    return pl.pallas_call(
        text_mlp_kernel,
        grid=(n // TOK_BLOCK,),
        in_specs=[
            token_rows(D), VMEM, block_of(1, TOK_BLOCK),
            const_spec((D, D)), const_spec((D,)), const_spec((D, FF)), const_spec((FF, D)), const_spec((D, D)),
        ],
        out_specs=[token_rows(D), token_rows(D), token_rows(FF)] + [VMEM] * 5,
        out_shape=[
            pltpu.HBM((n, D), BF), pltpu.HBM((n, D), F32), pltpu.HBM((n, FF), BF),
            shape((CAPS, FF), F32), shape((CAPS, D), BF), shape((CAPS, D), F32),
            shape((CAPS, D), BF), shape((CAPS, 128), F32),
        ],
        scratch_shapes=[pltpu.VMEM((CAPS, D), F32), pltpu.VMEM((CAPS, D), F32)],
        compiler_params=ROOM,
        cost_estimate=cost(11),
        name="text_mlp",
    )(tok, near(o), lab, wout, g2, wup, wdown, wproj)


def reorder(mine, row):
    return jnp.where(mine & 1 == 1, pltpu.roll(row, 64, 1), row)


def cosine_kernel(denom, scale_ref, mine_ref, emb, own, other, pair, g_ref, sum_ref):
    mine = mine_ref[0]
    scale = jnp.exp(jnp.full((1, 1), scale_ref[0], F32))
    g = jnp.concatenate([mm_nt(emb[...], own[...]), mm_nt(emb[...], other[...])], 1)
    g_ref[...] = g
    e = jnp.exp(g * scale)
    eg = e * g
    total = jnp.sum(e, -1, keepdims=True)
    hit = lax.broadcasted_iota(jnp.int32, g.shape, 1) == pair[...]
    own = jnp.sum(jnp.where(hit, g, 0.0), -1, keepdims=True)
    loss = jnp.sum(jnp.log(total) - 2.0 * scale * own, 0, keepdims=True)
    temp = jnp.sum(jnp.sum(eg, -1, keepdims=True) / total - 2.0 * own, 0, keepdims=True)
    n = g.shape[1] // 128
    for k, v in enumerate((jnp.sum(e, 0, keepdims=True), jnp.sum(eg, 0, keepdims=True))):
        for r in range(n):
            sum_ref[pl.ds(k * n + ((mine >> 1) ^ r), 1), :] = reorder(mine, v[:, 128 * r : 128 * (r + 1)])
    lane = lax.broadcasted_iota(jnp.int32, (8, 128), 1)
    sum_ref[2 * n :, :] = jnp.where(lane == 0, loss, jnp.where(lane == 1, temp, 0.0))


def times_images(dl, own, other):
    half = dl.shape[1] // 2
    return mm(dl[:, :half], own[...]) + mm(dl[:, half:], other[...])


def rows_kernel(denom, scale_ref, g_ref, own, other, pair, dt_ref):
    scale = jnp.exp(jnp.full((1, 1), scale_ref[0], F32))
    g = g_ref[...]
    e = jnp.exp(g * scale)
    hit = lax.broadcasted_iota(jnp.int32, g.shape, 1) == pair[...]
    p = e * (1.0 / jnp.sum(e, -1, keepdims=True))
    dl = jnp.where(hit, p - 2.0, p) * (scale * (1.0 / denom))
    dt_ref[...] = times_images(dl.astype(BF), own, other)


def quarter(mine, base, k, rows=48):
    far = (mine & 3) ^ k
    return pl.multiple_of(base + rows * ((far & 1) * 2 + (far >> 1)), 16)


def halves(mine, rows, send_ref, keep_ref, piece):
    for rel in range(8):
        ref = keep_ref if rel < 4 else send_ref
        at = (rel % 4) * rows
        if rows == 48:
            ref[at : at + 48, :] = piece((mine >> 2) ^ rel, 0).astype(BF)
            continue
        for k in range(4):
            ref[pl.ds(quarter(mine, at, k), 48), :] = piece((mine >> 2) ^ rel, k).astype(BF)


def block(acc, at, rows, col=0):
    return acc[pl.ds(pl.multiple_of(at * rows, 16), rows), D * col : D * (col + 1)]


def head_kernel(
    denom, scale_ref, mine_ref, g_ref, own, other, sums, dt_row, e_ref, pb, cnt, pu, wproj, wdown,
    sd_ref, kd_ref, sp_ref, kp_ref, du_ref, dy_ref, loss_out, temp_out, down, proj,
):
    mine = mine_ref[0]
    scale = jnp.exp(jnp.full((1, 1), scale_ref[0], F32))
    n = g_ref.shape[1] // 128

    def columns(k):
        return jnp.concatenate([reorder(mine, sums[pl.ds(k * n + ((mine >> 1) ^ r), 1), :]) for r in range(n)], 1)

    temp = jnp.sum(jnp.sum(sums[n : 2 * n, :] / sums[0:n, :], 0, keepdims=True), -1, keepdims=True)
    loss = jnp.sum(jnp.sum(jnp.log(sums[0:n, :]), 0, keepdims=True), -1, keepdims=True)
    loss_out[...] = (sums[2 * n : 2 * n + 1, 0:1] + loss) * (1.0 / denom)
    temp_out[...] = (sums[2 * n : 2 * n + 1, 1:2] + temp) * (scale * (1.0 / denom))
    inverse = 1.0 / columns(0)
    dl = jnp.exp(g_ref[...] * scale) * (inverse * (scale * (1.0 / denom)))
    dt = dt_row[...] + times_images(dl.astype(BF), own, other)
    e = e_ref[...]
    r = lax.rsqrt(jnp.sum(e * e, -1, keepdims=True) + EPS)
    de = (dt - e * (r * r * jnp.sum(dt * e, -1, keepdims=True))) * r
    de = de.astype(BF)
    dpooled = mm_nt(de, wproj[...])
    dy = dpooled * (1.0 / cnt[:, 0:1])
    dyb = dy.astype(BF)
    du = mm_nt(dyb, wdown[...])
    for i, piece in enumerate(split3(du)):
        for b in range(BLOCKS):
            du_ref[b, CAP_BLOCK * i : CAP_BLOCK * (i + 1), :] = piece[CAP_BLOCK * b : CAP_BLOCK * (b + 1)]
    for i, piece in enumerate(split3(dy)):
        for b in range(BLOCKS):
            dy_ref[b, CAP_BLOCK * i : CAP_BLOCK * (i + 1), :] = piece[CAP_BLOCK * b : CAP_BLOCK * (b + 1)]
    down[...] = mm_tn(jnp.concatenate(split3(pu[...]), 0), jnp.concatenate([dyb, dyb, dyb], 0))
    proj[...] = mm_tn(pb[...], de)
    halves(mine, 192, sd_ref, kd_ref, lambda at, k: block(down, at * 4 + k, 48))
    halves(mine, 48, sp_ref, kp_ref, lambda at, k: block(proj, at, 48))


def mlp_back_kernel(
    mine_ref, lab_ref, h2_all, gp_all, c2_all, du_ref, dy_ref, g2, wup,
    dx_all, dxb_all, send_ref, keep_ref, acc,
):
    step = pl.program_id(0)
    h2_ref, gp_ref, c2_ref = h2_all.at[held_rows()], gp_all.at[held_rows()], c2_all.at[held_rows()]
    dx_ref, dxb_ref = dx_all.at[held_rows()], dxb_all.at[held_rows()]

    @pl.when(step == 0)
    def _():
        acc[...] = jnp.zeros_like(acc)

    hit = lax.broadcasted_iota(jnp.int32, (3 * CAP_BLOCK, TOK_BLOCK), 0) % CAP_BLOCK == lab_ref[0]
    spread = jnp.where(hit, 1.0, 0.0).astype(BF)
    du = mm_tn(spread, du_ref[step])
    dz = (du * gp_ref[...].astype(F32)).astype(BF)
    dy = mm_tn(spread, dy_ref[step])
    dh = mm_nt(dz, wup[...])
    c2 = c2_ref[...]
    r = lax.rsqrt(row_mean(c2 * c2) + EPS)
    unit = c2 * r
    dn = dh * g2[...].reshape(1, D)
    dx = dy + r * (dn - row_mean(dn) - unit * row_mean(dn * unit))
    dx_ref[...] = dx
    dxb_ref[...] = dx.astype(BF)
    h2 = h2_ref[...]
    acc[...] += mm_tn(h2, dz)

    @pl.when(step == pl.num_programs(0) - 1)
    def _():
        halves(mine_ref[0], 192, send_ref, keep_ref, lambda at, k: block(acc, at, 48, k))


def att_back_kernel(
    mine_ref, qkv_all, p_all, dxb_all, dx_all, h1_ref, o_ref, tok_ref, wout, g1, wqkv,
    gtok_ref, send_ref, keep_ref, dqkv_all, acc,
):
    step = pl.program_id(0)
    qkv_ref, dxb_ref, dqkv_ref = qkv_all.at[held_rows()], dxb_all.at[held_rows()], dqkv_all.at[held_rows()]
    p_ref = p_all.at[pl.ds(2 * step, 2)]
    do = mm_nt(dxb_ref[...], wout[...]).astype(BF)
    low = lax.broadcasted_iota(jnp.int32, (PAIR, PAIR), 1) < HEAD
    zero = jnp.zeros((PAIR, PAIR), BF)
    half = HEAD**-0.5

    def twice(v):
        return jnp.concatenate([jnp.where(low, v, zero), jnp.where(low, zero, v)], 0)

    for pair in range(2):
        rows = slice(PAIR * pair, PAIR * pair + PAIR)
        for j in range(HEADS // 2):
            cols = slice(PAIR * j, PAIR * j + PAIR)
            q2 = qkv_ref[rows, PAIR * j : PAIR * j + PAIR]
            k2 = qkv_ref[rows, D + PAIR * j : D + PAIR * j + PAIR]
            v2 = qkv_ref[rows, 2 * D + PAIR * j : 2 * D + PAIR * j + PAIR]
            do2 = twice(do[rows, cols])
            pb = p_ref[pair, j]
            p = pb.astype(F32)
            dp = mm_nt(do2, v2)
            ds = (p * (dp - jnp.sum(dp * p, -1, keepdims=True))).astype(BF)
            dq = mm(jnp.concatenate([ds[:PAIR], ds[PAIR:]], 1), twice(k2)) * half
            dk = mm_tn(ds, twice(q2)) * half
            dv = mm_tn(pb, do2)
            dqkv_ref[rows, PAIR * j : PAIR * j + PAIR] = dq.astype(BF)
            dqkv_ref[rows, D + PAIR * j : D + PAIR * j + PAIR] = dk.astype(BF)
            dqkv_ref[rows, 2 * D + PAIR * j : 2 * D + PAIR * j + PAIR] = dv.astype(BF)
    x = tok_ref[...].astype(F32)
    centre = x - row_mean(x)
    r = lax.rsqrt(row_mean(centre * centre) + EPS)
    unit = centre * r
    dn = mm_nt(dqkv_ref[...], wqkv[...]) * g1[...].reshape(1, D)
    gtok_ref[...] = dx_all[held_rows(), :] + r * (dn - row_mean(dn) - unit * row_mean(dn * unit))

    @pl.when(step == pl.num_programs(0) - 1)
    def _():
        acc[:, :D] = mm_tn(o_ref[...], dxb_all[...])
        acc[:, D:] = mm_tn(h1_ref[...], dqkv_all[...])
        halves(mine_ref[0], 192, send_ref, keep_ref, lambda at, k: block(acc, at, 48, k))


def gain_of(grad, weight, gain):
    high, mid, _ = split3(grad * weight.astype(F32))
    ones = jnp.ones((8, grad.shape[1]), BF)
    total = mm_nt(ones, high) + mm_nt(ones, mid)
    return total[0:1] / gain.reshape(1, D)


def arrived(mine_ref, own, other, rows):
    for rel in range(8):
        src = own if rel < 4 else other
        yield (mine_ref[0] >> 2) ^ rel, src, (rel % 4) * rows


def spread_mlp_kernel(mine_ref, own, other, wup, g2, down_ref, up_ref, proj_ref, gain_ref):
    for at, src, row in arrived(mine_ref, own, other, 432):
        rows = pl.ds(pl.multiple_of(at * 48, 16), 48)
        for k in range(4):
            part = quarter(mine_ref[0], row, k, 96)
            down_ref[pl.ds(pl.multiple_of(at * 192 + 48 * k, 16), 48), :] = src[pl.ds(part, 48), :].astype(F32)
            up_ref[rows, D * k : D * (k + 1)] = src[pl.ds(pl.multiple_of(part + 48, 16), 48), :].astype(F32)
        proj_ref[rows, :] = src[row + 384 : row + 432, :].astype(F32)
    gain_ref[...] = gain_of(up_ref[...], wup[...], g2[...]).reshape(D)


def spread_att_kernel(mine_ref, own, other, wqkv, g1, out_ref, qkv_ref, gain_ref):
    for at, src, row in arrived(mine_ref, own, other, 192):
        rows = pl.ds(pl.multiple_of(at * 48, 16), 48)
        out_ref[rows, :] = src[pl.ds(quarter(mine_ref[0], row, 0), 48), :].astype(F32)
        for k in range(3):
            qkv_ref[rows, D * k : D * (k + 1)] = src[pl.ds(quarter(mine_ref[0], row, k + 1), 48), :].astype(F32)
    gain_ref[...] = gain_of(qkv_ref[...], wqkv[...], g1[...]).reshape(D)


def simple(kernel, outs, scratch=(), smem=0, us=3, name=None, held=(), held_out=True):
    def call(*args):
        args = [near(v) if i in held else v for i, v in enumerate(args)]
        return pl.pallas_call(
            kernel,
            in_specs=[SMEM] * smem + [VMEM] * (len(args) - smem),
            out_specs=[VMEM] * len(outs),
            out_shape=[(pltpu.VMEM if held_out else jax.ShapeDtypeStruct)(s, t) for s, t in outs],
            scratch_shapes=list(scratch),
            compiler_params=ROOM,
            cost_estimate=cost(us),
            name=name,
        )(*args)

    return call


def mlp_back(mine, lab, h2, gp, c2, du, dy, g2, wup):
    n = h2.shape[0]
    shape = pltpu.VMEM
    return pl.pallas_call(
        mlp_back_kernel,
        grid=(n // TOK_BLOCK,),
        in_specs=[SMEM, block_of(1, TOK_BLOCK)] + [VMEM] * 5 + [const_spec((D,)), const_spec((D, FF))],
        out_specs=[VMEM] * 4,
        out_shape=[shape((n, D), F32), shape((n, D), BF), shape((768, D), BF), shape((768, D), BF)],
        scratch_shapes=[pltpu.VMEM((D, FF), F32)],
        compiler_params=ROOM,
        cost_estimate=cost(9),
        name="mlp_back",
    )(mine, lab, near(h2), near(gp), near(c2), near(du), near(dy), g2, wup)


def att_back(mine, qkv, p, dxb, dx, h1, o, tok, wout, g1, wqkv):
    n = dxb.shape[0]
    return pl.pallas_call(
        att_back_kernel,
        grid=(n // TOK_BLOCK,),
        in_specs=[SMEM] + [VMEM] * 6 + [token_rows(D), const_spec((D, D)), const_spec((D,)), const_spec((D, 3 * D))],
        out_specs=[token_rows(D), VMEM, VMEM],
        out_shape=[pltpu.HBM((n, D), F32), pltpu.VMEM((768, D), BF), pltpu.VMEM((768, D), BF)],
        scratch_shapes=[pltpu.VMEM((n, 3 * D), BF), pltpu.VMEM((D, 4 * D), F32)],
        compiler_params=ROOM,
        cost_estimate=cost(14),
        name="att_back",
    )(mine, *[near(v) for v in (qkv, p, dxb, dx, h1, o)], tok, wout, g1, wqkv)


AXES = ("dp", "replica")


def swap(v, mask):
    return lax.ppermute(v, AXES, [(i, i ^ mask) for i in range(32)])


def plane(parts):
    return [swap(parts[m], 2 * m) for m in (1, 2, 3)]


def column(parts):
    return [swap(parts[m], 8 * m) for m in (1, 2, 3)]


def total_of(own, got):
    v = [own.astype(F32)] + [x.astype(F32) for x in got]
    return v[0] + v[1] if len(v) == 2 else (v[0] + v[1]) + (v[2] + v[3])


def added(own, got):
    return total_of(own, got).astype(BF)


def joined(own, got):
    return jnp.concatenate([own] + got, 0)


def shards(
    devices, tuned,
    text_tokens, segment_ids, pair_index, image_tokens,
    img_ln1, img_qkv, img_out, img_ln2, img_up, img_down, img_proj,
    txt_ln1, txt_qkv, txt_out, txt_ln2, txt_up, txt_down, txt_proj, log_scale,
):
    total = CAPS * devices
    denom = 2.0 * total
    row_of = jnp.arange(segment_ids.shape[0], dtype=jnp.int32) % (TOK_BLOCK // segment_ids.shape[1])
    lab = (segment_ids + PACK * row_of[:, None]).reshape(BLOCKS, 1, TOK_BLOCK)
    pair = pair_index
    if tuned:
        index = lax.axis_index(AXES)
        mine = ((index & 1) * 16 + ((index >> 1) & 3) * 4 + (index >> 3)).astype(jnp.int32).reshape(1)
        owner, row = pair // CAPS, pair % CAPS
        pair = (((owner & 1) * 16 + ((owner >> 1) & 3) * 4 + (owner >> 3)) ^ mine) * CAPS + row
    else:
        mine = jnp.zeros((1,), jnp.int32)
    pair = pair.reshape(CAPS, 1)
    lab, pair = lax.optimization_barrier((lab, pair))
    emb = image_tower(
        jnp.transpose(image_tokens, (1, 0, 2)), img_ln1, img_qkv, img_out, img_ln2, img_up, img_down, img_proj
    )
    if tuned:
        near = joined(emb, column([emb] * 4))
        o_now, o, qkv, p, h1 = text_att(text_tokens, lab, txt_ln1, txt_qkv)
        o_now, near = lax.optimization_barrier((o_now, near))
        got = plane([near] * 4)
    else:
        o_now, o, qkv, p, h1 = text_att(text_tokens, lab, txt_ln1, txt_qkv)
    h2, c2, gp, pu, pb, e, temb, cnt = text_mlp(text_tokens, o_now, lab, txt_out, txt_ln2, txt_up, txt_down, txt_proj)
    if tuned:
        near, got, temb = lax.optimization_barrier((near, got, temb))
        near = joined(near, got)
        own, other = near, swap(near, 1)
    else:
        own, other = jnp.split(lax.all_gather(emb, AXES, axis=0, tiled=True), 2)
    lines = total // 128
    g, sums = simple(
        functools.partial(cosine_kernel, denom),
        [((CAPS, total), F32), ((2 * lines + 8, 128), F32)],
        smem=2,
        us=3,
        name="cosine",
        held=(3, 4),
    )(log_scale, mine, temb, own, other, pair)
    (dt_row,) = simple(functools.partial(rows_kernel, denom), [((CAPS, D), F32)], smem=1, us=2, name="rows", held=(2, 3))(
        log_scale, g, own, other, pair
    )
    if tuned:
        sums = total_of(sums, [swap(sums, 1)])
        sums = total_of(sums, plane([sums] * 4))
        sums = total_of(sums, [swap(sums, 8)])
        sums = total_of(sums, [swap(sums, 16)])
    else:
        sums = lax.psum(sums, AXES)
    send_d, keep_d, send_p, keep_p, du, dy, loss, temp = simple(
        functools.partial(head_kernel, denom),
        [
            ((768, D), BF), ((768, D), BF), ((192, D), BF), ((192, D), BF),
            ((BLOCKS, 48, FF), BF), ((BLOCKS, 48, D), BF), ((1, 1), F32), ((1, 1), F32),
        ],
        [pltpu.VMEM((FF, D), F32), pltpu.VMEM((D, D), F32)],
        smem=2,
        us=5,
        name="head_back",
        held=(3, 4, 5),
    )(log_scale, mine, g, own, other, sums, dt_row, e, pb, cnt, pu, txt_proj, txt_down)
    dx, dxb, send_u, keep_u = mlp_back(mine, lab, h2, gp, c2, du, dy, txt_ln2, txt_up)

    def mlp_parts(d, u, p):
        both = jnp.concatenate([d.reshape(4, 4, 48, D), u.reshape(4, 4, 48, D)], 2).reshape(4, 384, D)
        return jnp.concatenate([both, p.reshape(4, 48, D)], 1)

    def spread_mlp(own, other):
        outs = [((FF, D), F32), ((D, FF), F32), ((D, D), F32), ((D,), F32)]
        return simple(spread_mlp_kernel, outs, smem=1, us=4, name="spread_mlp", held=(1, 2), held_out=False)(mine, own, other, txt_up, txt_ln2)

    def spread_att(own, other):
        outs = [((D, D), F32), ((D, 3 * D), F32), ((D,), F32)]
        return simple(spread_att_kernel, outs, smem=1, us=4, name="spread_att", held=(1, 2), held_out=False)(mine, own, other, txt_qkv, txt_ln1)

    if not tuned:
        grad_tokens, send_a, keep_a = att_back(
            mine, qkv, p, dxb, dx, h1, o, text_tokens, txt_out, txt_ln1, txt_qkv
        )
        sums = [keep_d, send_d, keep_u, send_u, keep_a, send_a, keep_p, send_p]
        d, d2, u, u2, a, a2, p, p2 = [v.astype(BF) for v in lax.psum([v.astype(F32) for v in sums], AXES)]
        grad_down, grad_up, grad_proj, gain2 = spread_mlp(
            mlp_parts(d, u, p).reshape(1728, D), mlp_parts(d2, u2, p2).reshape(1728, D)
        )
        grad_out, grad_qkv, gain1 = spread_att(a, a2)
    else:
        d = added(keep_d, [swap(send_d, 1)])
        pr = added(keep_p, [swap(send_p, 1)])
        m = mlp_parts(d, added(keep_u, [swap(send_u, 1)]), pr)
        dxb, m = lax.optimization_barrier((dxb, m))
        got = plane(m)
        grad_tokens, send_a, keep_a = att_back(
            mine, qkv, p, dxb, dx, h1, o, text_tokens, txt_out, txt_ln1, txt_qkv
        )
        other = swap(send_a, 1)
        got, keep_a = lax.optimization_barrier((got, keep_a))
        m = added(m[0], got)
        got = swap(m[192:], 8)
        a = added(keep_a, [other]).reshape(4, 192, D)
        got_a = plane(a)
        got, got_a[0] = lax.optimization_barrier((got, got_a[0]))
        m = added(joined(m[:192], [m[384:]]), [got])
        got = swap(m[96:], 16)
        got, got_a[1], got_a[2] = lax.optimization_barrier((got, got_a[1], got_a[2]))
        a = added(a[0], got_a)
        got_a = swap(a[96:], 8)
        m = added(joined(m[:96], [m[192:]]), [got])
        far = swap(m[:96], 16)
        a = added(a[:96], [got_a])
        got_a = swap(a[48:], 16)
        m = joined(m[:96], [far, m[96:]])
        m = joined(m[:192], [swap(m[:192], 8), m[192:]])
        got_m = plane([m] * 4)
        a, m = lax.optimization_barrier((added(a[:48], [got_a]), m))
        a = joined(a, [swap(a, 16)])
        a = joined(a, [swap(a, 8)])
        last, got_m[0], got_m[1] = lax.optimization_barrier((a, got_m[0], got_m[1]))
        got_a = plane([a, a, last, a])
        got_m[2], got_a[0], got_a[2] = lax.optimization_barrier((got_m[2], got_a[0], got_a[2]))
        m = joined(m, got_m)
        grad_down, grad_up, grad_proj, gain2 = spread_mlp(m, swap(m, 1))
        got_a, grad_up = lax.optimization_barrier((got_a, grad_up))
        a = joined(a, got_a)
        grad_out, grad_qkv, gain1 = spread_att(a, swap(a, 1))
    return (
        loss.reshape(1), grad_tokens, gain1, grad_qkv, grad_out, gain2,
        grad_up, grad_down, grad_proj, temp.reshape(1),
    )


def solution(mesh):
    both = ("dp", "replica")
    devices = mesh.shape["dp"] * mesh.shape["replica"]
    tuned = (mesh.shape["dp"], mesh.shape["replica"]) == (8, 4)
    rows = P(both, None)
    return jax.shard_map(
        functools.partial(shards, devices, tuned),
        mesh=mesh,
        in_specs=(rows, rows, P(both), P(both, None, None)) + (P(),) * 15,
        out_specs=(P(), rows) + (P(),) * 8,
        check_vma=False,
    )
```
